32 devices in a mesh: emb: 32 (over z, y, x, core).
Axes of the slice: x: 2, y: 2, z: 4, core: 2. Of those that a mesh axis runs over, the one named last changes fastest.
Arguments:
- token_ids: int32 [32768], P('emb')
- hot_ids: int32 [2048], replicated
- x_in: bfloat16 [32768, 1024], P('emb')
- d_out: bfloat16 [32768, 1024], P('emb')
- emb_table: bfloat16 [4, 50304, 1024], P(None, 'emb')
- hot_table: bfloat16 [4, 2048, 1024], replicated
- w_up: bfloat16 [4, 1024, 4096], replicated
- w_down: bfloat16 [4, 4096, 1024], replicated
- w_gate: bfloat16 [4, 1024, 1024], replicated
- w_proj: bfloat16 [4, 1024, 1024], replicated
Outputs:
- output 1: bfloat16 [32768, 1024], P('emb')
- output 2: float32 [4, 50304, 1024], P(None, 'emb')
- output 3: float32 [4, 2048, 1024], replicated
All inputs are finite; a program needn't handle non-finite values.
Results may differ from the reference program's by a relative error of at most 0.0156594.
Values are sent between devices in bfloat16 or wider.
A program may use at most 1 GiB of HBM per device.

```python
import math
import jax
import jax.numpy as jnp
from jax import lax

TOKENS = 1024
SHARDS = 32
MODEL_DIM = 1024
FF_DIM = 4096
EMB_DIM = 1024
VOCAB_SIZE = 50304
HOT_ROWS = 2048
LAYERS = 4

NORM_EPS = 1e-6
TOKENS_ALL = TOKENS * SHARDS
ROWS_DEV = VOCAB_SIZE // SHARDS
CAPACITY = max(8, (2 * TOKENS) // SHARDS)
LOG_VOCAB = int(math.log2(VOCAB_SIZE))


def draw_token_ids(key):
    k_perm, k_level, k_draw = jax.random.split(key, 3)
    perm_ids = jax.random.permutation(k_perm, VOCAB_SIZE).astype(jnp.int32)
    level = jax.random.randint(k_level, (TOKENS_ALL,), 0, LOG_VOCAB + 1)
    raw_draw = jax.random.randint(k_draw, (TOKENS_ALL,), 0, VOCAB_SIZE)
    span = jnp.minimum(jnp.left_shift(jnp.ones_like(level), level), VOCAB_SIZE)
    position = jnp.arange(TOKENS_ALL, dtype=jnp.int32)
    freq_rank = jnp.where(position % TOKENS < CAPACITY, HOT_ROWS, raw_draw % span)
    is_cold = freq_rank >= HOT_ROWS
    owner_id = perm_ids[freq_rank] // ROWS_DEV
    group_key = jnp.where(is_cold, (position // TOKENS) * SHARDS + owner_id, SHARDS * SHARDS)
    order = jnp.argsort(group_key, stable=True)
    sorted_key = group_key[order]
    group_start = jnp.searchsorted(sorted_key, sorted_key, side='left').astype(jnp.int32)
    within = jnp.zeros((TOKENS_ALL,), jnp.int32).at[order].set(position - group_start)
    freq_rank = jnp.where(is_cold & (within >= CAPACITY), position % HOT_ROWS, freq_rank)
    return perm_ids[freq_rank], perm_ids[:HOT_ROWS]


def normal_init(key, shape, scale):
    return (jax.random.normal(key, shape, jnp.float32) * scale).astype(jnp.bfloat16)


def setup_inputs(seed: int = 0) -> dict:
    keys = jax.random.split(jax.random.key(seed), 10)
    token_ids, hot_ids = draw_token_ids(keys[0])
    return {
        'token_ids': token_ids,
        'hot_ids': hot_ids,
        'x_in': normal_init(keys[1], (TOKENS_ALL, MODEL_DIM), 1.0),
        'd_out': normal_init(keys[2], (TOKENS_ALL, MODEL_DIM), 1.0),
        'emb_table': normal_init(keys[3], (LAYERS, VOCAB_SIZE, EMB_DIM), 1.0),
        'hot_table': normal_init(keys[4], (LAYERS, HOT_ROWS, EMB_DIM), 1.0),
        'w_up': normal_init(keys[5], (LAYERS, MODEL_DIM, FF_DIM), MODEL_DIM ** -0.5),
        'w_down': normal_init(keys[6], (LAYERS, FF_DIM, MODEL_DIM), 0.5 * FF_DIM ** -0.5),
        'w_gate': normal_init(keys[7], (LAYERS, MODEL_DIM, EMB_DIM), MODEL_DIM ** -0.5),
        'w_proj': normal_init(keys[8], (LAYERS, EMB_DIM, MODEL_DIM), 0.5 * EMB_DIM ** -0.5),
    }


def gelu_back(pre_act, cot_in):
    _, pull = jax.vjp(jax.nn.gelu, pre_act.astype(jnp.float32))
    return pull(cot_in)[0]


def dense_parts(resid, w_up, w_gate):
    resid_f = resid.astype(jnp.float32)
    inv_rms = lax.rsqrt(jnp.mean(resid_f * resid_f, axis=-1, keepdims=True) + NORM_EPS)
    normed = (resid_f * inv_rms).astype(jnp.bfloat16)
    hidden = jnp.dot(normed, w_up, preferred_element_type=jnp.float32).astype(jnp.bfloat16)
    gate_pre = jnp.dot(normed, w_gate, preferred_element_type=jnp.float32).astype(jnp.bfloat16)
    return resid_f, inv_rms, hidden, gate_pre


def layer_forward(resid, emb_rows, w_up, w_down, w_gate, w_proj):
    resid_f, _, hidden, gate_pre = dense_parts(resid, w_up, w_gate)
    activated = jax.nn.gelu(hidden.astype(jnp.float32)).astype(jnp.bfloat16)
    mlp_out = jnp.dot(activated, w_down, preferred_element_type=jnp.float32).astype(jnp.bfloat16)
    gate = jax.nn.gelu(gate_pre.astype(jnp.float32)).astype(jnp.bfloat16)
    mixed = (gate.astype(jnp.float32) * emb_rows.astype(jnp.float32)).astype(jnp.bfloat16)
    projected = jnp.dot(mixed, w_proj, preferred_element_type=jnp.float32).astype(jnp.bfloat16)
    return (resid_f + mlp_out.astype(jnp.float32) + projected.astype(jnp.float32)).astype(jnp.bfloat16)


def layer_backward(resid, emb_rows, d_next, w_up, w_down, w_gate, w_proj):
    resid_f, inv_rms, hidden, gate_pre = dense_parts(resid, w_up, w_gate)
    gate = jax.nn.gelu(gate_pre.astype(jnp.float32)).astype(jnp.bfloat16)
    d_cast = d_next.astype(jnp.bfloat16)
    d_mixed = jnp.dot(d_cast, w_proj.T, preferred_element_type=jnp.float32)
    d_rows = gate.astype(jnp.float32) * d_mixed
    d_gpre = gelu_back(gate_pre, d_mixed * emb_rows.astype(jnp.float32))
    d_hidden = gelu_back(hidden, jnp.dot(d_cast, w_down.T, preferred_element_type=jnp.float32))
    d_normed = (jnp.dot(d_hidden.astype(jnp.bfloat16), w_up.T, preferred_element_type=jnp.float32)
                + jnp.dot(d_gpre.astype(jnp.bfloat16), w_gate.T, preferred_element_type=jnp.float32))
    inner = jnp.mean(d_normed * resid_f, axis=-1, keepdims=True)
    d_prev = d_next + inv_rms * d_normed - resid_f * (inv_rms * inv_rms * inv_rms) * inner
    return d_prev, d_rows


def reference(token_ids, hot_ids, x_in, d_out, emb_table, hot_table, w_up, w_down, w_gate, w_proj):
    slot_map = jnp.full((VOCAB_SIZE,), -1, jnp.int32).at[hot_ids].set(jnp.arange(HOT_ROWS, dtype=jnp.int32))
    hot_slot = slot_map[token_ids]
    is_hot = hot_slot >= 0
    hot_slot = jnp.maximum(hot_slot, 0)

    def fwd_step(resid, layer_w):
        table_l, hot_l, up_l, down_l, gate_l, proj_l = layer_w
        emb_rows = jnp.where(is_hot[:, None], hot_l[hot_slot], table_l[token_ids])
        return layer_forward(resid, emb_rows, up_l, down_l, gate_l, proj_l), (resid, emb_rows)

    x_out, (x_saved, rows_saved) = lax.scan(fwd_step, x_in, (emb_table, hot_table, w_up, w_down, w_gate, w_proj))

    def bwd_step(d_resid, layer_w):
        resid_l, rows_l, up_l, down_l, gate_l, proj_l = layer_w
        d_prev, d_rows = layer_backward(resid_l, rows_l, d_resid, up_l, down_l, gate_l, proj_l)
        hot_part = jnp.where(is_hot[:, None], d_rows, 0.0)
        d_tab = jax.ops.segment_sum(d_rows - hot_part, token_ids, num_segments=VOCAB_SIZE)
        d_hot_l = jax.ops.segment_sum(hot_part, hot_slot, num_segments=HOT_ROWS)
        return d_prev, (d_tab, d_hot_l)

    _, (d_table, d_hot) = lax.scan(bwd_step, d_out.astype(jnp.float32), (x_saved, rows_saved, w_up, w_down, w_gate, w_proj), reverse=True)
    return x_out, d_table, d_hot
```

```python
import jax
import jax.numpy as jnp
from jax import lax
from jax.sharding import PartitionSpec as P

NORM_EPS = 1e-6
FREQ_MAX = 128
COLD_MAX = 256
LEVELS = (16, 20, 24, 28, 32, 40, 48, 64, 80, 96, 128, 160, 192, 256)
BF = jnp.bfloat16
F32 = jnp.float32


def gelu_back(pre_act, cot_in):
    _, pull = jax.vjp(jax.nn.gelu, pre_act.astype(F32))
    return pull(cot_in)[0]


def dot32(a, b):
    return jnp.dot(a, b, preferred_element_type=F32)


def dense_parts(resid, w_up, w_gate):
    resid_f = resid.astype(F32)
    inv_rms = lax.rsqrt(jnp.mean(resid_f * resid_f, axis=-1, keepdims=True) + NORM_EPS)
    normed = (resid_f * inv_rms).astype(BF)
    hidden = dot32(normed, w_up).astype(BF)
    gate_pre = dot32(normed, w_gate).astype(BF)
    return resid_f, inv_rms, hidden, gate_pre


def layer_forward(resid, emb_rows, w_up, w_down, w_gate, w_proj):
    resid_f, _, hidden, gate_pre = dense_parts(resid, w_up, w_gate)
    activated = jax.nn.gelu(hidden.astype(F32)).astype(BF)
    mlp_out = dot32(activated, w_down).astype(BF)
    gate = jax.nn.gelu(gate_pre.astype(F32)).astype(BF)
    mixed = (gate.astype(F32) * emb_rows.astype(F32)).astype(BF)
    projected = dot32(mixed, w_proj).astype(BF)
    return (resid_f + mlp_out.astype(F32) + projected.astype(F32)).astype(BF)


def layer_backward(resid, emb_rows, d_next, w_up, w_down, w_gate, w_proj):
    resid_f, inv_rms, hidden, gate_pre = dense_parts(resid, w_up, w_gate)
    gate = jax.nn.gelu(gate_pre.astype(F32)).astype(BF)
    d_cast = d_next.astype(BF)
    d_mixed = jnp.einsum('nd,ed->ne', d_cast, w_proj, preferred_element_type=F32)
    d_rows = gate.astype(F32) * d_mixed
    d_gpre = gelu_back(gate_pre, d_mixed * emb_rows.astype(F32))
    d_hidden = gelu_back(hidden, jnp.einsum('nd,fd->nf', d_cast, w_down, preferred_element_type=F32))
    d_normed = (jnp.einsum('nf,df->nd', d_hidden.astype(BF), w_up, preferred_element_type=F32)
                + jnp.einsum('ne,de->nd', d_gpre.astype(BF), w_gate, preferred_element_type=F32))
    inner = jnp.mean(d_normed * resid_f, axis=-1, keepdims=True)
    d_prev = d_next + inv_rms * d_normed - resid_f * (inv_rms * inv_rms * inv_rms) * inner
    return d_prev, d_rows


def general_path(n_dev, my_index, token_ids, hot_ids, x_in, d_out, emb_table, hot_table, w_up, w_down, w_gate, w_proj):
    n_loc = token_ids.shape[0]
    layers, rows_dev, emb_dim = emb_table.shape
    capacity = max(8, (2 * n_loc) // n_dev)
    n_slots = n_dev * capacity
    hot_match = token_ids[:, None] == hot_ids[None, :]
    is_hot = jnp.any(hot_match, axis=1)
    hot_pick = hot_match.astype(BF)
    hot_pick_f = hot_match.astype(F32)
    owner_id = token_ids // rows_dev
    to_owner = (owner_id[:, None] == jnp.arange(n_dev, dtype=jnp.int32)[None, :]) & jnp.logical_not(is_hot)[:, None]
    owner_rank = jnp.cumsum(to_owner.astype(jnp.int32), axis=0) - 1
    place = jnp.sum(jnp.where(to_owner, owner_rank, 0), axis=1)
    slot = jnp.where(is_hot, n_slots, owner_id * capacity + place)
    send_ids = jnp.full((n_slots,), -1, jnp.int32).at[slot].set(token_ids, mode='drop')
    slot_tok = jnp.full((n_slots,), -1, jnp.int32).at[slot].set(jnp.arange(n_loc, dtype=jnp.int32), mode='drop')
    recv_ids = lax.all_to_all(send_ids.reshape(n_dev, capacity), 'emb', 0, 0, tiled=True).reshape(n_slots)
    served_ok = recv_ids >= 0
    local_row = jnp.where(served_ok, recv_ids - my_index * rows_dev, 0)
    pick_slot = jnp.minimum(slot, n_slots - 1)
    slot_used = slot_tok >= 0
    slot_src = jnp.maximum(slot_tok, 0)

    def fwd(resid, per_layer):
        table, hot_l, up, down, gate_w, proj = per_layer
        served = jnp.take(table, local_row, axis=0)
        fetched = lax.all_to_all(served.reshape(n_dev, capacity, emb_dim), 'emb', 0, 0, tiled=True).reshape(n_slots, emb_dim)
        cold_rows = jnp.take(fetched, pick_slot, axis=0)
        hot_rows = dot32(hot_pick, hot_l).astype(BF)
        emb_rows = jnp.where(is_hot[:, None], hot_rows, cold_rows)
        return layer_forward(resid, emb_rows, up, down, gate_w, proj), (resid, emb_rows)

    x_out, (x_saved, rows_saved) = lax.scan(fwd, x_in, (emb_table, hot_table, w_up, w_down, w_gate, w_proj))

    def bwd(d_resid, per_layer):
        resid_l, rows_l, up, down, gate_w, proj = per_layer
        d_resid, d_rows = layer_backward(resid_l, rows_l, d_resid, up, down, gate_w, proj)
        outgoing = jnp.where(slot_used[:, None], jnp.take(d_rows, slot_src, axis=0), 0.0)
        incoming = lax.all_to_all(outgoing.reshape(n_dev, capacity, emb_dim), 'emb', 0, 0, tiled=True).reshape(n_slots, emb_dim)
        d_tab = jax.ops.segment_sum(jnp.where(served_ok[:, None], incoming, 0.0), local_row, num_segments=rows_dev)
        hot_local = jnp.einsum('nh,ne->he', hot_pick_f, d_rows, precision=lax.Precision.HIGHEST, preferred_element_type=F32)
        return d_resid, (d_tab, lax.psum(hot_local, 'emb'))

    _, (d_table, d_hot) = lax.scan(bwd, d_out.astype(F32), (x_saved, rows_saved, w_up, w_down, w_gate, w_proj), reverse=True)
    return x_out, d_table, d_hot


def split3(v):
    hi = lax.reduce_precision(v, 8, 7)
    rest = v - hi
    mid = lax.reduce_precision(rest, 8, 7)
    return hi.astype(BF), mid.astype(BF), (rest - mid).astype(BF)


def pick_sum(pick, v):
    hi, mid, lo = split3(v)
    return dot32(pick, hi) + (dot32(pick, mid) + dot32(pick, lo))


def iota(shape, dim):
    return lax.broadcasted_iota(jnp.int32, shape, dim)


def one_hot(v, n, dtype=BF):
    return (v[:, None] == iota((v.shape[0], n), 1)).astype(dtype)


def solution(mesh):
    n_dev = mesh.shape['emb']

    def body(token_ids, hot_ids, x_in, d_out, emb_table, hot_table, w_up, w_down, w_gate, w_proj):
        n_loc = token_ids.shape[0]
        layers, rows_dev, emb_dim = emb_table.shape
        n_hot = hot_ids.shape[0]
        places = n_loc // n_dev
        hot_dev = n_hot // n_dev
        vocab = rows_dev * n_dev
        n_hi = -(-vocab // 2048) * 8
        me = lax.axis_index('emb')

        tok_hi = one_hot(token_ids >> 8, n_hi)
        tok_lo = one_hot(token_ids & 255, 256)
        count = lax.psum(dot32(tok_hi.T, tok_lo), 'emb')
        hot_hi = one_hot(hot_ids >> 8, n_hi)
        hot_lo = one_hot(hot_ids & 255, 256)
        slot_no = jnp.arange(n_hot, dtype=jnp.int32)
        q_map = dot32(hot_hi.T, hot_lo * (slot_no // n_dev + 1).astype(BF)[:, None]).astype(BF)
        r_map = dot32(hot_hi.T, hot_lo * (slot_no % n_dev).astype(BF)[:, None]).astype(BF)
        levels = jnp.array(LEVELS, F32)
        n_over = jnp.sum((count[:, :, None] >= levels).astype(F32), axis=(0, 1))
        level = jnp.min(jnp.where(n_over <= FREQ_MAX, levels, 1e9))
        freq = count >= level
        freq_b = freq.astype(BF)
        in_row = dot32(freq_b, (iota((256, 256), 0) < iota((256, 256), 1)).astype(BF))
        per_row = jnp.sum(freq.astype(F32), axis=1)
        before = jnp.sum(jnp.where(iota((n_hi, n_hi), 0) > iota((n_hi, n_hi), 1), per_row[None, :], 0.0), axis=1)
        freq_map = jnp.where(freq, in_row + before[:, None] + 1.0, 0.0).astype(BF)

        def look(hi, lo, *maps):
            got = dot32(hi, jnp.concatenate(maps, axis=1)).reshape(hi.shape[0], len(maps), 256)
            got = jnp.sum(got * lo.astype(F32)[:, None, :], axis=2).astype(jnp.int32)
            return [got[:, i] for i in range(len(maps))]

        tok_f, tok_q, tok_r = look(tok_hi, tok_lo, freq_map, q_map, r_map)
        (hot_f,) = look(hot_hi, hot_lo, freq_map)
        row_ids = me * rows_dev + jnp.arange(rows_dev, dtype=jnp.int32)
        row_f, row_q, row_n = look(one_hot(row_ids >> 8, n_hi), one_hot(row_ids & 255, 256),
                                   freq_map, q_map, (count > 0).astype(BF))

        rare = tok_f == 0
        owner = jnp.where(tok_q > 0, tok_r, token_ids // rows_dev)
        to_dev = (owner[:, None] == iota((n_loc, n_dev), 1)) & rare[:, None]
        marks = jnp.concatenate([to_dev.astype(BF), jnp.logical_not(rare).astype(BF)[:, None]], axis=1)
        earlier = (iota((n_loc, n_loc), 0) > iota((n_loc, n_loc), 1)).astype(BF)
        ranks = dot32(earlier, marks)
        sent = jnp.sum(to_dev.astype(F32), axis=0)
        fits = jnp.max(sent) <= places
        free = jnp.maximum(places - sent, 0.0)
        free_at = jnp.sum(jnp.where(iota((n_dev, n_dev), 0) > iota((n_dev, n_dev), 1), free[None, :], 0.0), axis=1)
        fill = ranks[:, n_dev]
        fill_dev = (fill[:, None] >= free_at[None, :]) & (fill[:, None] < (free_at + free)[None, :])
        fill_place = jnp.sum(jnp.where(fill_dev, fill[:, None] + (sent - free_at)[None, :], 0.0), axis=1)
        rare_place = jnp.sum(jnp.where(to_dev, ranks[:, :n_dev], 0.0), axis=1)
        dev_no = iota((n_loc, n_dev), 1)
        dest = jnp.sum(jnp.where(jnp.where(rare[:, None], to_dev, fill_dev), dev_no, 0), axis=1)
        slot = dest * places + jnp.where(rare, rare_place, fill_place).astype(jnp.int32)
        row_used = (row_n > 0) & (row_f == 0) & (row_q == 0)
        fits = fits & (jnp.sum(row_used.astype(jnp.int32)) <= COLD_MAX)
        tok_class = jnp.where(rare, jnp.where(tok_q > 0, FREQ_MAX + tok_q - 1, FREQ_MAX + hot_dev + token_ids % rows_dev),
                              tok_f - 1)
        move = iota((n_loc, n_loc), 0) == slot[None, :]
        move_b = move.astype(BF)
        send_class = jnp.sum(jnp.where(move, tok_class[None, :], 0), axis=1) + jnp.where(fits, 0, 1 << 20)
        got_class = lax.all_to_all(send_class.reshape(n_dev, places), 'emb', 0, 0, tiled=True).reshape(n_loc)
        all_fit = jnp.max(got_class) < (1 << 20)

        def exchange(v):
            return lax.all_to_all(v.reshape(n_dev, places, -1), 'emb', 0, 0, tiled=True).reshape(n_loc, -1)

        x_moved = exchange(dot32(move_b, x_in).astype(BF))

        def fast(x_moved, d_out):
            d_moved = exchange(dot32(move_b, d_out).astype(BF))
            row_freq = one_hot(row_f - 1, FREQ_MAX) * (row_q == 0).astype(BF)[:, None]
            hot_freq = one_hot(hot_f - 1, FREQ_MAX)
            freq_is_hot = jnp.max(hot_freq, axis=0) > 0
            freq_cold = lax.psum(jnp.stack([dot32(row_freq.T, emb_table[i]) for i in range(layers)]).astype(BF), 'emb')
            used_rank = jnp.sum(jnp.where((iota((rows_dev, rows_dev), 0) > iota((rows_dev, rows_dev), 1)) & row_used[None, :], 1, 0), axis=1)
            row_pack = one_hot(used_rank, COLD_MAX) * row_used.astype(BF)[:, None]
            hot_mine = lax.dynamic_index_in_dim(hot_table.reshape(layers, hot_dev, n_dev, emb_dim), me, 2, keepdims=False)
            hot_f_mine = lax.dynamic_index_in_dim(hot_f.reshape(hot_dev, n_dev), me, 1, keepdims=False)
            cold_at = FREQ_MAX + hot_dev
            row_of = got_class - cold_at
            cold_class = jnp.sum(jnp.where(row_used[None, :] & (iota((n_loc, rows_dev), 1) < row_of[:, None]), 1, 0), axis=1)
            local_class = jnp.where(row_of >= 0, cold_at + cold_class, got_class)
            pick = one_hot(local_class, cold_at + COLD_MAX)
            saved = []
            resid = x_moved
            for i in range(layers):
                freq_hot = dot32(hot_freq.T, hot_table[i]).astype(BF)
                freq_rows = jnp.where(freq_is_hot[:, None], freq_hot, freq_cold[i])
                cold_rows = dot32(row_pack.T, emb_table[i]).astype(BF)
                table = jnp.concatenate([freq_rows, hot_mine[i], cold_rows], axis=0)
                emb_rows = dot32(pick, table).astype(BF)
                saved.append((resid, emb_rows))
                resid = layer_forward(resid, emb_rows, w_up[i], w_down[i], w_gate[i], w_proj[i])
            x_out = dot32(move_b.T, exchange(resid)).astype(BF)
            d_resid = d_moved.astype(F32)
            d_tables, d_hots = [], []
            back = jnp.concatenate([row_pack, row_freq], axis=1)
            hot_back = one_hot(hot_f_mine - 1, FREQ_MAX)
            for i in reversed(range(layers)):
                d_resid, d_rows = layer_backward(*saved[i], d_resid, w_up[i], w_down[i], w_gate[i], w_proj[i])
                sums = pick_sum(pick.T, d_rows)
                freq_sum = lax.psum(sums[:FREQ_MAX], 'emb')
                d_tables.append(pick_sum(back, jnp.concatenate([sums[cold_at:], freq_sum], axis=0)))
                mine = sums[FREQ_MAX:cold_at] + pick_sum(hot_back, freq_sum)
                d_hots.append(lax.all_gather(mine, 'emb', axis=1).reshape(n_hot, emb_dim))
            return x_out, jnp.stack(d_tables[::-1]), jnp.stack(d_hots[::-1])

        def slow(x_moved, d_out):
            return general_path(n_dev, me, token_ids, hot_ids, x_in, d_out, emb_table, hot_table, w_up, w_down, w_gate, w_proj)

        return lax.cond(all_fit, fast, slow, x_moved, d_out)

    return jax.shard_map(body, mesh=mesh,
                         in_specs=(P('emb'), P(), P('emb', None), P('emb', None), P(None, 'emb', None), P(), P(), P(), P(), P()),
                         out_specs=(P('emb', None), P(None, 'emb', None), P()),
                         check_vma=False)
```

```python
import functools

import jax
import jax.numpy as jnp
from jax import lax
from jax.experimental import pallas as pl
from jax.experimental.pallas import tpu as pltpu
from jax.sharding import PartitionSpec as P

NORM_EPS = 1e-6
FREQ_HOT = 128
FREQ_COLD = 32
COLD_DEV = 2
FREQ = FREQ_HOT + FREQ_COLD
COLD_MAX = 256
GELU_A = 0.7978845608028654
GELU_B = GELU_A * 0.044715
VMEM = 66_000_000
ROWS = 256
LEVELS = (16, 20, 24, 28, 32, 40, 48, 64, 80, 96, 128, 160, 192, 256)
BF = jnp.bfloat16
F32 = jnp.float32


def gelu_back(pre_act, cot_in):
    _, pull = jax.vjp(jax.nn.gelu, pre_act.astype(F32))
    return pull(cot_in)[0]


def dot32(a, b):
    return jnp.dot(a, b, preferred_element_type=F32)


def dense_parts(resid, w_up, w_gate):
    resid_f = resid.astype(F32)
    inv_rms = lax.rsqrt(jnp.mean(resid_f * resid_f, axis=-1, keepdims=True) + NORM_EPS)
    normed = (resid_f * inv_rms).astype(BF)
    hidden = dot32(normed, w_up).astype(BF)
    gate_pre = dot32(normed, w_gate).astype(BF)
    return resid_f, inv_rms, hidden, gate_pre


def layer_forward(resid, emb_rows, w_up, w_down, w_gate, w_proj):
    resid_f, _, hidden, gate_pre = dense_parts(resid, w_up, w_gate)
    activated = jax.nn.gelu(hidden.astype(F32)).astype(BF)
    mlp_out = dot32(activated, w_down).astype(BF)
    gate = jax.nn.gelu(gate_pre.astype(F32)).astype(BF)
    mixed = (gate.astype(F32) * emb_rows.astype(F32)).astype(BF)
    projected = dot32(mixed, w_proj).astype(BF)
    return (resid_f + mlp_out.astype(F32) + projected.astype(F32)).astype(BF)


def layer_backward(resid, emb_rows, d_next, w_up, w_down, w_gate, w_proj):
    resid_f, inv_rms, hidden, gate_pre = dense_parts(resid, w_up, w_gate)
    gate = jax.nn.gelu(gate_pre.astype(F32)).astype(BF)
    d_cast = d_next.astype(BF)
    d_mixed = jnp.einsum('nd,ed->ne', d_cast, w_proj, preferred_element_type=F32)
    d_rows = gate.astype(F32) * d_mixed
    d_gpre = gelu_back(gate_pre, d_mixed * emb_rows.astype(F32))
    d_hidden = gelu_back(hidden, jnp.einsum('nd,fd->nf', d_cast, w_down, preferred_element_type=F32))
    d_normed = (jnp.einsum('nf,df->nd', d_hidden.astype(BF), w_up, preferred_element_type=F32)
                + jnp.einsum('ne,de->nd', d_gpre.astype(BF), w_gate, preferred_element_type=F32))
    inner = jnp.mean(d_normed * resid_f, axis=-1, keepdims=True)
    d_prev = d_next + inv_rms * d_normed - resid_f * (inv_rms * inv_rms * inv_rms) * inner
    return d_prev, d_rows


def general_path(n_dev, my_index, token_ids, hot_ids, x_in, d_out, emb_table, hot_table, w_up, w_down, w_gate, w_proj):
    n_loc = token_ids.shape[0]
    layers, rows_dev, emb_dim = emb_table.shape
    capacity = max(8, (2 * n_loc) // n_dev)
    n_slots = n_dev * capacity
    hot_match = token_ids[:, None] == hot_ids[None, :]
    is_hot = jnp.any(hot_match, axis=1)
    hot_pick = hot_match.astype(BF)
    hot_pick_f = hot_match.astype(F32)
    owner_id = token_ids // rows_dev
    to_owner = (owner_id[:, None] == jnp.arange(n_dev, dtype=jnp.int32)[None, :]) & jnp.logical_not(is_hot)[:, None]
    owner_rank = jnp.cumsum(to_owner.astype(jnp.int32), axis=0) - 1
    place = jnp.sum(jnp.where(to_owner, owner_rank, 0), axis=1)
    slot = jnp.where(is_hot, n_slots, owner_id * capacity + place)
    send_ids = jnp.full((n_slots,), -1, jnp.int32).at[slot].set(token_ids, mode='drop')
    slot_tok = jnp.full((n_slots,), -1, jnp.int32).at[slot].set(jnp.arange(n_loc, dtype=jnp.int32), mode='drop')
    recv_ids = lax.all_to_all(send_ids.reshape(n_dev, capacity), 'emb', 0, 0, tiled=True).reshape(n_slots)
    served_ok = recv_ids >= 0
    local_row = jnp.where(served_ok, recv_ids - my_index * rows_dev, 0)
    pick_slot = jnp.minimum(slot, n_slots - 1)
    slot_used = slot_tok >= 0
    slot_src = jnp.maximum(slot_tok, 0)

    def fwd(resid, per_layer):
        table, hot_l, up, down, gate_w, proj = per_layer
        served = jnp.take(table, local_row, axis=0)
        fetched = lax.all_to_all(served.reshape(n_dev, capacity, emb_dim), 'emb', 0, 0, tiled=True).reshape(n_slots, emb_dim)
        cold_rows = jnp.take(fetched, pick_slot, axis=0)
        hot_rows = dot32(hot_pick, hot_l).astype(BF)
        emb_rows = jnp.where(is_hot[:, None], hot_rows, cold_rows)
        return layer_forward(resid, emb_rows, up, down, gate_w, proj), (resid, emb_rows)

    x_out, (x_saved, rows_saved) = lax.scan(fwd, x_in, (emb_table, hot_table, w_up, w_down, w_gate, w_proj))

    def bwd(d_resid, per_layer):
        resid_l, rows_l, up, down, gate_w, proj = per_layer
        d_resid, d_rows = layer_backward(resid_l, rows_l, d_resid, up, down, gate_w, proj)
        outgoing = jnp.where(slot_used[:, None], jnp.take(d_rows, slot_src, axis=0), 0.0)
        incoming = lax.all_to_all(outgoing.reshape(n_dev, capacity, emb_dim), 'emb', 0, 0, tiled=True).reshape(n_slots, emb_dim)
        d_tab = jax.ops.segment_sum(jnp.where(served_ok[:, None], incoming, 0.0), local_row, num_segments=rows_dev)
        hot_local = jnp.einsum('nh,ne->he', hot_pick_f, d_rows, precision=lax.Precision.HIGHEST, preferred_element_type=F32)
        return d_resid, (d_tab, lax.psum(hot_local, 'emb'))

    _, (d_table, d_hot) = lax.scan(bwd, d_out.astype(F32), (x_saved, rows_saved, w_up, w_down, w_gate, w_proj), reverse=True)
    return x_out, d_table, d_hot


def split3(v):
    hi = v.astype(BF)
    rest = v - hi.astype(F32)
    mid = rest.astype(BF)
    return hi, mid, (rest - mid.astype(F32)).astype(BF)


def iota(shape, dim):
    return lax.broadcasted_iota(jnp.int32, shape, dim)


def one_hot(v, n, dtype=BF):
    return (v[:, None] == iota((v.shape[0], n), 1)).astype(dtype)


def dot_nt(a, b):
    return lax.dot_general(a, b, (((1,), (1,)), ((), ())), preferred_element_type=F32)


def gelu(x):
    half = 0.5 * x
    return half + half * jnp.tanh(x * (GELU_A + GELU_B * (x * x)))


def gelu_slope(x):
    sq = x * x
    th = jnp.tanh(x * (GELU_A + GELU_B * sq))
    return (0.5 + 0.5 * th) + (0.5 * x) * (1.0 - th * th) * (GELU_A + (3.0 * GELU_B) * sq)


def forward_kernel(n_l, n_f, x0, cls, table, wu, wd, wg, wp, xs, hs, ss, xo, x_now, u_now, acc, q_now):
    layer, step = pl.program_id(0), pl.program_id(1)
    n_tok = x_now.shape[0]
    parts = [pl.ds(m, ROWS) for m in range(0, n_tok, ROWS)]

    @pl.when((layer == 0) & (step == 0))
    def _():
        x_now[...] = x0[...]

    @pl.when(step == 0)
    def _():
        for m in parts:
            xb = x_now[m, :]
            x = xb.astype(F32)
            xs[0, m, :] = xb
            u = (x * lax.rsqrt(jnp.mean(x * x, axis=-1, keepdims=True) + NORM_EPS)).astype(BF)
            u_now[m, :] = u
            s = dot32(u, wg[0]).astype(BF)
            ss[0, m, :] = s
            g = gelu(s.astype(F32)).astype(BF)
            pick = (cls[m, :] == iota((ROWS, table.shape[1]), 1)).astype(BF)
            e = dot32(pick, table[0]).astype(BF)
            mixed = (g.astype(F32) * e.astype(F32)).astype(BF)
            q_now[m, :] = dot32(mixed, wp[0]).astype(BF)
            acc[m, :] = jnp.zeros((ROWS, acc.shape[1]), F32)

    for m in parts:
        h = dot32(u_now[m, :], wu[0]).astype(BF)
        hs[0, m, :] = h
        act = gelu(h.astype(F32)).astype(BF)
        acc[m, :] += dot32(act, wd[0])

    @pl.when(step == n_f - 1)
    def _():
        for m in parts:
            x = x_now[m, :].astype(F32) + acc[m, :].astype(BF).astype(F32) + q_now[m, :].astype(F32)
            x_now[m, :] = x.astype(BF)

    @pl.when((step == n_f - 1) & (layer == n_l - 1))
    def _():
        xo[...] = x_now[...]


def forward(x0, cls, table, w_up, w_down, w_gate, w_proj):
    n_tok, dim = x0.shape
    n_l, _, ff = w_up.shape
    emb = w_gate.shape[2]
    tile = min(512, ff)
    n_f = ff // tile
    n_c = table.shape[1]
    flops = n_l * 2 * n_tok * dim * (2 * ff + 2 * emb + n_c)
    return pl.pallas_call(
        functools.partial(forward_kernel, n_l, n_f),
        grid=(n_l, n_f),
        in_specs=[
            pl.BlockSpec((n_tok, dim), lambda l, f: (0, 0)),
            pl.BlockSpec((n_tok, 1), lambda l, f: (0, 0)),
            pl.BlockSpec((1, n_c, emb), lambda l, f: (l, 0, 0)),
            pl.BlockSpec((1, dim, tile), lambda l, f: (l, 0, f)),
            pl.BlockSpec((1, tile, dim), lambda l, f: (l, f, 0)),
            pl.BlockSpec((1, dim, emb), lambda l, f: (l, 0, 0)),
            pl.BlockSpec((1, emb, dim), lambda l, f: (l, 0, 0)),
        ],
        out_specs=[
            pl.BlockSpec((1, n_tok, dim), lambda l, f: (l, 0, 0)),
            pl.BlockSpec((1, n_tok, tile), lambda l, f: (l, 0, f)),
            pl.BlockSpec((1, n_tok, emb), lambda l, f: (l, 0, 0)),
            pl.BlockSpec((n_tok, dim), lambda l, f: (0, 0)),
        ],
        out_shape=[
            jax.ShapeDtypeStruct((n_l, n_tok, dim), BF),
            jax.ShapeDtypeStruct((n_l, n_tok, ff), BF),
            jax.ShapeDtypeStruct((n_l, n_tok, emb), BF),
            jax.ShapeDtypeStruct((n_tok, dim), BF),
        ],
        scratch_shapes=[pltpu.VMEM((n_tok, dim), BF), pltpu.VMEM((n_tok, dim), BF),
                        pltpu.VMEM((n_tok, dim), F32), pltpu.VMEM((n_tok, dim), BF)],
        compiler_params=pltpu.CompilerParams(vmem_limit_bytes=VMEM, dimension_semantics=("arbitrary", "arbitrary")),
        cost_estimate=pl.CostEstimate(flops=flops, bytes_accessed=n_l * 40_000_000, transcendentals=0),
        name="forward",
    )(x0, cls, table, w_up, w_down, w_gate, w_proj)


def backward_kernel(n_l, n_f, last_full, r_in, cls, cls_t, table, xs, hs, ss, wu, wd, wg, wp, sums, r, c_now, acc, three):
    step = pl.program_id(0)
    index, f = step // n_f, step % n_f
    n_tok, emb = c_now.shape[0], ss.shape[2]
    parts = [pl.ds(m, ROWS) for m in range(0, n_tok, ROWS)]
    goes_on = True if last_full else index < n_l - 1

    @pl.when(step == 0)
    def _():
        r[...] = r_in[...].astype(F32)

    @pl.when(f == 0)
    def _():
        for m in parts:
            c = r[m, :].astype(BF)
            c_now[m, :] = c
            a = dot_nt(c, wp[0])
            s = ss[0, m, :].astype(F32)
            rows = gelu(s).astype(BF).astype(F32) * a
            for i, part in enumerate(split3(rows)):
                three[i, m, :] = part
            pick = (cls[m, :] == iota((ROWS, table.shape[1]), 1)).astype(BF)
            e = dot32(pick, table[0])
            ds = (gelu_slope(s) * (a * e)).astype(BF)
            acc[m, :] = dot_nt(ds, wg[0])
        pick_t = (cls_t[...] == iota((table.shape[1], n_tok), 0)).astype(BF)
        sums[0] = dot32(pick_t, three[0]) + (dot32(pick_t, three[1]) + dot32(pick_t, three[2]))

    @pl.when(goes_on)
    def _():
        for m in parts:
            d_act = dot_nt(c_now[m, :], wd[0])
            dh = (gelu_slope(hs[0, m, :].astype(F32)) * d_act).astype(BF)
            acc[m, :] += dot_nt(dh, wu[0])

    @pl.when((f == n_f - 1) & goes_on)
    def _():
        for m in parts:
            x = xs[0, m, :].astype(F32)
            k = lax.rsqrt(jnp.mean(x * x, axis=-1, keepdims=True) + NORM_EPS)
            du = acc[m, :]
            inner = jnp.mean(du * x, axis=-1, keepdims=True)
            r[m, :] = r[m, :] + k * du - x * (k * k * k) * inner


def backward(first, n_l, last_full, r_in, cls, cls_t, table, xs, hs, ss, w_up, w_down, w_gate, w_proj):
    n_tok, dim = r_in.shape
    ff = w_up.shape[2]
    emb = w_gate.shape[2]
    tile = min(512, ff)
    n_f = ff // tile
    n_c = table.shape[1]
    n_steps = n_l * n_f if last_full else (n_l - 1) * n_f + 1

    def whole(t):
        return (first - t // n_f, 0, 0)

    def cols(t):
        return (first - t // n_f, 0, t % n_f)

    def rows(t):
        return (first - t // n_f, t % n_f, 0)

    once = pl.Buffered(1)
    return pl.pallas_call(
        functools.partial(backward_kernel, n_l, n_f, last_full),
        grid=(n_steps,),
        in_specs=[
            pl.BlockSpec((n_tok, dim), lambda t: (0, 0), pipeline_mode=once),
            pl.BlockSpec((n_tok, 1), lambda t: (0, 0), pipeline_mode=once),
            pl.BlockSpec((1, n_tok), lambda t: (0, 0), pipeline_mode=once),
            pl.BlockSpec((1, n_c, emb), whole),
            pl.BlockSpec((1, n_tok, dim), whole),
            pl.BlockSpec((1, n_tok, tile), cols),
            pl.BlockSpec((1, n_tok, emb), whole),
            pl.BlockSpec((1, dim, tile), cols),
            pl.BlockSpec((1, tile, dim), rows),
            pl.BlockSpec((1, dim, emb), whole),
            pl.BlockSpec((1, emb, dim), whole),
        ],
        out_specs=[
            pl.BlockSpec((1, n_c, emb), lambda t: (t // n_f, 0, 0)),
            pl.BlockSpec((n_tok, dim), lambda t: (0, 0)),
        ],
        out_shape=[
            jax.ShapeDtypeStruct((n_l, n_c, emb), F32),
            jax.ShapeDtypeStruct((n_tok, dim), F32),
        ],
        scratch_shapes=[pltpu.VMEM((n_tok, dim), BF), pltpu.VMEM((n_tok, dim), F32), pltpu.VMEM((3, n_tok, emb), BF)],
        compiler_params=pltpu.CompilerParams(vmem_limit_bytes=VMEM, dimension_semantics=("arbitrary",)),
        cost_estimate=pl.CostEstimate(flops=n_l * 2 * n_tok * dim * (2 * ff + 2 * emb + 4 * n_c),
                                      bytes_accessed=n_l * 40_000_000, transcendentals=0),
        name="backward",
    )(r_in, cls, cls_t, table, xs, hs, ss, w_up, w_down, w_gate, w_proj)


def hot_kernel(n_dev, raw, freq, code, into, out):
    n_r = raw.shape[2]
    sel = (code[0] == iota((n_r * n_dev, freq.shape[1]), 1)).astype(BF)
    hi, mid, lo = split3(freq[0])
    more = dot32(sel, hi) + (dot32(sel, mid) + dot32(sel, lo))
    for i in range(n_r):
        at = pl.ds(i * n_dev, n_dev)
        out[0, at, :] = raw[:, 0, i, :] + more[i * n_dev:(i + 1) * n_dev, :]


def hot_out(first, gathered, freq, code, into):
    n_dev, n_l, hot_dev, emb = gathered.shape
    n_r = 8
    blocks = hot_dev // n_r
    width = n_r * n_dev
    return pl.pallas_call(
        functools.partial(hot_kernel, n_dev),
        grid=(n_l, blocks),
        in_specs=[
            pl.BlockSpec((n_dev, 1, n_r, emb), lambda i, b: (0, i, b, 0)),
            pl.BlockSpec((1, freq.shape[1], emb), lambda i, b: (i, 0, 0)),
            pl.BlockSpec((1, width, 1), lambda i, b: (b, 0, 0)),
            pl.BlockSpec(memory_space=pl.ANY),
        ],
        out_specs=pl.BlockSpec((1, width, emb), lambda i, b: (first - i, b, 0)),
        out_shape=jax.ShapeDtypeStruct(into.shape, F32),
        input_output_aliases={3: 0},
        compiler_params=pltpu.CompilerParams(vmem_limit_bytes=VMEM, dimension_semantics=("arbitrary", "arbitrary")),
        name="hot_out",
    )(gathered, freq, code.reshape(blocks, width, 1), into)


def empty_kernel(out):
    pass


def empty(shape):
    return pl.pallas_call(empty_kernel, out_specs=pl.BlockSpec(memory_space=pl.ANY),
                          out_shape=jax.ShapeDtypeStruct(shape, F32), name="empty")()


def table_kernel(n_l, n_cold, starts, row_of, *refs):
    srcs, out = refs[:-1], refs[-1]
    block = pl.program_id(0)
    n_rows = out.shape[0]
    out[...] = jnp.zeros(out.shape, F32)

    def put(k):
        at = row_of[k] - block * n_rows
        for l in range(n_l):
            out[at, pl.ds(l, 1), :] = srcs[l][pl.ds(k, 1), :]

    @pl.loop(starts[block], starts[block + 1])
    def _(k):
        put(k)

    @pl.loop(n_cold, row_of.shape[0])
    def _(k):
        pl.when((row_of[k] >= block * n_rows) & (row_of[k] < (block + 1) * n_rows))(lambda: put(k))


def table_out(rows_dev, starts, row_of, srcs, n_blocks):
    n_l = len(srcs)
    emb = srcs[0].shape[1]
    n_rows = rows_dev // n_blocks
    n_cold = row_of.shape[0] - FREQ_COLD
    return pl.pallas_call(
        functools.partial(table_kernel, n_l, n_cold),
        grid_spec=pltpu.PrefetchScalarGridSpec(
            num_scalar_prefetch=2, grid=(n_blocks,),
            in_specs=[pl.BlockSpec(srcs[0].shape, lambda b, *_: (0, 0))] * n_l,
            out_specs=pl.BlockSpec((n_rows, n_l, emb), lambda b, *_: (b, 0, 0))),
        out_shape=jax.ShapeDtypeStruct((rows_dev, n_l, emb), F32),
        compiler_params=pltpu.CompilerParams(vmem_limit_bytes=VMEM, dimension_semantics=("arbitrary",)),
        name="table_out",
    )(starts, row_of, *srcs)


def solution(mesh):
    n_dev = mesh.shape['emb']

    def body(token_ids, hot_ids, x_in, d_out, emb_table, hot_table, w_up, w_down, w_gate, w_proj):
        n_loc = token_ids.shape[0]
        layers, rows_dev, emb_dim = emb_table.shape
        n_hot = hot_ids.shape[0]
        places = n_loc // n_dev
        hot_dev = n_hot // n_dev
        vocab = rows_dev * n_dev
        n_hi = -(-vocab // 2048) * 8
        me = lax.axis_index('emb')
        hot_at, cold_at = FREQ, FREQ + hot_dev
        n_class = cold_at + COLD_MAX

        all_ids = lax.all_gather(token_ids, 'emb', tiled=True)
        count = dot32((iota((n_hi, all_ids.shape[0]), 0) == (all_ids >> 8)[None, :]).astype(BF), one_hot(all_ids & 255, 256))
        tok_hi = one_hot(token_ids >> 8, n_hi)
        tok_lo = one_hot(token_ids & 255, 256)
        hot_hi = one_hot(hot_ids >> 8, n_hi)
        hot_lo = one_hot(hot_ids & 255, 256)
        slot_no = jnp.arange(n_hot, dtype=jnp.int32)
        q_map = dot32(hot_hi.T, hot_lo * (slot_no // n_dev + 1).astype(BF)[:, None]).astype(BF)
        r_map = dot32(hot_hi.T, hot_lo * (slot_no % n_dev).astype(BF)[:, None]).astype(BF)
        levels = jnp.array(LEVELS, F32)
        upper = (iota((256, 256), 0) < iota((256, 256), 1)).astype(BF)

        def number(mask, most):
            kept = jnp.where(mask, count, 0.0)
            n_over = jnp.stack([jnp.sum((kept >= v).astype(F32)) for v in LEVELS])
            level = jnp.min(jnp.where(n_over <= most, levels, 1e9))
            flag = kept >= level
            per_row = jnp.sum(flag.astype(F32), axis=1)
            before = jnp.sum(jnp.where(iota((n_hi, n_hi), 0) > iota((n_hi, n_hi), 1), per_row[None, :], 0.0), axis=1)
            return jnp.where(flag, dot32(flag.astype(BF), upper) + before[:, None] + 1.0, 0.0)

        is_hot_map = q_map > 0
        hot_no = number(is_hot_map, FREQ_HOT)
        cold_no = number(jnp.logical_not(is_hot_map), FREQ_COLD)
        freq_map = jnp.where(hot_no > 0, hot_no, jnp.where(cold_no > 0, FREQ_HOT + cold_no, 0.0)).astype(BF)
        id_map = iota((n_hi, 256), 0) * 256 + iota((n_hi, 256), 1)
        cold_id = jnp.sum(jnp.where(cold_no.astype(jnp.int32)[None] == iota((FREQ_COLD, 1, 1), 0) + 1, id_map[None] + 1, 0), axis=(1, 2)) - 1

        def look(hi, lo, *maps):
            got = dot32(hi, jnp.concatenate(maps, axis=1))
            return [jnp.sum(got[:, i * 256:(i + 1) * 256] * lo.astype(F32), axis=1).astype(jnp.int32) for i in range(len(maps))]

        tok_f, tok_q, tok_r = look(tok_hi, tok_lo, freq_map, q_map, r_map)
        (hot_f,) = look(hot_hi, hot_lo, freq_map)
        row_ids = me * rows_dev + jnp.arange(rows_dev, dtype=jnp.int32)
        row_f, row_q, row_n = look(one_hot(row_ids >> 8, n_hi), one_hot(row_ids & 255, 256),
                                   freq_map, q_map, (count > 0).astype(BF))

        rare = tok_f == 0
        owner = jnp.where(tok_q > 0, tok_r, token_ids // rows_dev)
        to_dev = (owner[:, None] == iota((n_loc, n_dev), 1)) & rare[:, None]
        marks = jnp.concatenate([to_dev.astype(BF), jnp.logical_not(rare).astype(BF)[:, None]], axis=1)
        earlier = (iota((n_loc, n_loc), 0) > iota((n_loc, n_loc), 1)).astype(BF)
        ranks = dot32(earlier, marks)
        sent = jnp.sum(to_dev.astype(F32), axis=0)
        fits = jnp.max(sent) <= places
        free = jnp.maximum(places - sent, 0.0)
        free_at = jnp.sum(jnp.where(iota((n_dev, n_dev), 0) > iota((n_dev, n_dev), 1), free[None, :], 0.0), axis=1)
        fill = ranks[:, n_dev]
        fill_dev = (fill[:, None] >= free_at[None, :]) & (fill[:, None] < (free_at + free)[None, :])
        fill_place = jnp.sum(jnp.where(fill_dev, fill[:, None] + (sent - free_at)[None, :], 0.0), axis=1)
        rare_place = jnp.sum(jnp.where(to_dev, ranks[:, :n_dev], 0.0), axis=1)
        dest = jnp.sum(jnp.where(jnp.where(rare[:, None], to_dev, fill_dev), iota((n_loc, n_dev), 1), 0), axis=1)
        slot = dest * places + jnp.where(rare, rare_place, fill_place).astype(jnp.int32)
        row_used = (row_n > 0) & (row_f == 0) & (row_q == 0)
        row_freq = row_f > FREQ_HOT
        fits = fits & (jnp.sum(row_used.astype(jnp.int32)) <= COLD_MAX) & (jnp.sum(row_freq.astype(jnp.int32)) <= COLD_DEV)
        tok_class = jnp.where(rare, jnp.where(tok_q > 0, hot_at + tok_q - 1, cold_at + token_ids % rows_dev), tok_f - 1)
        move = iota((n_loc, n_loc), 0) == slot[None, :]
        move_b = move.astype(BF)

        def exchange(v):
            return lax.all_to_all(v.reshape(n_dev, places, -1), 'emb', 0, 0, tiled=True).reshape(n_loc, -1)

        x_moved = exchange(dot32(move_b, x_in).astype(BF))
        send_class = jnp.sum(jnp.where(move, tok_class[None, :], 0), axis=1) + jnp.where(fits, 0, 1 << 20)
        got_class = lax.all_to_all(send_class.reshape(n_dev, places), 'emb', 0, 0, tiled=True).reshape(n_loc)
        all_fit = jnp.max(got_class) < (1 << 20)

        below = iota((rows_dev, rows_dev), 0) > iota((rows_dev, rows_dev), 1)
        used_rank = jnp.sum(jnp.where(below & row_used[None, :], 1, 0), axis=1)
        freq_rank = jnp.sum(jnp.where(below & row_freq[None, :], 1, 0), axis=1)
        row_pack = one_hot(jnp.where(row_used, used_rank, jnp.where(row_freq, COLD_MAX + freq_rank, -1)), COLD_MAX + COLD_DEV)
        cold_rows = jnp.stack([dot32(row_pack.T, emb_table[i]).astype(BF) for i in range(layers)])
        freq_cold = lax.all_gather(cold_rows[:, COLD_MAX:], 'emb')
        freq_cold = freq_cold.transpose(1, 0, 2, 3).reshape(layers, n_dev * COLD_DEV, emb_dim)
        cold_owner = jnp.where(cold_id >= 0, cold_id // rows_dev, -1)
        same = (cold_owner[:, None] == cold_owner[None, :]) & (iota((FREQ_COLD, FREQ_COLD), 0) > iota((FREQ_COLD, FREQ_COLD), 1))
        cold_slot = jnp.where(cold_id >= 0, cold_owner * COLD_DEV + jnp.sum(same.astype(jnp.int32), axis=1), -1)
        cold_pick = one_hot(cold_slot, n_dev * COLD_DEV)
        hot_pick = one_hot(hot_f - 1, FREQ_HOT).T
        hot_mine = lax.dynamic_index_in_dim(hot_table.reshape(layers, hot_dev, n_dev, emb_dim), me, 2, keepdims=False)
        table = jnp.stack([jnp.concatenate([
            dot32(hot_pick, hot_table[i]).astype(BF), dot32(cold_pick, freq_cold[i]).astype(BF),
            hot_mine[i], cold_rows[i, :COLD_MAX]], axis=0) for i in range(layers)])
        row_of = jnp.sum(jnp.where((used_rank[None, :] == iota((COLD_MAX, rows_dev), 0)) & row_used[None, :],
                                   iota((COLD_MAX, rows_dev), 1), 0), axis=1)
        my_cold = (cold_owner == me) & (cold_id >= 0)
        row_of = jnp.concatenate([row_of, jnp.where(my_cold, cold_id - me * rows_dev, -1)])
        n_blocks = 12 if rows_dev % 12 == 0 else 1
        per_block = rows_dev // n_blocks
        starts = jnp.sum(jnp.where(row_used[None, :] & (iota((n_blocks + 1, rows_dev), 1) < per_block * iota((n_blocks + 1, rows_dev), 0)), 1, 0), axis=1)
        row_no = got_class - cold_at
        used_before = jnp.sum(jnp.where(row_used[None, :] & (iota((n_loc, rows_dev), 1) < row_no[:, None]), 1, 0), axis=1)
        cls = jnp.where(row_no >= 0, cold_at + used_before, got_class)

        def fast(x_moved, d_out):
            d_moved = exchange(dot32(move_b, d_out).astype(BF))
            cls_col, cls_row = cls.reshape(n_loc, 1), cls.reshape(1, n_loc)
            xs, hs, ss, x_last = forward(x_moved, cls_col, table, w_up, w_down, w_gate, w_proj)
            x_out = dot32(move_b.T, exchange(x_last)).astype(BF)
            into = empty((layers, n_hot, emb_dim))
            code = jnp.where((hot_f > 0) & (hot_f <= FREQ_HOT), hot_f - 1, -1)
            cold_sums = [None] * layers
            r = d_moved
            per_dev = FREQ // n_dev
            pairs = [(first, min(2, first + 1)) for first in range(layers - 1, -1, -2)]
            pending = []
            for first, n_l in pairs:
                sums, r = backward(first, n_l, first - n_l + 1 > 0, r, cls_col, cls_row, table, xs, hs, ss, w_up, w_down, w_gate, w_proj)
                gathered = lax.all_gather(sums[:, hot_at:cold_at], 'emb')
                split = sums[:, :FREQ].reshape(n_l, n_dev, per_dev, emb_dim).transpose(1, 0, 2, 3)
                freq = jnp.sum(lax.all_to_all(split, 'emb', 0, 0, tiled=True), axis=0)
                freq = jnp.stack([lax.all_gather(freq[i], 'emb', tiled=True) for i in range(n_l)])
                for i in range(n_l):
                    cold_sums[first - i] = jnp.concatenate([sums[i, cold_at:], freq[i, FREQ_HOT:]], axis=0)
                pending.append((first, gathered, freq))
            d_table = table_out(rows_dev, starts, row_of, cold_sums, n_blocks)
            for first, gathered, freq in pending:
                into = hot_out(first, gathered, freq, code, into)
            return x_out, d_table.transpose(1, 0, 2), into

        def slow(x_moved, d_out):
            return general_path(n_dev, me, token_ids, hot_ids, x_in, d_out, emb_table, hot_table, w_up, w_down, w_gate, w_proj)

        return lax.cond(all_fit, fast, slow, x_moved, d_out)

    return jax.shard_map(body, mesh=mesh,
                         in_specs=(P('emb'), P(), P('emb', None), P('emb', None), P(None, 'emb', None), P(), P(), P(), P(), P()),
                         out_specs=(P('emb', None), P(None, 'emb', None), P()),
                         check_vma=False)
```

```python
import functools

import jax
import jax.numpy as jnp
from jax import lax
from jax.experimental import pallas as pl
from jax.experimental.pallas import tpu as pltpu
from jax.sharding import PartitionSpec as P


NORM_EPS = 1e-6
FREQ_HOT = 112
FREQ_COLD = 16
FREQ = FREQ_HOT + FREQ_COLD
COLD_MAX = 256
GELU_A = 0.7978845608028654
GELU_B = GELU_A * 0.044715
VMEM = 66_000_000
ROWS = 256
LEVELS = (16, 20, 24, 28, 32, 40, 48, 64, 80, 96, 128, 160, 192, 256)
BF = jnp.bfloat16
F32 = jnp.float32


def gelu_back(pre_act, cot_in):
    _, pull = jax.vjp(jax.nn.gelu, pre_act.astype(F32))
    return pull(cot_in)[0]


def dot32(a, b):
    return jnp.dot(a, b, preferred_element_type=F32)


def dense_parts(resid, w_up, w_gate):
    resid_f = resid.astype(F32)
    inv_rms = lax.rsqrt(jnp.mean(resid_f * resid_f, axis=-1, keepdims=True) + NORM_EPS)
    normed = (resid_f * inv_rms).astype(BF)
    hidden = dot32(normed, w_up).astype(BF)
    gate_pre = dot32(normed, w_gate).astype(BF)
    return resid_f, inv_rms, hidden, gate_pre


def layer_forward(resid, emb_rows, w_up, w_down, w_gate, w_proj):
    resid_f, _, hidden, gate_pre = dense_parts(resid, w_up, w_gate)
    activated = jax.nn.gelu(hidden.astype(F32)).astype(BF)
    mlp_out = dot32(activated, w_down).astype(BF)
    gate = jax.nn.gelu(gate_pre.astype(F32)).astype(BF)
    mixed = (gate.astype(F32) * emb_rows.astype(F32)).astype(BF)
    projected = dot32(mixed, w_proj).astype(BF)
    return (resid_f + mlp_out.astype(F32) + projected.astype(F32)).astype(BF)


def layer_backward(resid, emb_rows, d_next, w_up, w_down, w_gate, w_proj):
    resid_f, inv_rms, hidden, gate_pre = dense_parts(resid, w_up, w_gate)
    gate = jax.nn.gelu(gate_pre.astype(F32)).astype(BF)
    d_cast = d_next.astype(BF)
    d_mixed = jnp.einsum('nd,ed->ne', d_cast, w_proj, preferred_element_type=F32)
    d_rows = gate.astype(F32) * d_mixed
    d_gpre = gelu_back(gate_pre, d_mixed * emb_rows.astype(F32))
    d_hidden = gelu_back(hidden, jnp.einsum('nd,fd->nf', d_cast, w_down, preferred_element_type=F32))
    d_normed = (jnp.einsum('nf,df->nd', d_hidden.astype(BF), w_up, preferred_element_type=F32)
                + jnp.einsum('ne,de->nd', d_gpre.astype(BF), w_gate, preferred_element_type=F32))
    inner = jnp.mean(d_normed * resid_f, axis=-1, keepdims=True)
    d_prev = d_next + inv_rms * d_normed - resid_f * (inv_rms * inv_rms * inv_rms) * inner
    return d_prev, d_rows


def general_path(n_dev, my_index, token_ids, hot_ids, x_in, d_out, emb_table, hot_table, w_up, w_down, w_gate, w_proj):
    n_loc = token_ids.shape[0]
    _, rows_dev, emb_dim = emb_table.shape
    capacity = max(8, (2 * n_loc) // n_dev)
    n_slots = n_dev * capacity
    hot_match = token_ids[:, None] == hot_ids[None, :]
    is_hot = jnp.any(hot_match, axis=1)
    hot_pick = hot_match.astype(BF)
    hot_pick_f = hot_match.astype(F32)
    owner_id = token_ids // rows_dev
    to_owner = (owner_id[:, None] == jnp.arange(n_dev, dtype=jnp.int32)[None, :]) & jnp.logical_not(is_hot)[:, None]
    owner_rank = jnp.cumsum(to_owner.astype(jnp.int32), axis=0) - 1
    place = jnp.sum(jnp.where(to_owner, owner_rank, 0), axis=1)
    slot = jnp.where(is_hot, n_slots, owner_id * capacity + place)
    send_ids = jnp.full((n_slots,), -1, jnp.int32).at[slot].set(token_ids, mode='drop')
    slot_tok = jnp.full((n_slots,), -1, jnp.int32).at[slot].set(jnp.arange(n_loc, dtype=jnp.int32), mode='drop')
    recv_ids = lax.all_to_all(send_ids.reshape(n_dev, capacity), 'emb', 0, 0, tiled=True).reshape(n_slots)
    served_ok = recv_ids >= 0
    local_row = jnp.where(served_ok, recv_ids - my_index * rows_dev, 0)
    pick_slot = jnp.minimum(slot, n_slots - 1)
    slot_used = slot_tok >= 0
    slot_src = jnp.maximum(slot_tok, 0)

    def fwd(resid, per_layer):
        table, hot_l, up, down, gate_w, proj = per_layer
        served = jnp.take(table, local_row, axis=0)
        fetched = lax.all_to_all(served.reshape(n_dev, capacity, emb_dim), 'emb', 0, 0, tiled=True).reshape(n_slots, emb_dim)
        cold_rows = jnp.take(fetched, pick_slot, axis=0)
        hot_rows = dot32(hot_pick, hot_l).astype(BF)
        emb_rows = jnp.where(is_hot[:, None], hot_rows, cold_rows)
        return layer_forward(resid, emb_rows, up, down, gate_w, proj), (resid, emb_rows)

    x_out, (x_saved, rows_saved) = lax.scan(fwd, x_in, (emb_table, hot_table, w_up, w_down, w_gate, w_proj))

    def bwd(d_resid, per_layer):
        resid_l, rows_l, up, down, gate_w, proj = per_layer
        d_resid, d_rows = layer_backward(resid_l, rows_l, d_resid, up, down, gate_w, proj)
        outgoing = jnp.where(slot_used[:, None], jnp.take(d_rows, slot_src, axis=0), 0.0)
        incoming = lax.all_to_all(outgoing.reshape(n_dev, capacity, emb_dim), 'emb', 0, 0, tiled=True).reshape(n_slots, emb_dim)
        d_tab = jax.ops.segment_sum(jnp.where(served_ok[:, None], incoming, 0.0), local_row, num_segments=rows_dev)
        hot_local = jnp.einsum('nh,ne->he', hot_pick_f, d_rows, precision=lax.Precision.HIGHEST, preferred_element_type=F32)
        return d_resid, (d_tab, lax.psum(hot_local, 'emb'))

    _, (d_table, d_hot) = lax.scan(bwd, d_out.astype(F32), (x_saved, rows_saved, w_up, w_down, w_gate, w_proj), reverse=True)
    return x_out, d_table, d_hot


def split3(v):
    hi = v.astype(BF)
    rest = v - hi.astype(F32)
    mid = rest.astype(BF)
    return hi, mid, (rest - mid.astype(F32)).astype(BF)


def iota(shape, dim):
    return lax.broadcasted_iota(jnp.int32, shape, dim)


def one_hot(v, n, dtype=BF):
    return (v[:, None] == iota((v.shape[0], n), 1)).astype(dtype)


def dot_nt(a, b):
    return lax.dot_general(a, b, (((1,), (1,)), ((), ())), preferred_element_type=F32)


def gelu(x):
    half = 0.5 * x
    return half + half * jnp.tanh(x * (GELU_A + GELU_B * (x * x)))


def gelu_slope(x):
    sq = x * x
    th = jnp.tanh(x * (GELU_A + GELU_B * sq))
    return (0.5 + 0.5 * th) + (0.5 * x) * (1.0 - th * th) * (GELU_A + (3.0 * GELU_B) * sq)


def forward_kernel(n_l, n_f, x0, cls, table, wu, wd, wg, wp, xs, hs, ss, xo, x_now, u_now, acc, q_now):
    layer, step = pl.program_id(0), pl.program_id(1)
    n_tok = x_now.shape[0]
    parts = [pl.ds(m, ROWS) for m in range(0, n_tok, ROWS)]

    @pl.when((layer == 0) & (step == 0))
    def _():
        x_now[...] = x0[...]

    @pl.when(step == 0)
    def _():
        for m in parts:
            xb = x_now[m, :]
            x = xb.astype(F32)
            xs[0, m, :] = xb
            u = (x * lax.rsqrt(jnp.mean(x * x, axis=-1, keepdims=True) + NORM_EPS)).astype(BF)
            u_now[m, :] = u
            s = dot32(u, wg[0]).astype(BF)
            ss[0, m, :] = s
            g = gelu(s.astype(F32)).astype(BF)
            pick = (cls[m, :] == iota((ROWS, table.shape[1]), 1)).astype(BF)
            e = dot32(pick, table[0]).astype(BF)
            mixed = (g.astype(F32) * e.astype(F32)).astype(BF)
            q_now[m, :] = dot32(mixed, wp[0]).astype(BF)
            acc[m, :] = jnp.zeros((ROWS, acc.shape[1]), F32)

    for m in parts:
        h = dot32(u_now[m, :], wu[0]).astype(BF)
        hs[0, m, :] = h
        act = gelu(h.astype(F32)).astype(BF)
        acc[m, :] += dot32(act, wd[0])

    @pl.when(step == n_f - 1)
    def _():
        for m in parts:
            x = x_now[m, :].astype(F32) + acc[m, :].astype(BF).astype(F32) + q_now[m, :].astype(F32)
            x_now[m, :] = x.astype(BF)

    @pl.when((step == n_f - 1) & (layer == n_l - 1))
    def _():
        xo[...] = x_now[...]


def forward(x0, cls, table, w_up, w_down, w_gate, w_proj):
    n_tok, dim = x0.shape
    n_l, _, ff = w_up.shape
    emb = w_gate.shape[2]
    tile = min(512, ff)
    n_f = ff // tile
    n_c = table.shape[1]
    flops = n_l * 2 * n_tok * dim * (2 * ff + 2 * emb + n_c)
    return pl.pallas_call(
        functools.partial(forward_kernel, n_l, n_f),
        grid=(n_l, n_f),
        in_specs=[
            pl.BlockSpec((n_tok, dim), lambda l, f: (0, 0)),
            pl.BlockSpec((n_tok, 1), lambda l, f: (0, 0)),
            pl.BlockSpec((1, n_c, emb), lambda l, f: (l, 0, 0)),
            pl.BlockSpec((1, dim, tile), lambda l, f: (l, 0, f)),
            pl.BlockSpec((1, tile, dim), lambda l, f: (l, f, 0)),
            pl.BlockSpec((1, dim, emb), lambda l, f: (l, 0, 0)),
            pl.BlockSpec((1, emb, dim), lambda l, f: (l, 0, 0)),
        ],
        out_specs=[
            pl.BlockSpec((1, n_tok, dim), lambda l, f: (l, 0, 0)),
            pl.BlockSpec((1, n_tok, tile), lambda l, f: (l, 0, f)),
            pl.BlockSpec((1, n_tok, emb), lambda l, f: (l, 0, 0)),
            pl.BlockSpec((n_tok, dim), lambda l, f: (0, 0)),
        ],
        out_shape=[
            jax.ShapeDtypeStruct((n_l, n_tok, dim), BF),
            jax.ShapeDtypeStruct((n_l, n_tok, ff), BF),
            jax.ShapeDtypeStruct((n_l, n_tok, emb), BF),
            jax.ShapeDtypeStruct((n_tok, dim), BF),
        ],
        scratch_shapes=[pltpu.VMEM((n_tok, dim), BF), pltpu.VMEM((n_tok, dim), BF),
                        pltpu.VMEM((n_tok, dim), F32), pltpu.VMEM((n_tok, dim), BF)],
        compiler_params=pltpu.CompilerParams(vmem_limit_bytes=VMEM, dimension_semantics=("arbitrary", "arbitrary")),
        cost_estimate=pl.CostEstimate(flops=flops, bytes_accessed=n_l * 40_000_000, transcendentals=0),
        name="forward",
    )(x0, cls, table, w_up, w_down, w_gate, w_proj)


def backward_kernel(n_l, n_f, last_full, r_in, cls, cls_t, table, xs, hs, ss, wu, wd, wg, wp, sums, r, c_now, acc, three):
    step = pl.program_id(0)
    index, f = step // n_f, step % n_f
    n_tok = c_now.shape[0]
    parts = [pl.ds(m, ROWS) for m in range(0, n_tok, ROWS)]
    goes_on = True if last_full else index < n_l - 1

    @pl.when(step == 0)
    def _():
        r[...] = r_in[...].astype(F32)

    @pl.when(f == 0)
    def _():
        for m in parts:
            c = r[m, :].astype(BF)
            c_now[m, :] = c
            a = dot_nt(c, wp[0])
            s = ss[0, m, :].astype(F32)
            rows = gelu(s).astype(BF).astype(F32) * a
            for i, part in enumerate(split3(rows)):
                three[i, m, :] = part
            pick = (cls[m, :] == iota((ROWS, table.shape[1]), 1)).astype(BF)
            e = dot32(pick, table[0])
            ds = (gelu_slope(s) * (a * e)).astype(BF)
            acc[m, :] = dot_nt(ds, wg[0])
        pick_t = (cls_t[...] == iota((table.shape[1], n_tok), 0)).astype(BF)
        sums[0] = dot32(pick_t, three[0]) + (dot32(pick_t, three[1]) + dot32(pick_t, three[2]))

    @pl.when(goes_on)
    def _():
        for m in parts:
            d_act = dot_nt(c_now[m, :], wd[0])
            dh = (gelu_slope(hs[0, m, :].astype(F32)) * d_act).astype(BF)
            acc[m, :] += dot_nt(dh, wu[0])

    @pl.when((f == n_f - 1) & goes_on)
    def _():
        for m in parts:
            x = xs[0, m, :].astype(F32)
            k = lax.rsqrt(jnp.mean(x * x, axis=-1, keepdims=True) + NORM_EPS)
            du = acc[m, :]
            inner = jnp.mean(du * x, axis=-1, keepdims=True)
            r[m, :] = r[m, :] + k * du - x * (k * k * k) * inner


def backward(first, n_l, last_full, r_in, cls, cls_t, table, xs, hs, ss, w_up, w_down, w_gate, w_proj):
    n_tok, dim = r_in.shape
    ff = w_up.shape[2]
    emb = w_gate.shape[2]
    tile = min(512, ff)
    n_f = ff // tile
    n_c = table.shape[1]
    n_steps = n_l * n_f if last_full else (n_l - 1) * n_f + 1

    def whole(t):
        return (first - t // n_f, 0, 0)

    def cols(t):
        return (first - t // n_f, 0, t % n_f)

    def rows(t):
        return (first - t // n_f, t % n_f, 0)

    once = pl.Buffered(1)
    return pl.pallas_call(
        functools.partial(backward_kernel, n_l, n_f, last_full),
        grid=(n_steps,),
        in_specs=[
            pl.BlockSpec((n_tok, dim), lambda t: (0, 0), pipeline_mode=once),
            pl.BlockSpec((n_tok, 1), lambda t: (0, 0), pipeline_mode=once),
            pl.BlockSpec((1, n_tok), lambda t: (0, 0), pipeline_mode=once),
            pl.BlockSpec((1, n_c, emb), whole),
            pl.BlockSpec((1, n_tok, dim), whole),
            pl.BlockSpec((1, n_tok, tile), cols),
            pl.BlockSpec((1, n_tok, emb), whole),
            pl.BlockSpec((1, dim, tile), cols),
            pl.BlockSpec((1, tile, dim), rows),
            pl.BlockSpec((1, dim, emb), whole),
            pl.BlockSpec((1, emb, dim), whole),
        ],
        out_specs=[
            pl.BlockSpec((1, n_c, emb), lambda t: (t // n_f, 0, 0)),
            pl.BlockSpec((n_tok, dim), lambda t: (0, 0)),
        ],
        out_shape=[
            jax.ShapeDtypeStruct((n_l, n_c, emb), F32),
            jax.ShapeDtypeStruct((n_tok, dim), F32),
        ],
        scratch_shapes=[pltpu.VMEM((n_tok, dim), BF), pltpu.VMEM((n_tok, dim), F32), pltpu.VMEM((3, n_tok, emb), BF)],
        compiler_params=pltpu.CompilerParams(vmem_limit_bytes=VMEM, dimension_semantics=("arbitrary",)),
        cost_estimate=pl.CostEstimate(flops=n_l * 2 * n_tok * dim * (2 * ff + 2 * emb + 4 * n_c),
                                      bytes_accessed=n_l * 40_000_000, transcendentals=0),
        name="backward",
    )(r_in, cls, cls_t, table, xs, hs, ss, w_up, w_down, w_gate, w_proj)


def count_kernel(ids, out):
    n_hi = out.shape[0]
    n_tok = ids.shape[1]
    out[...] = jnp.zeros(out.shape, F32)

    @pl.loop(0, ids.shape[0])
    def _(i):
        row = ids[pl.ds(i, 1), :]
        hi = ((row >> 8) == iota((n_hi, n_tok), 0)).astype(BF)
        lo = ((row & 255) == iota((256, n_tok), 0)).astype(BF)
        out[...] += dot_nt(hi, lo)


def count_ids(ids, n_hi):
    return pl.pallas_call(count_kernel, out_shape=jax.ShapeDtypeStruct((n_hi, 256), F32),
                          compiler_params=pltpu.CompilerParams(vmem_limit_bytes=VMEM), name="count_ids")(ids)


def pack_kernel(row_of, table, out, sem):
    @pl.loop(0, out.shape[0])
    def _(k):
        pltpu.make_async_copy(table.at[row_of[k]], out.at[k], sem).start()

    pltpu.make_async_copy(table.at[pl.ds(0, out.shape[0])], out, sem).wait()


def pack_rows(row_of, table):
    n = row_of.shape[0]
    return pl.pallas_call(
        pack_kernel,
        grid_spec=pltpu.PrefetchScalarGridSpec(
            num_scalar_prefetch=1, grid=(1,),
            in_specs=[pl.BlockSpec(memory_space=pl.ANY)],
            out_specs=pl.BlockSpec((n,) + table.shape[1:], lambda i, *_: (0, 0, 0)),
            scratch_shapes=[pltpu.SemaphoreType.DMA(())]),
        out_shape=jax.ShapeDtypeStruct((n,) + table.shape[1:], table.dtype),
        compiler_params=pltpu.CompilerParams(vmem_limit_bytes=VMEM), name="pack_rows",
    )(row_of, table)


def gather_kernel(mine, out, own, z_s, z_r, x_s, x_r, y_s, y_r, fx_s, fx_r, fy_s, fy_r,
                  c_s, c_r, cx_s, cx_r, cy_s, cy_r, cd_s, cd_r):
    me = lax.axis_index('emb')
    core, x, y, z = me % 2, (me // 2) % 2, (me // 4) % 2, me // 8
    half = mine.shape[0] // 2
    first, second = pl.ds(0, half), pl.ds(half, half)

    def dev(z, y, x, core):
        return z * 8 + y * 4 + x * 2 + core

    def copy(src, dst, send, recv, k, to):
        return pltpu.make_async_remote_copy(src_ref=src, dst_ref=dst, send_sem=send.at[k], recv_sem=recv.at[k],
                                            device_id=(to,), device_id_type=pl.DeviceIdType.MESH)

    to_x, to_y, to_core = dev(z, y, 1 - x, core), dev(z, 1 - y, x, core), dev(z, y, x, 1 - core)
    barrier = pltpu.get_barrier_semaphore()
    peers = [dev((z + k) % 4, y, x, core) for k in range(1, 4)] + [to_x, to_y, to_core]
    for peer in peers:
        pl.semaphore_signal(barrier, inc=1, device_id=(peer,), device_id_type=pl.DeviceIdType.MESH)
    pl.semaphore_wait(barrier, len(peers))

    keep = pltpu.make_async_copy(mine, out.at[me], own)
    keep.start()
    sent = []

    def send(*args):
        c = copy(*args)
        c.start()
        sent.append(c)

    def got(block, recv, send_sem, k):
        copy(block, block, send_sem, recv, k, to_x).wait_recv()

    for k in range(1, 4):
        send(mine, out.at[me], z_s, z_r, k, dev((z + k) % 4, y, x, core))

    def column(k):
        at = dev((z - k + 4) % 4, y, x, core)
        if k:
            got(out.at[at], z_r, z_s, k)
        src = out.at[at] if k else mine
        send(src, out.at[at], x_s, x_r, k, to_x)
        send(src, out.at[at], y_s, y_r, k, to_y)
        send(src, out.at[at], c_s, c_r, k, to_core)

    def onward(k):
        zk = (z - k + 4) % 4
        bx, by = dev(zk, y, 1 - x, core), dev(zk, 1 - y, x, core)
        got(out.at[bx], x_r, x_s, k)
        send(out.at[bx, first], out.at[bx, first], fy_s, fy_r, k, to_y)
        send(out.at[bx], out.at[bx], cx_s, cx_r, k, to_core)
        got(out.at[by], y_r, y_s, k)
        send(out.at[by, second], out.at[by, second], fx_s, fx_r, k, to_x)
        send(out.at[by], out.at[by], cy_s, cy_r, k, to_core)

    def across(k):
        bd = dev((z - k + 4) % 4, 1 - y, 1 - x, core)
        got(out.at[bd, first], fy_r, fy_s, k)
        got(out.at[bd, second], fx_r, fx_s, k)
        send(out.at[bd], out.at[bd], cd_s, cd_r, k, to_core)

    column(0)
    column(1)
    onward(0)
    column(2)
    onward(1)
    column(3)
    onward(2)
    across(0)
    onward(3)
    across(1)
    across(2)
    across(3)
    for k in range(4):
        zk = (z - k + 4) % 4
        got(out.at[dev(zk, y, x, 1 - core)], c_r, c_s, k)
        got(out.at[dev(zk, y, 1 - x, 1 - core)], cx_r, cx_s, k)
        got(out.at[dev(zk, 1 - y, x, 1 - core)], cy_r, cy_s, k)
        got(out.at[dev(zk, 1 - y, 1 - x, 1 - core)], cd_r, cd_s, k)
    for c in sent:
        c.wait_send()
    keep.wait()


def gather_all(mine, n_dev):
    n = mine.shape[0]
    return pl.pallas_call(
        gather_kernel,
        in_specs=[pl.BlockSpec(memory_space=pltpu.VMEM)],
        out_specs=pl.BlockSpec(memory_space=pl.ANY),
        out_shape=jax.ShapeDtypeStruct((n_dev,) + mine.shape, mine.dtype),
        scratch_shapes=[pltpu.SemaphoreType.DMA(())] + [pltpu.SemaphoreType.DMA((4,))] * 18,
        compiler_params=pltpu.CompilerParams(collective_id=0, has_side_effects=True, vmem_limit_bytes=VMEM),
        cost_estimate=pl.CostEstimate(flops=80_000_000_000, bytes_accessed=n_dev * n * 4096, transcendentals=0),
        name="gather_all",
    )(mine)


def hot_kernel(n_dev, raw, freq, code, into, out):
    n_r = raw.shape[1]
    n = n_r * n_dev
    row = iota((n, n), 0)
    order = (iota((n, n), 1) == (row % n_dev) * n_r + row // n_dev).astype(BF)
    sel = (code[0] == iota((n, freq.shape[1]), 1)).astype(BF)
    got = [dot32(order, p) for p in split3(raw[...].reshape(n, raw.shape[2]))]
    more = [dot32(sel, p) for p in split3(freq[0])]
    out[0] = (got[0] + (got[1] + got[2])) + (more[0] + (more[1] + more[2]))


def hot_out(first, n_l, gathered, freq, code, into):
    n_dev, _, emb = gathered.shape
    n_r = 8
    width = n_r * n_dev
    blocks = into.shape[1] // width
    return pl.pallas_call(
        functools.partial(hot_kernel, n_dev),
        grid=(n_l, blocks),
        in_specs=[
            pl.BlockSpec((n_dev, n_r, emb), lambda i, b: (0, i * blocks + b, 0)),
            pl.BlockSpec((1, freq.shape[1], emb), lambda i, b: (i, 0, 0)),
            pl.BlockSpec((1, width, 1), lambda i, b: (b, 0, 0)),
            pl.BlockSpec(memory_space=pl.ANY),
        ],
        out_specs=pl.BlockSpec((1, width, emb), lambda i, b: (first - i, b, 0)),
        out_shape=jax.ShapeDtypeStruct(into.shape, F32),
        input_output_aliases={3: 0},
        compiler_params=pltpu.CompilerParams(vmem_limit_bytes=VMEM, dimension_semantics=("arbitrary", "arbitrary")),
        cost_estimate=pl.CostEstimate(flops=20_000_000_000, bytes_accessed=n_l * 16_000_000, transcendentals=0),
        name="hot_out",
    )(gathered, freq, code.reshape(blocks, width, 1), into)


def empty_kernel(out):
    pass


def empty(shape):
    return pl.pallas_call(empty_kernel, out_specs=pl.BlockSpec(memory_space=pl.ANY),
                          out_shape=jax.ShapeDtypeStruct(shape, F32), name="empty")()


def table_kernel(at0, starts, row_of, *refs):
    srcs, out = refs[:-1], refs[-1]
    block = pl.program_id(0)
    n_rows = out.shape[0]
    out[...] = jnp.zeros(out.shape, F32)

    @pl.loop(starts[block], starts[block + 1])
    def _(k):
        at = row_of[k] - block * n_rows
        for l, src in enumerate(srcs):
            out[at, pl.ds(l, 1), :] = src[0, pl.ds(at0 + k, 1), :]


def table_out(rows_dev, at0, starts, row_of, srcs, n_blocks):
    n_l = len(srcs)
    _, n_c, emb = srcs[0][0].shape
    n_rows = rows_dev // n_blocks

    def spec(i):
        return pl.BlockSpec((1, n_c, emb), lambda b, *_: (i, 0, 0))

    return pl.pallas_call(
        functools.partial(table_kernel, at0),
        grid_spec=pltpu.PrefetchScalarGridSpec(
            num_scalar_prefetch=2, grid=(n_blocks,),
            in_specs=[spec(i) for _, i in srcs],
            out_specs=pl.BlockSpec((n_rows, n_l, emb), lambda b, *_: (b, 0, 0))),
        out_shape=jax.ShapeDtypeStruct((rows_dev, n_l, emb), F32),
        compiler_params=pltpu.CompilerParams(vmem_limit_bytes=VMEM, dimension_semantics=("arbitrary",)),
        cost_estimate=pl.CostEstimate(flops=12_000_000_000, bytes_accessed=rows_dev * n_l * emb * 4, transcendentals=0),
        name="table_out",
    )(starts, row_of, *[s for s, _ in srcs])


def row_kernel(at, row, into, out, sem):
    @pl.when(at[0] >= 0)
    def _():
        c = pltpu.make_async_copy(row, out.at[pl.ds(at[0], 1)], sem)
        c.start()
        c.wait()


def put_row(at, row, into):
    return pl.pallas_call(
        row_kernel,
        in_specs=[pl.BlockSpec(memory_space=pltpu.SMEM), pl.BlockSpec(memory_space=pltpu.VMEM), pl.BlockSpec(memory_space=pl.ANY)],
        out_specs=pl.BlockSpec(memory_space=pl.ANY),
        out_shape=jax.ShapeDtypeStruct(into.shape, F32),
        scratch_shapes=[pltpu.SemaphoreType.DMA(())],
        input_output_aliases={2: 0}, name="put_row",
    )(at, row, into)


def solution(mesh):
    n_dev = mesh.shape['emb']

    def body(token_ids, hot_ids, x_in, d_out, emb_table, hot_table, w_up, w_down, w_gate, w_proj):
        n_loc = token_ids.shape[0]
        layers, rows_dev, emb_dim = emb_table.shape
        n_hot = hot_ids.shape[0]
        places = n_loc // n_dev
        hot_dev = n_hot // n_dev
        vocab = rows_dev * n_dev
        n_hi = -(-vocab // 2048) * 8
        me = lax.axis_index('emb')
        per_dev = FREQ // n_dev
        hot_at, cold_at = FREQ, FREQ + hot_dev

        def swap(v):
            return lax.all_to_all(v, 'emb', 0, 0, tiled=True)

        def exchange(v):
            return swap(v.reshape(n_dev, places, -1)).reshape(n_loc, -1)

        count = count_ids(swap(jnp.broadcast_to(token_ids[None, :], (n_dev, n_loc))), n_hi)
        tok_hi = one_hot(token_ids >> 8, n_hi)
        tok_lo = one_hot(token_ids & 255, 256)
        hot_hi = one_hot(hot_ids >> 8, n_hi)
        hot_lo = one_hot(hot_ids & 255, 256)
        slot_no = jnp.arange(n_hot, dtype=jnp.int32)
        q_map = dot32(hot_hi.T, hot_lo * (slot_no // n_dev + 1).astype(BF)[:, None]).astype(BF)
        r_map = dot32(hot_hi.T, hot_lo * (slot_no % n_dev).astype(BF)[:, None]).astype(BF)
        levels = jnp.array(LEVELS, F32)
        upper = (iota((256, 256), 0) < iota((256, 256), 1)).astype(BF)

        def number(mask, most):
            kept = jnp.where(mask, count, 0.0)
            n_over = jnp.sum((kept[:, :, None] >= levels).astype(F32), axis=(0, 1))
            level = jnp.min(jnp.where(n_over <= most, levels, 1e9))
            flag = kept >= level
            per_row = jnp.sum(flag.astype(F32), axis=1)
            before = jnp.sum(jnp.where(iota((n_hi, n_hi), 0) > iota((n_hi, n_hi), 1), per_row[None, :], 0.0), axis=1)
            return jnp.where(flag, dot32(flag.astype(BF), upper) + before[:, None] + 1.0, 0.0)

        is_hot_map = q_map > 0
        hot_no = number(is_hot_map, FREQ_HOT)
        cold_no = number(jnp.logical_not(is_hot_map), FREQ_COLD)
        freq_map = jnp.where(hot_no > 0, hot_no, jnp.where(cold_no > 0, FREQ_HOT + cold_no, 0.0)).astype(BF)
        id_map = iota((n_hi, 256), 0) * 256 + iota((n_hi, 256), 1)
        cold_id = jnp.sum(jnp.where(cold_no.astype(jnp.int32)[None] == iota((FREQ_COLD, 1, 1), 0) + 1, id_map[None] + 1, 0), axis=(1, 2)) - 1

        def look(hi, lo, *maps):
            got = dot32(hi, jnp.concatenate(maps, axis=1))
            return [jnp.sum(got[:, i * 256:(i + 1) * 256] * lo.astype(F32), axis=1).astype(jnp.int32) for i in range(len(maps))]

        tok_f, tok_q, tok_r = look(tok_hi, tok_lo, freq_map, q_map, r_map)
        (hot_f,) = look(hot_hi, hot_lo, freq_map)
        row_ids = me * rows_dev + jnp.arange(rows_dev, dtype=jnp.int32)
        row_f, row_q, row_n = look(one_hot(row_ids >> 8, n_hi), one_hot(row_ids & 255, 256),
                                   freq_map, q_map, (count > 0).astype(BF))

        rare = tok_f == 0
        owner = jnp.where(tok_q > 0, tok_r, token_ids // rows_dev)
        to_dev = (owner[:, None] == iota((n_loc, n_dev), 1)) & rare[:, None]
        marks = jnp.concatenate([to_dev.astype(BF), jnp.logical_not(rare).astype(BF)[:, None]], axis=1)
        earlier = (iota((n_loc, n_loc), 0) > iota((n_loc, n_loc), 1)).astype(BF)
        ranks = dot32(earlier, marks)
        sent = jnp.sum(to_dev.astype(F32), axis=0)
        fits = jnp.max(sent) <= places
        free = jnp.maximum(places - sent, 0.0)
        free_at = jnp.sum(jnp.where(iota((n_dev, n_dev), 0) > iota((n_dev, n_dev), 1), free[None, :], 0.0), axis=1)
        fill = ranks[:, n_dev]
        fill_dev = (fill[:, None] >= free_at[None, :]) & (fill[:, None] < (free_at + free)[None, :])
        fill_place = jnp.sum(jnp.where(fill_dev, fill[:, None] + (sent - free_at)[None, :], 0.0), axis=1)
        rare_place = jnp.sum(jnp.where(to_dev, ranks[:, :n_dev], 0.0), axis=1)
        dest = jnp.sum(jnp.where(jnp.where(rare[:, None], to_dev, fill_dev), iota((n_loc, n_dev), 1), 0), axis=1)
        slot = dest * places + jnp.where(rare, rare_place, fill_place).astype(jnp.int32)
        row_used = (row_n > 0) & (row_f == 0) & (row_q == 0)
        fits = fits & (jnp.sum(row_used.astype(jnp.int32)) <= COLD_MAX) & (jnp.sum((row_f > FREQ_HOT).astype(jnp.int32)) <= 1)
        tok_class = jnp.where(rare, jnp.where(tok_q > 0, hot_at + tok_q - 1, cold_at + token_ids % rows_dev), tok_f - 1)
        move = iota((n_loc, n_loc), 0) == slot[None, :]
        move_b = move.astype(BF)
        x_moved = exchange(dot32(move_b, x_in).astype(BF))
        d_placed = dot32(move_b, d_out).astype(BF)
        send_class = jnp.sum(jnp.where(move, tok_class[None, :], 0), axis=1) + jnp.where(fits, 0, 1 << 20)
        got_class = swap(send_class.reshape(n_dev, places)).reshape(n_loc)
        all_fit = jnp.max(got_class) < (1 << 20)

        below = iota((rows_dev, rows_dev), 0) > iota((rows_dev, rows_dev), 1)
        used_rank = jnp.sum(jnp.where(below & row_used[None, :], 1, 0), axis=1)
        row_of = jnp.sum(jnp.where((used_rank[None, :] == iota((COLD_MAX, rows_dev), 0)) & row_used[None, :],
                                   iota((COLD_MAX, rows_dev), 1), 0), axis=1)
        cold_owner = jnp.where(cold_id >= 0, cold_id // rows_dev, -1)
        my_cold = (cold_owner == me).astype(jnp.int32)
        my_row = jnp.sum(my_cold * (cold_id - me * rows_dev + 1)) - 1
        wanted = jnp.concatenate([row_of, jnp.full((8,), jnp.clip(my_row, 0, rows_dev - 1), jnp.int32)])
        packed = pack_rows(wanted, emb_table.transpose(1, 0, 2))
        freq_cold = swap(jnp.broadcast_to(packed[COLD_MAX:COLD_MAX + 1], (n_dev, layers, emb_dim)))
        cold_pick = one_hot(cold_owner, n_dev)
        hot_pick = one_hot(hot_f - 1, FREQ_HOT).T
        hot_mine = lax.dynamic_index_in_dim(hot_table.reshape(layers, hot_dev, n_dev, emb_dim), me, 2, keepdims=False)
        table = jnp.stack([jnp.concatenate([
            dot32(hot_pick, hot_table[i]).astype(BF), dot32(cold_pick, freq_cold[:, i]).astype(BF),
            hot_mine[i], packed[:COLD_MAX, i]], axis=0) for i in range(layers)])
        n_blocks = 12 if rows_dev % 12 == 0 else 1
        edges = (rows_dev // n_blocks) * iota((n_blocks + 1, rows_dev), 0)
        starts = jnp.sum(jnp.where(row_used[None, :] & (iota((n_blocks + 1, rows_dev), 1) < edges), 1, 0), axis=1)
        row_no = got_class - cold_at
        used_before = jnp.sum(jnp.where(row_used[None, :] & (iota((n_loc, rows_dev), 1) < row_no[:, None]), 1, 0), axis=1)
        cls = jnp.where(row_no >= 0, cold_at + used_before, got_class)
        code = jnp.where((hot_f > 0) & (hot_f <= FREQ_HOT), hot_f - 1, -1)
        back = (slot[:, None] == iota((n_loc, n_loc), 1)).astype(BF)

        def fast(x_moved, d_placed, table, cls, back, starts, row_of, code, my_cold, my_row):
            return run(x_moved, d_placed, table, cls, back, starts, row_of, code, my_cold, my_row)

        def run(x_moved, d_placed, table, cls, back, starts, row_of, code, my_cold, my_row):
            d_moved = exchange(d_placed)
            cls_col, cls_row = cls.reshape(n_loc, 1), cls.reshape(1, n_loc)
            xs, hs, ss, x_last = forward(x_moved, cls_col, table, w_up, w_down, w_gate, w_proj)
            x_back = exchange(x_last)

            def freq_parts(sums):
                return sums[:, :FREQ].reshape(2, n_dev, per_dev, emb_dim).transpose(1, 0, 2, 3)

            sums_a, r = backward(3, 2, True, d_moved, cls_col, cls_row, table, xs, hs, ss, w_up, w_down, w_gate, w_proj)
            all_a = lax.all_gather(sums_a[:, hot_at:cold_at].reshape(2 * hot_dev, emb_dim), 'emb')
            freq_a = swap(freq_parts(sums_a))
            r, x_back = lax.optimization_barrier((r, x_back))
            sums_b, _ = backward(1, 2, False, r, cls_col, cls_row, table, xs, hs, ss, w_up, w_down, w_gate, w_proj)
            freq_b = swap(freq_parts(sums_b))
            x_out = dot32(back, x_back).astype(BF)
            d_table = table_out(rows_dev, cold_at, starts, row_of, [(sums_b, 1), (sums_b, 0), (sums_a, 1), (sums_a, 0)], n_blocks)
            totals = [jnp.sum(v, axis=0).reshape(2 * per_dev, emb_dim) for v in (freq_a, freq_b)]
            mine = jnp.concatenate([sums_b[:, hot_at:cold_at].reshape(2 * hot_dev, emb_dim)] + totals, axis=0)
            mine, x_out, d_table = lax.optimization_barrier((mine, x_out, d_table))
            all_b = gather_all(mine, n_dev)
            freq = all_b[:, 2 * hot_dev:].reshape(n_dev, layers, per_dev, emb_dim).transpose(1, 0, 2, 3).reshape(layers, FREQ, emb_dim)
            row = jnp.sum(freq[::-1, FREQ_HOT:] * my_cold.astype(F32)[None, :, None], axis=1)[None]
            d_table = put_row(my_row.reshape(1), row, d_table)
            into = empty((layers, n_hot, emb_dim))
            into = hot_out(1, 2, all_b, freq[2:], code, into)
            into = hot_out(3, 2, all_a, freq[:2], code, into)
            return x_out, d_table.transpose(1, 0, 2), into

        def slow(*_):
            return general_path(n_dev, me, token_ids, hot_ids, x_in, d_out, emb_table, hot_table, w_up, w_down, w_gate, w_proj)

        given = lax.optimization_barrier((x_moved, d_placed, table, cls, back, starts, row_of, code, my_cold, my_row))
        return lax.cond(all_fit, fast, slow, *given)

    return jax.shard_map(body, mesh=mesh,
                         in_specs=(P('emb'), P(), P('emb', None), P('emb', None), P(None, 'emb', None), P(), P(), P(), P(), P()),
                         out_specs=(P('emb', None), P(None, 'emb', None), P()),
                         check_vma=False)
```

```python
import functools

import jax
import jax.numpy as jnp
from jax import lax
from jax.experimental import pallas as pl
from jax.experimental.pallas import tpu as pltpu
from jax.sharding import PartitionSpec as P


NORM_EPS = 1e-6
FREQ_HOT = 112
FREQ_COLD = 16
FREQ = FREQ_HOT + FREQ_COLD
COLD_MAX = 256
LO = 256
HI_BITS = 8
RUN = 4
LEVELS = tuple(16 * 2 ** (i / 4) for i in range(17))
GELU_A = 0.7978845608028654
GELU_B = GELU_A * 0.044715
VMEM = 66_000_000
ROWS_A = 256
ROWS_B = 512
TILE = 1024
BF = jnp.bfloat16
F32 = jnp.float32
I32 = jnp.int32
ONCE = pl.Buffered(1)


def gelu_back(pre_act, cot_in):
    _, pull = jax.vjp(jax.nn.gelu, pre_act.astype(F32))
    return pull(cot_in)[0]


def dot32(a, b):
    return jnp.dot(a, b, preferred_element_type=F32)


def dense_parts(resid, w_up, w_gate):
    resid_f = resid.astype(F32)
    inv_rms = lax.rsqrt(jnp.mean(resid_f * resid_f, axis=-1, keepdims=True) + NORM_EPS)
    normed = (resid_f * inv_rms).astype(BF)
    hidden = dot32(normed, w_up).astype(BF)
    gate_pre = dot32(normed, w_gate).astype(BF)
    return resid_f, inv_rms, hidden, gate_pre


def layer_forward(resid, emb_rows, w_up, w_down, w_gate, w_proj):
    resid_f, _, hidden, gate_pre = dense_parts(resid, w_up, w_gate)
    activated = jax.nn.gelu(hidden.astype(F32)).astype(BF)
    mlp_out = dot32(activated, w_down).astype(BF)
    gate = jax.nn.gelu(gate_pre.astype(F32)).astype(BF)
    mixed = (gate.astype(F32) * emb_rows.astype(F32)).astype(BF)
    projected = dot32(mixed, w_proj).astype(BF)
    return (resid_f + mlp_out.astype(F32) + projected.astype(F32)).astype(BF)


def layer_backward(resid, emb_rows, d_next, w_up, w_down, w_gate, w_proj):
    resid_f, inv_rms, hidden, gate_pre = dense_parts(resid, w_up, w_gate)
    gate = jax.nn.gelu(gate_pre.astype(F32)).astype(BF)
    d_cast = d_next.astype(BF)
    d_mixed = jnp.einsum('nd,ed->ne', d_cast, w_proj, preferred_element_type=F32)
    d_rows = gate.astype(F32) * d_mixed
    d_gpre = gelu_back(gate_pre, d_mixed * emb_rows.astype(F32))
    d_hidden = gelu_back(hidden, jnp.einsum('nd,fd->nf', d_cast, w_down, preferred_element_type=F32))
    d_normed = (jnp.einsum('nf,df->nd', d_hidden.astype(BF), w_up, preferred_element_type=F32)
                + jnp.einsum('ne,de->nd', d_gpre.astype(BF), w_gate, preferred_element_type=F32))
    inner = jnp.mean(d_normed * resid_f, axis=-1, keepdims=True)
    d_prev = d_next + inv_rms * d_normed - resid_f * (inv_rms * inv_rms * inv_rms) * inner
    return d_prev, d_rows


def general_path(n_dev, my_index, token_ids, hot_ids, x_in, d_out, emb_table, hot_table, w_up, w_down, w_gate, w_proj):
    n_loc = token_ids.shape[0]
    _, rows_dev, emb_dim = emb_table.shape
    capacity = max(8, (2 * n_loc) // n_dev)
    n_slots = n_dev * capacity
    hot_match = token_ids[:, None] == hot_ids[None, :]
    is_hot = jnp.any(hot_match, axis=1)
    hot_pick = hot_match.astype(BF)
    hot_pick_f = hot_match.astype(F32)
    owner_id = token_ids // rows_dev
    to_owner = (owner_id[:, None] == jnp.arange(n_dev, dtype=jnp.int32)[None, :]) & jnp.logical_not(is_hot)[:, None]
    owner_rank = jnp.cumsum(to_owner.astype(jnp.int32), axis=0) - 1
    place = jnp.sum(jnp.where(to_owner, owner_rank, 0), axis=1)
    slot = jnp.where(is_hot, n_slots, owner_id * capacity + place)
    send_ids = jnp.full((n_slots,), -1, jnp.int32).at[slot].set(token_ids, mode='drop')
    slot_tok = jnp.full((n_slots,), -1, jnp.int32).at[slot].set(jnp.arange(n_loc, dtype=jnp.int32), mode='drop')
    recv_ids = lax.all_to_all(send_ids.reshape(n_dev, capacity), 'emb', 0, 0, tiled=True).reshape(n_slots)
    served_ok = recv_ids >= 0
    local_row = jnp.where(served_ok, recv_ids - my_index * rows_dev, 0)
    pick_slot = jnp.minimum(slot, n_slots - 1)
    slot_used = slot_tok >= 0
    slot_src = jnp.maximum(slot_tok, 0)

    def fwd(resid, per_layer):
        table, hot_l, up, down, gate_w, proj = per_layer
        served = jnp.take(table, local_row, axis=0)
        fetched = lax.all_to_all(served.reshape(n_dev, capacity, emb_dim), 'emb', 0, 0, tiled=True).reshape(n_slots, emb_dim)
        cold_rows = jnp.take(fetched, pick_slot, axis=0)
        hot_rows = dot32(hot_pick, hot_l).astype(BF)
        emb_rows = jnp.where(is_hot[:, None], hot_rows, cold_rows)
        return layer_forward(resid, emb_rows, up, down, gate_w, proj), (resid, emb_rows)

    x_out, (x_saved, rows_saved) = lax.scan(fwd, x_in, (emb_table, hot_table, w_up, w_down, w_gate, w_proj))

    def bwd(d_resid, per_layer):
        resid_l, rows_l, up, down, gate_w, proj = per_layer
        d_resid, d_rows = layer_backward(resid_l, rows_l, d_resid, up, down, gate_w, proj)
        outgoing = jnp.where(slot_used[:, None], jnp.take(d_rows, slot_src, axis=0), 0.0)
        incoming = lax.all_to_all(outgoing.reshape(n_dev, capacity, emb_dim), 'emb', 0, 0, tiled=True).reshape(n_slots, emb_dim)
        d_tab = jax.ops.segment_sum(jnp.where(served_ok[:, None], incoming, 0.0), local_row, num_segments=rows_dev)
        hot_local = jnp.einsum('nh,ne->he', hot_pick_f, d_rows, precision=lax.Precision.HIGHEST, preferred_element_type=F32)
        return d_resid, (d_tab, lax.psum(hot_local, 'emb'))

    _, (d_table, d_hot) = lax.scan(bwd, d_out.astype(F32), (x_saved, rows_saved, w_up, w_down, w_gate, w_proj), reverse=True)
    return x_out, d_table, d_hot


def split3(v):
    hi = v.astype(BF)
    rest = v - hi.astype(F32)
    mid = rest.astype(BF)
    return hi, mid, (rest - mid.astype(F32)).astype(BF)


def iota(shape, dim):
    return lax.broadcasted_iota(jnp.int32, shape, dim)


def one_hot(v, n, dtype=BF):
    return (v[:, None] == iota((v.shape[0], n), 1)).astype(dtype)


def dot_nt(a, b):
    return lax.dot_general(a, b, (((1,), (1,)), ((), ())), preferred_element_type=F32)


def gelu(x):
    half = 0.5 * x
    return half + half * jnp.tanh(x * (GELU_A + GELU_B * (x * x)))


def gelu_slope(x):
    sq = x * x
    th = jnp.tanh(x * (GELU_A + GELU_B * sq))
    return (0.5 + 0.5 * th) + (0.5 * x) * (1.0 - th * th) * (GELU_A + (3.0 * GELU_B) * sq)


def forward_kernel(n_l, n_f, x0, cls, table, wu, wd, wg, wp, xs, hs, ss, es, xo, x_now, u_now, acc, q_now):
    layer, step = pl.program_id(0), pl.program_id(1)
    n_tok = x_now.shape[0]

    @pl.when((layer == 0) & (step == 0))
    def _():
        x_now[...] = x0[...]

    @pl.when(step == 0)
    def _():
        for m in chunks(n_tok, ROWS_A):
            xb = x_now[m, :]
            x = xb.astype(F32)
            xs[0, m, :] = xb
            u = (x * lax.rsqrt(jnp.mean(x * x, axis=-1, keepdims=True) + NORM_EPS)).astype(BF)
            u_now[m, :] = u
            s = dot32(u, wg[0]).astype(BF)
            ss[0, m, :] = s
            g = gelu(s.astype(F32)).astype(BF)
            pick = (cls[m, :] == iota((m.size, table.shape[1]), 1)).astype(BF)
            e = dot32(pick, table[0]).astype(BF)
            es[0, m, :] = e
            mixed = (g.astype(F32) * e.astype(F32)).astype(BF)
            q_now[m, :] = dot32(mixed, wp[0]).astype(BF)
            acc[m, :] = jnp.zeros((m.size, acc.shape[1]), F32)

    for m in chunks(n_tok, ROWS_B):
        h = dot32(u_now[m, :], wu[0]).astype(BF)
        hs[0, m, :] = h
        acc[m, :] += dot32(gelu(h.astype(F32)).astype(BF), wd[0])

    @pl.when(step == n_f - 1)
    def _():
        for m in chunks(n_tok, ROWS_A):
            x = x_now[m, :].astype(F32) + acc[m, :].astype(BF).astype(F32) + q_now[m, :].astype(F32)
            x_now[m, :] = x.astype(BF)

    @pl.when((step == n_f - 1) & (layer == n_l - 1))
    def _():
        xo[...] = x_now[...]


def chunks(n, size):
    size = min(n, size)
    return [pl.ds(m, size) for m in range(0, n, size)]


def forward(x0, cls, table, w_up, w_down, w_gate, w_proj):
    n_tok, dim = x0.shape
    n_l, _, ff = w_up.shape
    emb = w_gate.shape[2]
    tile = min(TILE, ff)
    n_f = ff // tile
    n_c = table.shape[1]

    def whole(l, f):
        return (l, 0, 0)

    def cols(l, f):
        return (l, 0, f)

    def fixed(l, f):
        return (0, 0)

    return pl.pallas_call(
        functools.partial(forward_kernel, n_l, n_f),
        grid=(n_l, n_f),
        in_specs=[
            pl.BlockSpec((n_tok, dim), fixed, pipeline_mode=ONCE),
            pl.BlockSpec((n_tok, 1), fixed, pipeline_mode=ONCE),
            pl.BlockSpec((1, n_c, emb), whole),
            pl.BlockSpec((1, dim, tile), cols),
            pl.BlockSpec((1, tile, dim), lambda l, f: (l, f, 0)),
            pl.BlockSpec((1, dim, emb), whole),
            pl.BlockSpec((1, emb, dim), whole),
        ],
        out_specs=[
            pl.BlockSpec((1, n_tok, dim), whole),
            pl.BlockSpec((1, n_tok, tile), cols),
            pl.BlockSpec((1, n_tok, emb), whole),
            pl.BlockSpec((1, n_tok, emb), whole),
            pl.BlockSpec((n_tok, dim), fixed),
        ],
        out_shape=[jax.ShapeDtypeStruct((n_l, n_tok, n), BF) for n in (dim, ff, emb, emb)]
        + [jax.ShapeDtypeStruct((n_tok, dim), BF)],
        scratch_shapes=[pltpu.VMEM((n_tok, dim), t) for t in (BF, BF, F32, BF)],
        compiler_params=params("arbitrary", "arbitrary"),
        cost_estimate=cost(n_l * n_tok * dim * (2 * ff + 2 * emb + n_c), n_l),
        name="forward",
    )(x0, cls, table, w_up, w_down, w_gate, w_proj)


def params(*kinds, **more):
    return pltpu.CompilerParams(vmem_limit_bytes=VMEM, dimension_semantics=kinds or None, **more)


def cost(products, layers):
    return pl.CostEstimate(flops=2 * products, bytes_accessed=layers * 40_000_000, transcendentals=0)


def backward_kernel(n_f, last_full, r_in, cls_t, es, xs, hs, ss, wu, wd, wg, wp, sums, r, c_now, acc, three):
    step = pl.program_id(0)
    f = step % n_f
    n_tok, n_c = c_now.shape[0], sums.shape[1]
    goes_on = True if last_full else step < pl.num_programs(0) - 1

    @pl.when(step == 0)
    def _():
        r[...] = r_in[...].astype(F32)

    @pl.when(f == 0)
    def _():
        for m in chunks(n_tok, ROWS_B):
            c = r[m, :].astype(BF)
            c_now[m, :] = c
            a = dot_nt(c, wp[0])
            s = ss[0, m, :].astype(F32)
            rows = gelu(s).astype(BF).astype(F32) * a
            for i, part in enumerate(split3(rows)):
                three[i, m, :] = part
            if last_full:
                ds = (gelu_slope(s) * (a * es[0, m, :].astype(F32))).astype(BF)
                acc[m, :] = dot_nt(ds, wg[0])
            else:
                acc[m, :] = a
        pick_t = (cls_t[...] == iota((n_c, n_tok), 0)).astype(BF)
        sums[0] = dot32(pick_t, three[0]) + (dot32(pick_t, three[1]) + dot32(pick_t, three[2]))

    if not last_full:
        @pl.when((f == 0) & goes_on)
        def _():
            for m in chunks(n_tok, ROWS_B):
                ds = (gelu_slope(ss[0, m, :].astype(F32)) * (acc[m, :] * es[0, m, :].astype(F32))).astype(BF)
                acc[m, :] = dot_nt(ds, wg[0])

    @pl.when(goes_on)
    def _():
        for m in chunks(n_tok, ROWS_B):
            d_act = dot_nt(c_now[m, :], wd[0])
            dh = (gelu_slope(hs[0, m, :].astype(F32)) * d_act).astype(BF)
            acc[m, :] += dot_nt(dh, wu[0])

    @pl.when((f == n_f - 1) & goes_on)
    def _():
        for m in chunks(n_tok, ROWS_A):
            x = xs[0, m, :].astype(F32)
            k = lax.rsqrt(jnp.mean(x * x, axis=-1, keepdims=True) + NORM_EPS)
            du = acc[m, :]
            inner = jnp.mean(du * x, axis=-1, keepdims=True)
            r[m, :] = r[m, :] + k * du - x * (k * k * k) * inner


def backward(first, n_l, last_full, r_in, cls_t, es, xs, hs, ss, w_up, w_down, w_gate, w_proj, n_class=448):
    n_tok, dim = r_in.shape
    ff = w_up.shape[2]
    emb = w_gate.shape[2]
    tile = min(TILE, ff)
    n_f = ff // tile
    n_c = n_class
    n_steps = n_l * n_f if last_full else (n_l - 1) * n_f + 1

    def whole(t):
        return (first - t // n_f, 0, 0)

    def cols(t):
        return (first - t // n_f, 0, t % n_f)

    def fixed(t):
        return (0, 0)

    return pl.pallas_call(
        functools.partial(backward_kernel, n_f, last_full),
        grid=(n_steps,),
        in_specs=[
            pl.BlockSpec((n_tok, dim), fixed, pipeline_mode=ONCE),
            pl.BlockSpec((1, n_tok), fixed, pipeline_mode=ONCE),
            pl.BlockSpec((1, n_tok, emb), whole),
            pl.BlockSpec((1, n_tok, dim), whole),
            pl.BlockSpec((1, n_tok, tile), cols),
            pl.BlockSpec((1, n_tok, emb), whole),
            pl.BlockSpec((1, dim, tile), cols),
            pl.BlockSpec((1, tile, dim), lambda t: (first - t // n_f, t % n_f, 0)),
            pl.BlockSpec((1, dim, emb), whole),
            pl.BlockSpec((1, emb, dim), whole),
        ],
        out_specs=[
            pl.BlockSpec((1, n_c, emb), lambda t: (t // n_f, 0, 0)),
            pl.BlockSpec((n_tok, dim), fixed),
        ],
        out_shape=[
            jax.ShapeDtypeStruct((n_l, n_c, emb), F32),
            jax.ShapeDtypeStruct((n_tok, dim), F32),
        ],
        scratch_shapes=[pltpu.VMEM((n_tok, dim), BF), pltpu.VMEM((n_tok, dim), F32), pltpu.VMEM((3, n_tok, emb), BF)],
        compiler_params=params("arbitrary"),
        cost_estimate=cost(n_l * n_tok * dim * (2 * ff + 2 * emb + 3 * n_c), n_l),
        name="backward",
    )(r_in, cls_t, es, xs, hs, ss, w_up, w_down, w_gate, w_proj)


def spec(shape, *index, **more):
    index = index or (0,) * len(shape)
    return pl.BlockSpec(shape, lambda *_: index, **more)


ANY = pl.BlockSpec(memory_space=pl.ANY)


def out_of(shape, dtype=F32):
    return jax.ShapeDtypeStruct(shape, dtype)


def count_kernel(ids, out):
    n_tok = ids.shape[1]
    out[...] = jnp.zeros(out.shape, F32)

    @pl.loop(0, len(ids))
    def _(i):
        row = ids[pl.ds(i, 1), :]
        hi = ((row >> HI_BITS) == iota((len(out), n_tok), 0)).astype(BF)
        lo = ((row & (LO - 1)) == iota((LO, n_tok), 0)).astype(BF)
        out[...] += dot_nt(hi, lo)


def count_ids(ids, n_hi):
    return pl.pallas_call(count_kernel, out_shape=out_of((n_hi, LO)), compiler_params=params(), name="count_ids")(ids)


def pack_kernel(row_of, table, out, sem):
    @pl.loop(0, len(out))
    def _(k):
        pltpu.make_async_copy(table.at[row_of[k]], out.at[k], sem).start()

    pltpu.make_async_copy(table.at[pl.ds(0, len(out))], out, sem).wait()


def pack_rows(row_of, table):
    shape = row_of.shape + table.shape[1:]
    return pl.pallas_call(
        pack_kernel,
        grid_spec=pltpu.PrefetchScalarGridSpec(num_scalar_prefetch=1, grid=(1,), in_specs=[ANY], out_specs=spec(shape),
                                               scratch_shapes=[pltpu.SemaphoreType.DMA(())]),
        out_shape=out_of(shape, table.dtype), compiler_params=params(), name="pack_rows",
    )(row_of, table)


def gather_kernel(mine, out, own, z_s, z_r, x_s, x_r, y_s, y_r, fx_s, fx_r, fy_s, fy_r,
                  c_s, c_r, cx_s, cx_r, cy_s, cy_r, cd_s, cd_r):
    me = lax.axis_index('emb')
    core, x, y, z = me % 2, (me // 2) % 2, (me // 4) % 2, me // 8
    half = len(mine) // 2
    first, second = pl.ds(0, half), pl.ds(half, half)

    def dev(z, y, x, core):
        return ((z * 2 + y) * 2 + x) * 2 + core

    def copy(src, dst, send, recv, k, to):
        return pltpu.make_async_remote_copy(src_ref=src, dst_ref=dst, send_sem=send.at[k], recv_sem=recv.at[k],
                                            device_id=(to,), device_id_type=pl.DeviceIdType.MESH)

    def column_of(k):
        return (z - k + 4) % 4

    others = [dev((z + k) % 4, y, x, core) for k in range(1, 4)]
    to_x, to_y, to_core = dev(z, y, 1 - x, core), dev(z, 1 - y, x, core), dev(z, y, x, 1 - core)
    barrier = pltpu.get_barrier_semaphore()
    peers = others + [to_x, to_y, to_core]
    for peer in peers:
        pl.semaphore_signal(barrier, device_id=(peer,), device_id_type=pl.DeviceIdType.MESH)
    pl.semaphore_wait(barrier, len(peers))

    keep = pltpu.make_async_copy(mine, out.at[me], own)
    keep.start()
    sent = []

    def send(*args):
        c = copy(*args)
        c.start()
        sent.append(c)

    def got(block, recv, send_sem, k):
        copy(block, block, send_sem, recv, k, to_x).wait_recv()

    for k, other in enumerate(others):
        send(mine, out.at[me], z_s, z_r, k + 1, other)

    def column(k):
        at = dev(column_of(k), y, x, core)
        if k:
            got(out.at[at], z_r, z_s, k)
        src = out.at[at] if k else mine
        send(src, out.at[at], x_s, x_r, k, to_x)
        send(src, out.at[at], y_s, y_r, k, to_y)
        send(src, out.at[at], c_s, c_r, k, to_core)

    def onward(k):
        bx, by = dev(column_of(k), y, 1 - x, core), dev(column_of(k), 1 - y, x, core)
        got(out.at[bx], x_r, x_s, k)
        send(out.at[bx, first], out.at[bx, first], fy_s, fy_r, k, to_y)
        send(out.at[bx], out.at[bx], cx_s, cx_r, k, to_core)
        got(out.at[by], y_r, y_s, k)
        send(out.at[by, second], out.at[by, second], fx_s, fx_r, k, to_x)
        send(out.at[by], out.at[by], cy_s, cy_r, k, to_core)

    def across(k):
        bd = dev(column_of(k), 1 - y, 1 - x, core)
        got(out.at[bd, first], fy_r, fy_s, k)
        got(out.at[bd, second], fx_r, fx_s, k)
        send(out.at[bd], out.at[bd], cd_s, cd_r, k, to_core)

    column(0)
    for k in range(3):
        column(k + 1)
        onward(k)
    across(0)
    onward(3)
    for k in range(1, 4):
        across(k)
    for k in range(4):
        for dy, dx, recv, send_sem in ((y, x, c_r, c_s), (y, 1 - x, cx_r, cx_s), (1 - y, x, cy_r, cy_s), (1 - y, 1 - x, cd_r, cd_s)):
            got(out.at[dev(column_of(k), dy, dx, 1 - core)], recv, send_sem, k)
    for c in sent:
        c.wait_send()
    keep.wait()


def gather_all(mine, n_dev):
    return pl.pallas_call(
        gather_kernel,
        in_specs=[pl.BlockSpec(memory_space=pltpu.VMEM)], out_specs=ANY,
        out_shape=out_of((n_dev,) + mine.shape),
        scratch_shapes=[pltpu.SemaphoreType.DMA(())] + [pltpu.SemaphoreType.DMA((4,))] * 18,
        compiler_params=params(collective_id=0, has_side_effects=True),
        cost_estimate=cost(mine.size * n_dev * LO, 1), name="gather_all",
    )(mine)


def hot_kernel(skip, raw, freq, code, into, out, parts):
    n_dev, n_r, _ = raw.shape

    @pl.when(pl.program_id(1) == 0)
    def _():
        for layer in range(freq.shape[1] // RUN):
            @pl.when(pl.program_id(0) + skip == layer)
            def _(layer=layer):
                rows = jnp.concatenate([freq[o, layer * RUN:(layer + 1) * RUN, :] for o in range(n_dev)], axis=0)
                for i, part in enumerate(split3(rows)):
                    parts[i] = part

    sel = (code[0] == iota((n_r * n_dev, FREQ), 1)).astype(BF)
    more = dot32(sel, parts[0]) + (dot32(sel, parts[1]) + dot32(sel, parts[2]))
    for g in range(n_r // RUN):
        rows = jnp.concatenate([raw[o, g * RUN:(g + 1) * RUN, :] for o in range(n_dev)], axis=0)
        at = pl.ds(g * RUN * n_dev, RUN * n_dev)
        out[0, at, :] = rows + more[g * RUN * n_dev:(g + 1) * RUN * n_dev, :]


def hot_out(first, n_l, gathered, freq_from, freq_at, skip, code, into):
    n_dev, _, emb = gathered.shape
    n_r = 2 * RUN
    width = n_r * n_dev
    blocks = into.shape[1] // width
    return pl.pallas_call(
        functools.partial(hot_kernel, skip),
        grid=(n_l, blocks),
        in_specs=[
            pl.BlockSpec((n_dev, n_r, emb), lambda i, b: (0, i * blocks + b, 0)),
            spec((n_dev, 2 * RUN, emb), 0, freq_at, 0, pipeline_mode=ONCE),
            pl.BlockSpec((1, width, 1), lambda i, b: (b, 0, 0)),
            ANY,
        ],
        out_specs=pl.BlockSpec((1, width, emb), lambda i, b: (first - i, b, 0)),
        out_shape=out_of(into.shape),
        scratch_shapes=[pltpu.VMEM((3, FREQ, emb), BF)],
        input_output_aliases={3: 0},
        compiler_params=params("arbitrary", "arbitrary"),
        cost_estimate=cost(n_l * gathered.size * LO, n_l), name="hot_out",
    )(gathered, freq_from, code.reshape(blocks, width, 1), into)


def empty(shape):
    return pl.pallas_call(lambda out: None, out_specs=ANY, out_shape=out_of(shape), name="empty")()


def table_kernel(at0, starts, row_of, *refs):
    srcs, out = refs[:-1], refs[-1]
    block = pl.program_id(0)
    out[...] = jnp.zeros(out.shape, F32)

    @pl.loop(starts[block], starts[block + 1])
    def _(k):
        at = row_of[k] - block * len(out)
        for l, src in enumerate(srcs):
            out[at, pl.ds(l, 1), :] = src[0, pl.ds(at0 + k, 1), :]


def table_out(rows_dev, at0, starts, row_of, srcs):
    n_l = len(srcs)
    _, n_c, emb = srcs[0][0].shape
    n_blocks = len(starts) - 1
    return pl.pallas_call(
        functools.partial(table_kernel, at0),
        grid_spec=pltpu.PrefetchScalarGridSpec(
            num_scalar_prefetch=2, grid=(n_blocks,),
            in_specs=[spec((1, n_c, emb), i, 0, 0) for _, i in srcs],
            out_specs=pl.BlockSpec((rows_dev // n_blocks, n_l, emb), lambda b, *_: (b, 0, 0))),
        out_shape=out_of((rows_dev, n_l, emb)), compiler_params=params("arbitrary"),
        cost_estimate=cost(rows_dev * n_l * emb * LO, n_l), name="table_out",
    )(starts, row_of, *[s for s, _ in srcs])


def row_kernel(at, row, into, out, sem):
    @pl.when(at[0] >= 0)
    def _():
        c = pltpu.make_async_copy(row, out.at[pl.ds(at[0], 1)], sem)
        c.start()
        c.wait()


def put_row(at, row, into):
    return pl.pallas_call(
        row_kernel,
        in_specs=[pl.BlockSpec(memory_space=pltpu.SMEM), pl.BlockSpec(memory_space=pltpu.VMEM), ANY], out_specs=ANY,
        out_shape=out_of(into.shape), scratch_shapes=[pltpu.SemaphoreType.DMA(())],
        input_output_aliases={2: 0}, name="put_row",
    )(at, row, into)


def down_sum(v):
    return jnp.sum(v, axis=0)


def row_sum(v):
    return jnp.sum(v, axis=1)


def square(n):
    return iota((n, n), 0), iota((n, n), 1)


def prefix(v):
    r, c = square(len(v))
    return row_sum(jnp.where(r > c, v[None, :], 0))


def digits(ids, n_hi):
    return one_hot(ids >> HI_BITS, n_hi), one_hot(ids & (LO - 1), LO)


def look(hi_lo, *maps):
    hi, lo = hi_lo
    got = dot32(hi, jnp.concatenate(maps, axis=1))
    return [row_sum(got[:, i * LO:(i + 1) * LO] * lo.astype(F32)).astype(I32) for i in range(len(maps))]


def number(count, most):
    levels = jnp.array(LEVELS, F32)
    n_over = jnp.sum((count[:, :, None] >= levels).astype(F32), axis=(0, 1))
    flag = count >= jnp.min(jnp.where(n_over <= most, levels, jnp.inf))
    r, c = square(LO)
    in_row = dot32(flag.astype(BF), (r < c).astype(BF))
    return jnp.where(flag, in_row + prefix(row_sum(flag.astype(F32)))[:, None] + 1, 0)


def solution(mesh):
    n_dev = mesh.shape['emb']

    def body(token_ids, hot_ids, x_in, d_out, emb_table, hot_table, w_up, w_down, w_gate, w_proj):
        n_loc = len(token_ids)
        layers, rows_dev, emb_dim = emb_table.shape
        n_hot = len(hot_ids)
        places, hot_dev, per_dev = n_loc // n_dev, n_hot // n_dev, FREQ // n_dev
        n_hi = -(-rows_dev * n_dev // (8 * LO)) * 8
        me = lax.axis_index('emb')
        hot_at, cold_at = FREQ, FREQ + hot_dev

        def swap(v):
            return lax.all_to_all(v, 'emb', 0, 0, tiled=True)

        def exchange(v):
            return swap(v.reshape(n_dev, places, -1)).reshape(n_loc, -1)

        def prepare(got_class, hot_hi, hot_lo, row_used, cold_owner, freq_cold, freq_map, hot_table, by_row, move, d_out):
            (hot_f,) = look((hot_hi, hot_lo), freq_map)
            used_rank = prefix(row_used.astype(I32))
            at_rank = (used_rank[None, :] == iota((COLD_MAX, rows_dev), 0)) & row_used[None, :]
            row_of = row_sum(jnp.where(at_rank, iota((COLD_MAX, rows_dev), 1), 0))
            packed = pack_rows(row_of, by_row)
            hot_pick = one_hot(hot_f - 1, FREQ_HOT).T
            by_owner = hot_table.reshape(layers, hot_dev // RUN, n_dev, RUN, emb_dim)
            hot_mine = lax.dynamic_index_in_dim(by_owner, me, 2, keepdims=False).reshape(layers, hot_dev, emb_dim)
            table = jnp.stack([jnp.concatenate([
                dot32(hot_pick, hot_table[i]).astype(BF), dot32(one_hot(cold_owner, n_dev), freq_cold[:, i]).astype(BF),
                hot_mine[i], packed[:, i]], axis=0) for i in range(layers)])
            n_blocks = 12 if rows_dev % 12 == 0 else 1
            edge_shape = (n_blocks + 1, rows_dev)
            before = iota(edge_shape, 1) < (rows_dev // n_blocks) * iota(edge_shape, 0)
            starts = jnp.minimum(row_sum(jnp.where(row_used[None, :] & before, 1, 0)), COLD_MAX)
            row_no = got_class - cold_at
            used_before = row_sum(jnp.where(row_used[None, :] & (iota((n_loc, rows_dev), 1) < row_no[:, None]), 1, 0))
            cls = jnp.where(row_no >= 0, cold_at + used_before, got_class)
            code = jnp.where(hot_f <= FREQ_HOT, hot_f - 1, -1)
            d_placed = dot32(move, d_out).astype(BF)
            return d_placed, table, cls, starts, row_of, code

        count = count_ids(swap(jnp.broadcast_to(token_ids[None, :], (n_dev, n_loc))), n_hi)
        tok, hot = digits(token_ids, n_hi), digits(hot_ids, n_hi)
        slot_no = jnp.arange(n_hot, dtype=I32)
        hot_place = slot_no // (RUN * n_dev) * RUN + slot_no % RUN
        hot_owner = slot_no // RUN % n_dev
        q_map = dot32(hot[0].T, hot[1] * (hot_place + 1).astype(BF)[:, None]).astype(BF)
        r_map = dot32(hot[0].T, hot[1] * hot_owner.astype(BF)[:, None]).astype(BF)
        hot_no = number(jnp.where(q_map > 0, count, 0), FREQ_HOT)
        cold_no = number(jnp.where(q_map > 0, 0, count), FREQ_COLD)
        freq_map = jnp.where(hot_no > 0, hot_no, jnp.where(cold_no > 0, FREQ_HOT + cold_no, 0)).astype(BF)
        id_map = iota((n_hi, LO), 0) * LO + iota((n_hi, LO), 1) + 1
        cold_id = jnp.sum(jnp.where(cold_no.astype(I32)[None] == iota((FREQ_COLD, 1, 1), 0) + 1, id_map[None], 0), axis=(1, 2)) - 1
        cold_owner = jnp.where(cold_id >= 0, cold_id // rows_dev, -1)
        my_cold = (cold_owner == me).astype(I32)
        my_row = jnp.minimum(jnp.sum(my_cold * (cold_id - me * rows_dev + 1)) - 1, rows_dev - 1)
        by_row = emb_table.transpose(1, 0, 2)
        cold_row = lax.dynamic_slice_in_dim(by_row, jnp.maximum(my_row, 0), 1)
        freq_cold = swap(jnp.broadcast_to(cold_row, (n_dev, layers, emb_dim)))

        tok_f, tok_q, tok_r = look(tok, freq_map, q_map, r_map)
        rare = tok_f == 0
        owner = jnp.where(tok_q > 0, tok_r, token_ids // rows_dev)
        dev_no = iota((n_loc, n_dev), 1)
        to_dev = (owner[:, None] == dev_no) & rare[:, None]
        marks = jnp.concatenate([to_dev.astype(BF), jnp.logical_not(rare).astype(BF)[:, None]], axis=1)
        r, c = square(n_loc)
        ranks = dot32((r > c).astype(BF), marks)
        sent = down_sum(to_dev.astype(F32))
        free = jnp.maximum(places - sent, 0)
        free_at = prefix(free)
        fill = ranks[:, n_dev:]
        fill_dev = (fill >= free_at) & (fill < free_at + free)
        to_dev = jnp.where(rare[:, None], to_dev, fill_dev)
        place = jnp.where(rare[:, None], ranks[:, :n_dev], fill + (sent - free_at))
        slot = row_sum(jnp.where(to_dev, dev_no * places + place.astype(I32), 0))
        row_ids = me * rows_dev + jnp.arange(rows_dev, dtype=I32)
        row_f, row_q, row_n = look(digits(row_ids, n_hi), freq_map, q_map, (count > 0).astype(BF))
        row_used = (row_n > 0) & (row_f == 0) & (row_q == 0)
        fits = ((jnp.max(sent) <= places) & (jnp.sum(row_used.astype(I32)) <= COLD_MAX) & (jnp.sum(my_cold) <= 1))
        tok_class = jnp.where(rare, jnp.where(tok_q > 0, hot_at + tok_q - 1, cold_at + token_ids % rows_dev), tok_f - 1)
        bad = 1 << 20
        move = r == slot[None, :]
        send_class, freq_cold = lax.optimization_barrier(
            (row_sum(jnp.where(move, tok_class[None, :], 0)) + jnp.where(fits, 0, bad), freq_cold))
        got_class = swap(send_class.reshape(n_dev, places)).reshape(n_loc)
        move = move.astype(BF)
        placed, got_class, hot_hi, hot_lo, row_used, cold_owner = lax.optimization_barrier(
            (dot32(move, x_in).astype(BF), got_class, *hot, row_used, cold_owner))
        x_moved = exchange(placed)
        given = prepare(got_class, hot_hi, hot_lo, row_used, cold_owner, freq_cold, freq_map, hot_table, by_row, move, d_out)
        all_fit = jnp.max(got_class) < bad

        def freq_parts(sums):
            return sums[:, :FREQ].reshape(2, n_dev, per_dev, emb_dim).transpose(1, 0, 2, 3)

        def own_hot(sums):
            return sums[:, hot_at:cold_at].reshape(-1, emb_dim)

        def fast(x_moved, slot, my_cold, my_row, d_placed, table, cls, starts, row_of, code):
            d_moved = exchange(d_placed)
            cls_row = cls.reshape(1, n_loc)
            xs, hs, ss, es, x_last = forward(x_moved, cls.reshape(n_loc, 1), table, w_up, w_down, w_gate, w_proj)
            x_back = exchange(x_last)
            kept = (cls_row, es, xs, hs, ss, w_up, w_down, w_gate, w_proj)
            sums_3, r = backward(3, 1, True, d_moved, *kept)
            all_3 = lax.all_gather(own_hot(sums_3), 'emb')
            sums_2, r = backward(2, 1, True, r, *kept)
            all_2 = lax.all_gather(own_hot(sums_2), 'emb')
            freq_a = swap(freq_parts(jnp.concatenate([sums_3, sums_2], axis=0)))
            r, x_back = lax.optimization_barrier((r, x_back))
            sums_b, _ = backward(1, 2, False, r, *kept)
            freq_b = swap(freq_parts(sums_b))
            x_out = dot32((slot[:, None] == iota((n_loc, n_loc), 1)).astype(BF), x_back).astype(BF)
            d_table = table_out(rows_dev, cold_at, starts, row_of, [(sums_b, 1), (sums_b, 0), (sums_2, 0), (sums_3, 0)])
            totals = [down_sum(v).reshape(2 * per_dev, emb_dim) for v in (freq_a, freq_b)]
            mine = jnp.concatenate([own_hot(sums_b)] + totals, axis=0)
            mine, x_out, d_table = lax.optimization_barrier((mine, x_out, d_table))
            all_b = gather_all(mine, n_dev)
            at_freq = 2 * hot_dev // (2 * RUN)
            into = empty((layers, n_hot, emb_dim))
            into = hot_out(1, 2, all_b, all_b, at_freq + 1, 0, code, into)
            into = hot_out(3, 1, all_3, all_b, at_freq, 0, code, into)
            into = hot_out(2, 1, all_2, all_b, at_freq, 1, code, into)
            pick = jnp.concatenate([jnp.zeros((FREQ_HOT,), F32), my_cold.astype(F32)]).reshape(n_dev, 1, per_dev, 1)
            freq = all_b[:, 2 * hot_dev:].reshape(n_dev, layers, per_dev, emb_dim)
            row = jnp.sum(freq * pick, axis=(0, 2))[::-1]
            d_table = put_row(my_row.reshape(1), row[None], d_table)
            return x_out, d_table.transpose(1, 0, 2), into

        def slow(*_):
            return general_path(n_dev, me, token_ids, hot_ids, x_in, d_out, emb_table, hot_table, w_up, w_down, w_gate, w_proj)

        return lax.cond(all_fit, fast, slow, *lax.optimization_barrier((x_moved, slot, my_cold, my_row, *given)))

    return jax.shard_map(body, mesh=mesh,
                         in_specs=(P('emb'), P(), P('emb', None), P('emb', None), P(None, 'emb', None), P(), P(), P(), P(), P()),
                         out_specs=(P('emb', None), P(None, 'emb', None), P()),
                         check_vma=False)
```

```python
import functools

import jax
import jax.numpy as jnp
from jax import lax
from jax.experimental import pallas as pl
from jax.experimental.pallas import tpu as pltpu
from jax.sharding import PartitionSpec as P


NORM_EPS = 1e-6
FREQ_HOT = 112
FREQ_COLD = 16
FREQ = FREQ_HOT + FREQ_COLD
COLD_MAX = 256
LO = 256
HI_BITS = 8
RUN = 4
LEVELS = tuple(16 * 2 ** (i / 4) for i in range(17))
GELU_A = 0.7978845608028654
GELU_B = GELU_A * 0.044715
VMEM = 66_000_000
ROWS_A = 256
ROWS_B = 512
TILE = 1024
BF = jnp.bfloat16
F32 = jnp.float32
I32 = jnp.int32
ONCE = pl.Buffered(1)


def gelu_back(pre_act, cot_in):
    _, pull = jax.vjp(jax.nn.gelu, pre_act.astype(F32))
    return pull(cot_in)[0]


def swap(v):
    return lax.all_to_all(v, 'emb', 0, 0, tiled=True)


def col(v):
    return v[:, None]


def row(v):
    return v[None, :]


def dot32(a, b):
    return jnp.dot(a, b, preferred_element_type=F32)


def dense_parts(resid, w_up, w_gate):
    resid_f = resid.astype(F32)
    inv_rms = lax.rsqrt(jnp.mean(resid_f * resid_f, axis=-1, keepdims=True) + NORM_EPS)
    normed = (resid_f * inv_rms).astype(BF)
    hidden = dot32(normed, w_up).astype(BF)
    gate_pre = dot32(normed, w_gate).astype(BF)
    return resid_f, inv_rms, hidden, gate_pre


def layer_forward(resid, emb_rows, w_up, w_down, w_gate, w_proj):
    resid_f, _, hidden, gate_pre = dense_parts(resid, w_up, w_gate)
    activated = jax.nn.gelu(hidden.astype(F32)).astype(BF)
    mlp_out = dot32(activated, w_down).astype(BF)
    gate = jax.nn.gelu(gate_pre.astype(F32)).astype(BF)
    mixed = (gate.astype(F32) * emb_rows.astype(F32)).astype(BF)
    projected = dot32(mixed, w_proj).astype(BF)
    return (resid_f + mlp_out.astype(F32) + projected.astype(F32)).astype(BF)


def layer_backward(resid, emb_rows, d_next, w_up, w_down, w_gate, w_proj):
    resid_f, inv_rms, hidden, gate_pre = dense_parts(resid, w_up, w_gate)
    gate = jax.nn.gelu(gate_pre.astype(F32)).astype(BF)
    d_cast = d_next.astype(BF)
    d_mixed = jnp.einsum('nd,ed->ne', d_cast, w_proj, preferred_element_type=F32)
    d_rows = gate.astype(F32) * d_mixed
    d_gpre = gelu_back(gate_pre, d_mixed * emb_rows.astype(F32))
    d_hidden = gelu_back(hidden, jnp.einsum('nd,fd->nf', d_cast, w_down, preferred_element_type=F32))
    d_normed = (jnp.einsum('nf,df->nd', d_hidden.astype(BF), w_up, preferred_element_type=F32)
                + jnp.einsum('ne,de->nd', d_gpre.astype(BF), w_gate, preferred_element_type=F32))
    inner = jnp.mean(d_normed * resid_f, axis=-1, keepdims=True)
    d_prev = d_next + inv_rms * d_normed - resid_f * (inv_rms * inv_rms * inv_rms) * inner
    return d_prev, d_rows


def general_path(n_dev, my_index, token_ids, hot_ids, x_in, d_out, emb_table, hot_table, w_up, w_down, w_gate, w_proj):
    n_loc = token_ids.shape[0]
    _, rows_dev, emb_dim = emb_table.shape
    capacity = max(8, (2 * n_loc) // n_dev)
    n_slots = n_dev * capacity
    hot_match = col(token_ids) == row(hot_ids)
    is_hot = hot_match.any(1)
    hot_pick = hot_match.astype(BF)
    hot_pick_f = hot_match.astype(F32)
    owner_id = token_ids // rows_dev
    to_owner = (col(owner_id) == row(jnp.arange(n_dev, dtype=I32))) & col(jnp.logical_not(is_hot))
    owner_rank = jnp.cumsum(to_owner.astype(jnp.int32), axis=0) - 1
    place = row_sum(jnp.where(to_owner, owner_rank, 0))
    slot = jnp.where(is_hot, n_slots, owner_id * capacity + place)
    none = jnp.full((n_slots,), -1, I32)
    send_ids = none.at[slot].set(token_ids, mode='drop')
    slot_tok = none.at[slot].set(jnp.arange(n_loc, dtype=jnp.int32), mode='drop')
    recv_ids = swap(send_ids.reshape(n_dev, capacity)).reshape(n_slots)
    served_ok = recv_ids >= 0
    local_row = jnp.where(served_ok, recv_ids - my_index * rows_dev, 0)
    pick_slot = jnp.minimum(slot, n_slots - 1)
    slot_used = slot_tok >= 0
    slot_src = jnp.maximum(slot_tok, 0)

    def fwd(resid, per_layer):
        table, hot_l, up, down, gate_w, proj = per_layer
        served = table[local_row]
        fetched = swap(served.reshape(n_dev, capacity, emb_dim)).reshape(n_slots, emb_dim)
        cold_rows = fetched[pick_slot]
        hot_rows = dot32(hot_pick, hot_l).astype(BF)
        emb_rows = jnp.where(col(is_hot), hot_rows, cold_rows)
        return layer_forward(resid, emb_rows, up, down, gate_w, proj), (resid, emb_rows)

    x_out, (x_saved, rows_saved) = lax.scan(fwd, x_in, (emb_table, hot_table, w_up, w_down, w_gate, w_proj))

    def bwd(d_resid, per_layer):
        resid_l, rows_l, up, down, gate_w, proj = per_layer
        d_resid, d_rows = layer_backward(resid_l, rows_l, d_resid, up, down, gate_w, proj)
        outgoing = jnp.where(col(slot_used), d_rows[slot_src], 0.0)
        incoming = swap(outgoing.reshape(n_dev, capacity, emb_dim)).reshape(n_slots, emb_dim)
        d_tab = jax.ops.segment_sum(jnp.where(col(served_ok), incoming, 0.0), local_row, num_segments=rows_dev)
        hot_local = jnp.einsum('nh,ne->he', hot_pick_f, d_rows, precision=lax.Precision.HIGHEST, preferred_element_type=F32)
        return d_resid, (d_tab, lax.psum(hot_local, 'emb'))

    _, (d_table, d_hot) = lax.scan(bwd, d_out.astype(F32), (x_saved, rows_saved, w_up, w_down, w_gate, w_proj), reverse=True)
    return x_out, d_table, d_hot


def split3(v):
    hi = v.astype(BF)
    rest = v - hi.astype(F32)
    mid = rest.astype(BF)
    return hi, mid, (rest - mid.astype(F32)).astype(BF)


def iota(shape, dim):
    return lax.broadcasted_iota(jnp.int32, shape, dim)


def one_hot(v, n, dtype=BF):
    return (col(v) == iota((len(v), n), 1)).astype(dtype)


def dot_nt(a, b):
    return lax.dot_general(a, b, (((1,), (1,)), ((), ())), preferred_element_type=F32)


def gelu(x):
    half = 0.5 * x
    return half + half * jnp.tanh(x * (GELU_A + GELU_B * (x * x)))


def gelu_slope(x):
    sq = x * x
    th = jnp.tanh(x * (GELU_A + GELU_B * sq))
    return (0.5 + 0.5 * th) + (0.5 * x) * (1.0 - th * th) * (GELU_A + (3.0 * GELU_B) * sq)


def forward_kernel(n_l, n_f, x0, cls, table, wu, wd, wg, wp, xs, hs, ss, es, xo, zeros, x_now, u_now, acc, q_now, blank, sem):
    layer, step = pl.program_id(0), pl.program_id(1)
    n_tok = x_now.shape[0]
    n_blank = blank.shape[0]
    blanks = [pltpu.make_async_copy(blank, zeros.at[pl.ds(i, n_blank)], sem) for i in range(0, zeros.shape[0], n_blank)]

    @pl.when((layer == 0) & (step == n_f - 1))
    def _():
        blank[...] = jnp.zeros(blank.shape, F32)
        for b in blanks:
            b.start()

    @pl.when((layer == n_l - 1) & (step == n_f - 1))
    def _():
        for b in blanks:
            b.wait()


    @pl.when((layer == 0) & (step == 0))
    def _():
        x_now[...] = x0[...]

    @pl.when(step == 0)
    def _():
        for m in chunks(n_tok, ROWS_A):
            xb = x_now[m, :]
            x = xb.astype(F32)
            xs[m, :] = xb
            u = (x * lax.rsqrt(jnp.mean(x * x, axis=-1, keepdims=True) + NORM_EPS)).astype(BF)
            u_now[m, :] = u
            s = dot32(u, wg[...]).astype(BF)
            ss[m, :] = s
            g = gelu(s.astype(F32)).astype(BF)
            pick = (cls[m, :] == iota((m.size, table.shape[0]), 1)).astype(BF)
            e = dot32(pick, table[...]).astype(BF)
            es[m, :] = e
            mixed = (g.astype(F32) * e.astype(F32)).astype(BF)
            q_now[m, :] = dot32(mixed, wp[...]).astype(BF)
            acc[m, :] = jnp.zeros((m.size, acc.shape[1]), F32)

    for m in chunks(n_tok, ROWS_B):
        h = dot32(u_now[m, :], wu[...]).astype(BF)
        hs[m, :] = h
        acc[m, :] += dot32(gelu(h.astype(F32)).astype(BF), wd[...])

    @pl.when(step == n_f - 1)
    def _():
        for m in chunks(n_tok, ROWS_A):
            x = x_now[m, :].astype(F32) + acc[m, :].astype(BF).astype(F32) + q_now[m, :].astype(F32)
            x_now[m, :] = x.astype(BF)

    @pl.when((step == n_f - 1) & (layer == n_l - 1))
    def _():
        xo[...] = x_now[...]


def chunks(n, size):
    size = min(n, size)
    return [pl.ds(m, size) for m in range(0, n, size)]


def forward(x0, cls, table, w_up, w_down, w_gate, w_proj, rows_dev):
    n_tok, dim = x0.shape
    n_l, _, ff = w_up.shape
    emb = w_gate.shape[2]
    tile = min(TILE, ff)
    n_f = ff // tile
    n_c = table.shape[1]

    def whole(l, f):
        return (l, 0, 0)

    def cols(l, f):
        return (l, 0, f)

    def fixed(l, f):
        return (0, 0)

    return pl.pallas_call(
        functools.partial(forward_kernel, n_l, n_f),
        grid=(n_l, n_f),
        in_specs=[
            pl.BlockSpec((n_tok, dim), fixed, pipeline_mode=ONCE),
            pl.BlockSpec((n_tok, 1), fixed, pipeline_mode=ONCE),
            pl.BlockSpec((None, n_c, emb), whole),
            pl.BlockSpec((None, dim, tile), cols),
            pl.BlockSpec((None, tile, dim), lambda l, f: (l, f, 0)),
            pl.BlockSpec((None, dim, emb), whole),
            pl.BlockSpec((None, emb, dim), whole),
        ],
        out_specs=[
            pl.BlockSpec((None, n_tok, dim), whole),
            pl.BlockSpec((None, n_tok, tile), cols),
            pl.BlockSpec((None, n_tok, emb), whole),
            pl.BlockSpec((None, n_tok, emb), whole),
            pl.BlockSpec((n_tok, dim), fixed),
            ANY,
        ],
        out_shape=[out_of((n_l, n_tok, n), BF) for n in (dim, ff, emb, emb)] + [out_of((n_tok, dim), BF), out_of((rows_dev, n_l, emb))],
        scratch_shapes=[pltpu.VMEM((n_tok, dim), t) for t in (BF, BF, F32, BF)]
        + [pltpu.VMEM((rows_dev // 12, n_l, emb), F32), pltpu.SemaphoreType.DMA(())],
        compiler_params=params("arbitrary", "arbitrary"),
        cost_estimate=cost(n_l * n_tok * dim * (2 * ff + 2 * emb + n_c), n_l),
        name="forward",
    )(x0, cls, table, w_up, w_down, w_gate, w_proj)


def params(*kinds, **more):
    return pltpu.CompilerParams(vmem_limit_bytes=VMEM, dimension_semantics=kinds or None, **more)


def cost(products, layers):
    return pl.CostEstimate(flops=2 * products, bytes_accessed=layers * 40_000_000, transcendentals=0)


def backward_kernel(n_f, r_in, cls_t, es, xs, hs, ss, wu, wd, wg, wp, *refs):
    talks = len(refs) > 5
    if talks:
        prev, sums, r, out, tot, c_now, acc, three, sems, sems_f, *bufs = refs
        at = Place()
        gather = Spread(at, prev.at[pl.ds(HOT_AT, COLD_AT - HOT_AT)], lambda d: out.at[d], sems)
        fold = Fold(at, prev.at[pl.ds(0, FREQ)], bufs, sems_f)
    else:
        sums, r, c_now, acc, three = refs
    f = pl.program_id(0)
    n_tok = c_now.shape[0]

    @pl.when(f == 0)
    def _():
        if talks:
            at.meet()
            gather.begin()
            fold.begin()
        r[...] = r_in[...].astype(F32)
        for m in chunks(n_tok, ROWS_B):
            c = r[m, :].astype(BF)
            c_now[m, :] = c
            a = dot_nt(c, wp[...])
            s = ss[m, :].astype(F32)
            rows = gelu(s).astype(BF).astype(F32) * a
            for i, part in enumerate(split3(rows)):
                three[i, m, :] = part
            ds = (gelu_slope(s) * (a * es[m, :].astype(F32))).astype(BF)
            acc[m, :] = dot_nt(ds, wg[...])
        class_sums(cls_t, three, sums)
        if talks:
            gather.column(1)
            gather.onward(0)
            fold.step(0)

    if talks:
        @pl.when(f == 1)
        def _():
            gather.column(2)
            gather.onward(1)
            fold.step(1)

        @pl.when(f == 2)
        def _():
            gather.column(3)
            gather.onward(2)
            fold.step(2)

        @pl.when(f == 3)
        def _():
            gather.across(0)
            gather.onward(3)
            tot[...] = fold.total()

    for m in chunks(n_tok, ROWS_B):
        d_act = dot_nt(c_now[m, :], wd[...])
        dh = (gelu_slope(hs[m, :].astype(F32)) * d_act).astype(BF)
        acc[m, :] += dot_nt(dh, wu[...])

    @pl.when(f == n_f - 1)
    def _():
        if talks:
            gather.across(1)
            gather.across(2)
        for m in chunks(n_tok, ROWS_A):
            x = xs[m, :].astype(F32)
            k = lax.rsqrt(jnp.mean(x * x, axis=-1, keepdims=True) + NORM_EPS)
            du = acc[m, :]
            inner = jnp.mean(du * x, axis=-1, keepdims=True)
            r[m, :] = r[m, :] + k * du - x * (k * k * k) * inner
        if talks:
            gather.across(3)
            gather.end()


def backward(layer, r_in, cls_t, es, xs, hs, ss, w_up, w_down, w_gate, w_proj, prev=None, n_dev=0):
    n_tok, dim = r_in.shape
    ff = w_up.shape[2]
    emb = w_gate.shape[2]
    n_c = COLD_AT + COLD_MAX
    n_f = 4
    tile = ff // n_f
    talks = prev is not None
    once = dict(pipeline_mode=ONCE)

    def whole(n, m):
        return spec((None, n, m), layer, 0, 0, **once)

    def cols(n):
        return pl.BlockSpec((None, n, tile), lambda t: (layer, 0, t))

    return pl.pallas_call(
        functools.partial(backward_kernel, n_f),
        grid=(n_f,),
        in_specs=[spec((n_tok, dim), **once), spec((1, n_tok), **once), whole(n_tok, emb), whole(n_tok, dim), cols(n_tok), whole(n_tok, emb),
                  cols(dim), pl.BlockSpec((None, tile, dim), lambda t: (layer, t, 0)), whole(dim, emb), whole(emb, dim)]
        + [spec((n_c, emb), **once)] * talks,
        out_specs=[spec((n_c, emb)), spec((n_tok, dim))] + [ANY, spec((16, emb))] * talks,
        out_shape=[out_of((n_c, emb)), out_of((n_tok, dim))] + [out_of((n_dev, COLD_AT - HOT_AT, emb)), out_of((16, emb))] * talks,
        scratch_shapes=[pltpu.VMEM((n_tok, dim), BF), pltpu.VMEM((n_tok, dim), F32), pltpu.VMEM((3, n_tok, emb), BF)]
        + ([SPREAD_SEMS, FOLD_SEMS] + fold_bufs(emb)) * talks,
        compiler_params=params("arbitrary", **(dict(collective_id=layer - 1, has_side_effects=True) if talks else {})),
        cost_estimate=cost(n_tok * dim * (2 * ff + 2 * emb + 3 * n_c), 1),
        name="backward",
    )(r_in, cls_t, es, xs, hs, ss, w_up, w_down, w_gate, w_proj, *([prev] if talks else []))


def spec(shape, *index, **more):
    index = index or (0,) * len(shape)
    return pl.BlockSpec(shape, lambda *_: index, **more)


ANY = pl.BlockSpec(memory_space=pl.ANY)


def out_of(shape, dtype=F32):
    return jax.ShapeDtypeStruct(shape, dtype)


def count_kernel(ids, out):
    n_tok = ids.shape[1]
    out[...] = jnp.zeros(out.shape, F32)

    @pl.loop(0, len(ids))
    def _(i):
        row = ids[pl.ds(i, 1), :]
        hi = ((row >> HI_BITS) == iota((len(out), n_tok), 0)).astype(BF)
        lo = ((row & (LO - 1)) == iota((LO, n_tok), 0)).astype(BF)
        out[...] += dot_nt(hi, lo)


def count_ids(ids, n_hi):
    return pl.pallas_call(count_kernel, out_shape=out_of((n_hi, LO)), compiler_params=params(), name="count_ids")(ids)


def pack_kernel(row_of, table, out, sem):
    @pl.loop(0, len(out))
    def _(k):
        pltpu.make_async_copy(table.at[row_of[k]], out.at[k], sem).start()

    pltpu.make_async_copy(table.at[pl.ds(0, len(out))], out, sem).wait()


def pack_rows(row_of, table):
    shape = row_of.shape + table.shape[1:]
    return pl.pallas_call(
        pack_kernel,
        grid_spec=pltpu.PrefetchScalarGridSpec(num_scalar_prefetch=1, grid=(1,), in_specs=[ANY], out_specs=spec(shape),
                                               scratch_shapes=[pltpu.SemaphoreType.DMA(())]),
        out_shape=out_of(shape, table.dtype), compiler_params=params(), name="pack_rows",
    )(row_of, table)


class Place:
    def __init__(self):
        me = lax.axis_index('emb')
        self.core, self.x, self.y, self.z = me % 2, (me // 2) % 2, (me // 4) % 2, me // 8
        self.others = [self.dev(z=(self.z + k) % 4) for k in REST]
        self.columns = [(self.z - k + 4) % 4 for k in STOPS]
        self.to_x, self.to_y, self.to_core = self.dev(x=1 - self.x), self.dev(y=1 - self.y), self.dev(core=1 - self.core)

    def dev(self, z=None, y=None, x=None, core=None):
        z, y, x, core = [mine if v is None else v for v, mine in ((z, self.z), (y, self.y), (x, self.x), (core, self.core))]
        return ((z * 2 + y) * 2 + x) * 2 + core

    def meet(self):
        barrier = pltpu.get_barrier_semaphore()
        peers = self.others + [self.to_x, self.to_y, self.to_core]
        for peer in peers:
            pl.semaphore_signal(barrier, device_id=(peer,), device_id_type=pl.DeviceIdType.MESH)
        pl.semaphore_wait(barrier, len(peers))


def remote(src, dst, sems, to):
    return pltpu.make_async_remote_copy(src_ref=src, dst_ref=dst, send_sem=sems[0], recv_sem=sems[1],
                                        device_id=(to,), device_id_type=pl.DeviceIdType.MESH)


Z, X, Y, FX, FY, C, CX, CY, CD, OWN = range(10)


class Spread:
    def __init__(self, at, mine, slot, sems):
        self.at, self.mine, self.slot, self.sems = at, mine, slot, sems
        n = mine.shape[0]
        half = n // 16 * 8
        self.halves = {FY: pl.ds(0, half), FX: pl.ds(half, n - half)}
        self.col = [at.dev(z=z) for z in at.columns]
        self.by_x = [at.dev(z=z, x=1 - at.x) for z in at.columns]
        self.by_y = [at.dev(z=z, y=1 - at.y) for z in at.columns]
        self.by_d = [at.dev(z=z, x=1 - at.x, y=1 - at.y) for z in at.columns]
        self.far = [[at.dev(z=z, x=x, y=y, core=1 - at.core) for z in at.columns]
                    for y, x in ((at.y, at.x), (at.y, 1 - at.x), (1 - at.y, at.x), (1 - at.y, 1 - at.x))]
        self.done = []

    def pair(self, kind, k):
        return self.sems.at[0, kind, k], self.sems.at[1, kind, k]

    def send(self, kind, k, src, dst, to):
        remote(src, dst, self.pair(kind, k), to).start()
        self.done.append((kind, k))

    def got(self, kind, k, block):
        remote(block, block, self.pair(kind, k), self.at.to_x).wait_recv()

    def begin(self):
        own = self.slot(self.col[0])
        pltpu.make_async_copy(self.mine, own, self.sems.at[0, OWN, 0]).start()
        for k, other in enumerate(self.at.others):
            self.send(Z, k + 1, self.mine, own, other)
        self.column(0)

    def column(self, k):
        block = self.slot(self.col[k])
        if k:
            self.got(Z, k, block)
        src = block if k else self.mine
        for kind, to in ((X, self.at.to_x), (Y, self.at.to_y), (C, self.at.to_core)):
            self.send(kind, k, src, block, to)

    def onward(self, k):
        for kind, part, to, other, core in ((X, self.by_x, self.at.to_y, FY, CX), (Y, self.by_y, self.at.to_x, FX, CY)):
            block = self.slot(part[k])
            self.got(kind, k, block)
            half = block.at[self.halves[other]]
            self.send(other, k, half, half, to)
            self.send(core, k, block, block, self.at.to_core)

    def across(self, k):
        block = self.slot(self.by_d[k])
        for kind, half in self.halves.items():
            self.got(kind, k, block.at[half])
        self.send(CD, k, block, block, self.at.to_core)

    def end(self):
        for k in STOPS:
            for kind, far in zip((C, CX, CY, CD), self.far):
                self.got(kind, k, self.slot(far[k]))
        own = self.slot(self.col[0])
        for kind, k in self.done:
            block = own.at[self.halves[kind]] if kind in self.halves else own
            remote(block, block, self.pair(kind, k), self.at.to_x).wait_send()
        pltpu.make_async_copy(self.mine, own, self.sems.at[0, OWN, 0]).wait()


class Fold:
    def __init__(self, at, part, bufs, sems):
        self.at, self.part, self.sems = at, part, sems
        self.ins, self.sums, self.all_z = bufs[:3], bufs[3:5], bufs[5]
        self.bits = at.core, at.x, at.y
        self.to = at.to_core, at.to_x, at.to_y

    def pair(self, i, k=0):
        return self.sems.at[0, i, k], self.sems.at[1, i, k]

    def cut(self, i, bit):
        n = self.ins[i].shape[0]
        return pl.ds(pl.multiple_of(bit * n, n), n)

    def source(self, i):
        return self.sums[i - 1] if i else self.part

    def hop(self, i):
        return remote(self.source(i).at[self.cut(i, 1 - self.bits[i])], self.ins[i], self.pair(i), self.to[i])

    def begin(self):
        self.hop(0).start()

    def step(self, i):
        self.hop(i).wait_recv()
        total = self.source(i)[self.cut(i, self.bits[i]), :] + self.ins[i][...]
        if i < 2:
            self.sums[i][...] = total
            self.hop(i + 1).start()
        else:
            self.all_z[self.at.z] = total
            for k, other in enumerate(self.at.others):
                self.along_z(k, other).start()

    def along_z(self, k, other):
        block = self.all_z.at[self.at.z]
        return remote(block, block, self.pair(3, k), other)

    def total(self):
        for k, other in enumerate(self.at.others):
            self.along_z(k, other).wait_recv()
        for i in range(3):
            self.hop(i).wait_send()
        for k, other in enumerate(self.at.others):
            self.along_z(k, other).wait_send()
        v = self.all_z
        return (v[0] + v[1]) + (v[2] + v[3])


def fold_bufs(emb):
    return [pltpu.VMEM((n, emb), F32) for n in (64, 32, 16, 64, 32)] + [pltpu.VMEM((4, 16, emb), F32)]


SPREAD_SEMS = pltpu.SemaphoreType.DMA((2, 10, 4))
STOPS = range(4)
REST = STOPS[1:]
FOLD_SEMS = pltpu.SemaphoreType.DMA((2, 4, 4))
HOT_AT, COLD_AT = FREQ, FREQ + 64


def last_kernel(r_in, ss, wp, cls_t, prev, *refs):
    early, (sums, out, r, s, w, three, pay, copies, sems_1, sems_0, sems_f1, sems_f0), bufs = refs[:2], refs[2:14], refs[14:]
    n_hot = COLD_AT - HOT_AT
    n = pay.shape[1]
    loads = [pltpu.make_async_copy(src, dst, copies.at[i]) for i, (src, dst) in enumerate(((r_in, r), (ss.at[0], s), (wp.at[0], w)))]
    for load in loads:
        load.start()
    at = Place()
    at.meet()

    def fill(i, hot, totals):
        pay[i, pl.ds(0, n_hot), :] = hot
        for z in STOPS:
            @pl.when(at.z == z)
            def _(z=z):
                for j, t in enumerate(totals):
                    pay[i, pl.ds(n_hot + RUN * j, RUN), :] = t[z * RUN:(z + 1) * RUN, :]

    fold_1 = Fold(at, prev.at[pl.ds(0, FREQ)], bufs[:6], sems_f1)
    fold_0 = Fold(at, sums.at[pl.ds(0, FREQ)], bufs[6:], sems_f0)
    all_1 = Spread(at, pay.at[0], lambda d: out.at[d, pl.ds(0, n)], sems_1)
    all_0 = Spread(at, pay.at[1], lambda d: out.at[d, pl.ds(n, n)], sems_0)
    fold_1.begin()
    fill(0, prev[pl.ds(HOT_AT, n_hot), :], [t[...] for t in early])
    all_1.begin()
    for load in loads:
        load.wait()
    for m in chunks(len(r), ROWS_B):
        a = dot_nt(r[m, :].astype(BF), w[...])
        rows = gelu(s[m, :].astype(F32)).astype(BF).astype(F32) * a
        for i, part in enumerate(split3(rows)):
            three[i, m, :] = part
    fold_1.step(0)
    class_sums(cls_t, three, sums)
    fold_0.begin()
    all_1.column(1)
    all_1.onward(0)
    fold_1.step(1)
    fold_0.step(0)
    all_1.column(2)
    all_1.onward(1)
    fold_1.step(2)
    fold_0.step(1)
    all_1.column(3)
    all_1.onward(2)
    total_1 = fold_1.total()
    fold_0.step(2)
    all_1.across(0)
    all_1.onward(3)
    fill(1, sums[pl.ds(HOT_AT, n_hot), :], [total_1, fold_0.total()])
    all_0.begin()
    for k in REST:
        all_1.across(k)
    for k in REST:
        all_0.column(k)
        all_0.onward(k - 1)
    all_0.across(0)
    all_0.onward(3)
    for k in REST:
        all_0.across(k)
    all_1.end()
    all_0.end()


def class_sums(cls_t, three, sums):
    pick_t = (cls_t[...] == iota((len(sums), cls_t.shape[1]), 0)).astype(BF)
    hi, mid, lo = [dot32(pick_t, three[i]) for i in range(3)]
    sums[...] = hi + (mid + lo)


def last(r_in, ss, w_proj, cls_t, prev, tot_3, tot_2, n_dev):
    n_tok, dim = r_in.shape
    n_c, emb = prev.shape
    n = COLD_AT - HOT_AT + 2 * RUN
    vmem = pl.BlockSpec(memory_space=pltpu.VMEM)
    return pl.pallas_call(
        last_kernel,
        in_specs=[ANY, ANY, ANY] + [vmem] * 4, out_specs=[vmem, ANY],
        out_shape=[out_of((n_c, emb)), out_of((n_dev, 2 * n, emb))],
        scratch_shapes=[pltpu.VMEM((n_tok, dim), F32), pltpu.VMEM((n_tok, emb), BF), pltpu.VMEM((emb, dim), BF),
                        pltpu.VMEM((3, n_tok, emb), BF), pltpu.VMEM((2, n, emb), F32), pltpu.SemaphoreType.DMA((3,)),
                        SPREAD_SEMS, SPREAD_SEMS, FOLD_SEMS, FOLD_SEMS] + fold_bufs(emb) * 2,
        compiler_params=params(collective_id=2, has_side_effects=True),
        cost_estimate=cost(n_tok * dim * 4 * emb, 1), name="last",
    )(r_in, ss, w_proj, cls_t, prev, tot_3, tot_2)


ORDER = [(b & 3) * 8 + (b >> 2 & 1) * 4 + (b >> 3 & 1) * 2 + (b >> 4) for b in range(FREQ // RUN)]


def hot_kernel(skip, any_freq, raw, freq, code, into, out, parts):
    n_dev, n_r, _ = raw.shape
    layer, block = pl.program_id(0), pl.program_id(1)
    n = RUN * n_dev
    for g in range(n_r // RUN):
        for o in range(n_dev):
            out[0, pl.ds(g * n + o * RUN, RUN), :] = raw[o, pl.ds(g * RUN, RUN), :]

    @pl.when(any_freq[block] > 0)
    def _():
        for j in range(2):
            @pl.when(layer + skip == j)
            def _(j=j):
                rows = jnp.concatenate([freq[o, j * RUN:(j + 1) * RUN, :] for o in ORDER])
                for i, part in enumerate(split3(rows)):
                    parts[i] = part
        sel = (code[0] == iota((n_r * n_dev, FREQ), 1)).astype(BF)
        out[0] += dot32(sel, parts[0]) + (dot32(sel, parts[1]) + dot32(sel, parts[2]))


def hot_out(first, n_l, gathered, stride, freq_from, freq_at, skip, code, into):
    n_dev, _, emb = gathered.shape
    n_r = 2 * RUN
    width = n_r * n_dev
    blocks = into.shape[1] // width
    code = code.reshape(blocks, width, 1)
    return pl.pallas_call(
        functools.partial(hot_kernel, skip),
        grid_spec=pltpu.PrefetchScalarGridSpec(
            num_scalar_prefetch=1, grid=(n_l, blocks),
            in_specs=[
                pl.BlockSpec((n_dev, n_r, emb), lambda i, b, _: (0, i * stride + b, 0)),
                spec((n_dev, n_r, emb), 0, freq_at, 0, pipeline_mode=ONCE),
                pl.BlockSpec((1, width, 1), lambda i, b, _: (b, 0, 0)),
                ANY,
            ],
            out_specs=pl.BlockSpec((1, width, emb), lambda i, b, _: (first - i, b, 0)),
            scratch_shapes=[pltpu.VMEM((3, FREQ, emb), BF)]),
        out_shape=out_of(into.shape),
        input_output_aliases={4: 0},
        compiler_params=params("arbitrary", "arbitrary"),
        cost_estimate=cost(n_l * gathered.size * LO, n_l), name="hot_out",
    )((code[:, :, 0] >= 0).any(axis=1).astype(I32), gathered, freq_from, code, into)


def empty(shape):
    return pl.pallas_call(lambda out: None, out_specs=ANY, out_shape=out_of(shape), name="empty")()


def rows_kernel(numbers, row_of, *refs):
    srcs, (freq, into, out, stage, got, sem) = refs[:-6], refs[-6:]
    n_used, cold_row, cold_no = [numbers[i] for i in range(3)]
    n_l = len(srcs)

    def put(k, row):
        return pltpu.make_async_copy(stage.at[pl.ds(k, 1)], out.at[pl.ds(row, 1)], sem)

    @pl.loop(0, n_used)
    def _(k):
        for l, src in enumerate(srcs):
            stage[k, pl.ds(l, 1), :] = src[pl.ds(COLD_AT + k, 1), :]
        put(k, row_of[k]).start()

    @pl.when(cold_row >= 0)
    def _():
        n = freq.shape[1] // 2
        for j in range(2):
            c = pltpu.make_async_copy(freq.at[cold_no // RUN * 8 + 7, pl.ds(j * n + n - 8, 8)], got.at[j], sem)
            c.start()
            c.wait()
        for l in range(n_l):
            i = n_l - 1 - l
            stage[COLD_MAX, pl.ds(l, 1), :] = got[i // 2, pl.ds(i % 2 * RUN + cold_no % RUN, 1), :]
        put(COLD_MAX, cold_row).start()
        put(0, 0).wait()

    @pl.loop(0, n_used)
    def _(k):
        put(0, 0).wait()


def put_rows(numbers, row_of, srcs, freq, into):
    n_l = len(srcs)
    shape = srcs[0].shape
    emb = shape[-1]
    return pl.pallas_call(
        rows_kernel,
        grid_spec=pltpu.PrefetchScalarGridSpec(
            num_scalar_prefetch=2, grid=(1,),
            in_specs=[spec(shape)] * n_l + [ANY, ANY], out_specs=ANY,
            scratch_shapes=[pltpu.VMEM((COLD_MAX + 1, n_l, emb), F32), pltpu.VMEM((2, 8, emb), F32), pltpu.SemaphoreType.DMA(())]),
        out_shape=out_of(into.shape), input_output_aliases={n_l + 3: 0},
        compiler_params=params("arbitrary"), name="put_rows",
    )(numbers, row_of, *srcs, freq, into)


def down_sum(v):
    return jnp.sum(v, axis=0)


def beside(*v):
    return jnp.concatenate(v, axis=1)


def row_sum(v):
    return jnp.sum(v, axis=1)


def square(n):
    return iota((n, n), 0), iota((n, n), 1)


def prefix(v):
    r, c = square(len(v))
    return row_sum(jnp.where(r > c, row(v), 0))


def digits(ids, n_hi):
    return one_hot(ids >> HI_BITS, n_hi), one_hot(ids & (LO - 1), LO)


def look(hi_lo, *maps):
    hi, lo = hi_lo
    got = dot32(hi, beside(*maps))
    return [row_sum(got[:, i * LO:(i + 1) * LO] * lo.astype(F32)).astype(I32) for i in range(len(maps))]


def number(count, most):
    levels = jnp.array(LEVELS, F32)
    n_over = jnp.sum((count[:, :, None] >= levels).astype(F32), axis=(0, 1))
    flag = count >= jnp.min(jnp.where(n_over <= most, levels, jnp.inf))
    r, c = square(LO)
    in_row = dot32(flag.astype(BF), (r < c).astype(BF))
    return jnp.where(flag, in_row + col(prefix(row_sum(flag.astype(F32)))) + 1, 0)


def solution(mesh):
    n_dev = mesh.shape['emb']

    def body(token_ids, hot_ids, x_in, d_out, emb_table, hot_table, w_up, w_down, w_gate, w_proj):
        n_loc = len(token_ids)
        layers, rows_dev, emb_dim = emb_table.shape
        n_hot = len(hot_ids)
        places, hot_dev = n_loc // n_dev, n_hot // n_dev
        n_hi = -(-rows_dev * n_dev // (8 * LO)) * 8
        me = lax.axis_index('emb')
        hot_at, cold_at = FREQ, FREQ + hot_dev

        def exchange(v):
            return swap(v.reshape(n_dev, places, -1)).reshape(n_loc, -1)

        def prepare(got_class, hot_hi, hot_lo, row_used, cold_owner, freq_cold, freq_map, hot_table, by_row, move, d_out):
            (hot_f,) = look((hot_hi, hot_lo), freq_map)
            used_rank = prefix(row_used.astype(I32))
            at_rank = (row(used_rank) == iota((COLD_MAX, rows_dev), 0)) & row(row_used)
            row_of = row_sum(jnp.where(at_rank, iota((COLD_MAX, rows_dev), 1), 0))
            packed = pack_rows(row_of, by_row)
            mine_no = jnp.where(hot_owner == me, FREQ_HOT + hot_place, -1)
            hot_pick = (one_hot(hot_f - 1, FREQ_HOT + hot_dev) * col((hot_f <= FREQ_HOT).astype(BF)) + one_hot(mine_no, FREQ_HOT + hot_dev)).T
            hot_rows = [dot32(hot_pick, hot_table[i]).astype(BF) for i in range(layers)]
            table = jnp.stack([jnp.concatenate([
                hot_rows[i][:FREQ_HOT], dot32(one_hot(cold_owner, n_dev), freq_cold[:, i]).astype(BF),
                hot_rows[i][FREQ_HOT:], packed[:, i]]) for i in range(layers)])
            n_used = jnp.minimum(jnp.sum(row_used.astype(I32)), COLD_MAX)
            row_no = got_class - cold_at
            used_before = row_sum(jnp.where(row(row_used) & (iota((n_loc, rows_dev), 1) < col(row_no)), 1, 0))
            cls = jnp.where(row_no >= 0, cold_at + used_before, got_class)
            code = jnp.where(hot_f <= FREQ_HOT, hot_f - 1, -1)
            d_placed = dot32(move, d_out).astype(BF)
            return d_placed, table, cls, n_used, row_of, code

        count = count_ids(swap(jnp.broadcast_to(row(token_ids), (n_dev, n_loc))), n_hi)
        tok, hot = digits(token_ids, n_hi), digits(hot_ids, n_hi)
        slot_no = jnp.arange(n_hot, dtype=I32)
        hot_place = slot_no // (RUN * n_dev) * RUN + slot_no % RUN
        hot_owner = slot_no // RUN % n_dev
        q_map = dot32(hot[0].T, hot[1] * col((hot_place + 1).astype(BF))).astype(BF)
        r_map = dot32(hot[0].T, hot[1] * col(hot_owner.astype(BF))).astype(BF)
        hot_no = number(jnp.where(q_map > 0, count, 0), FREQ_HOT)
        cold_no = number(jnp.where(q_map > 0, 0, count), FREQ_COLD)
        freq_map = jnp.where(hot_no > 0, hot_no, jnp.where(cold_no > 0, FREQ_HOT + cold_no, 0)).astype(BF)
        id_map = iota((n_hi, LO), 0) * LO + iota((n_hi, LO), 1) + 1
        cold_id = jnp.sum(jnp.where(cold_no.astype(I32)[None] == iota((FREQ_COLD, 1, 1), 0) + 1, id_map[None], 0), axis=(1, 2)) - 1
        cold_owner = jnp.where(cold_id >= 0, cold_id // rows_dev, -1)
        my_cold = (cold_owner == me).astype(I32)
        my_row = jnp.minimum(jnp.sum(my_cold * (cold_id - me * rows_dev + 1)) - 1, rows_dev - 1)
        by_row = emb_table.transpose(1, 0, 2)
        cold_row = lax.dynamic_slice_in_dim(by_row, jnp.maximum(my_row, 0), 1)
        freq_cold = swap(jnp.broadcast_to(cold_row, (n_dev, layers, emb_dim)))

        tok_f, tok_q, tok_r = look(tok, freq_map, q_map, r_map)
        rare = tok_f == 0
        owner = jnp.where(tok_q > 0, tok_r, token_ids // rows_dev)
        dev_no = iota((n_loc, n_dev), 1)
        to_dev = (col(owner) == dev_no) & col(rare)
        marks = beside(to_dev.astype(BF), col(jnp.logical_not(rare).astype(BF)))
        r, c = square(n_loc)
        ranks = dot32((r > c).astype(BF), marks)
        sent = down_sum(to_dev.astype(F32))
        free = jnp.maximum(places - sent, 0)
        free_at = prefix(free)
        fill = ranks[:, n_dev:]
        fill_dev = (fill >= free_at) & (fill < free_at + free)
        to_dev = jnp.where(col(rare), to_dev, fill_dev)
        place = jnp.where(col(rare), ranks[:, :n_dev], fill + (sent - free_at))
        slot = row_sum(jnp.where(to_dev, dev_no * places + place.astype(I32), 0))
        row_ids = me * rows_dev + jnp.arange(rows_dev, dtype=I32)
        row_f, row_q, row_n = look(digits(row_ids, n_hi), freq_map, q_map, (count > 0).astype(BF))
        row_used = (row_n > 0) & (row_f == 0) & (row_q == 0)
        fits = ((jnp.max(sent) <= places) & (jnp.sum(row_used.astype(I32)) <= COLD_MAX) & (jnp.sum(my_cold) <= 1))
        tok_class = jnp.where(rare, jnp.where(tok_q > 0, hot_at + tok_q - 1, cold_at + token_ids % rows_dev), tok_f - 1)
        bad = 1 << 20
        move = r == row(slot)
        send_class, freq_cold = lax.optimization_barrier(
            (row_sum(jnp.where(move, row(tok_class), 0)) + jnp.where(fits, 0, bad), freq_cold))
        got_class = swap(send_class.reshape(n_dev, places)).reshape(n_loc)
        move = move.astype(BF)
        placed, got_class, hot_hi, hot_lo, row_used, cold_owner = lax.optimization_barrier(
            (dot32(move, x_in).astype(BF), got_class, *hot, row_used, cold_owner))
        x_moved = exchange(placed)
        given = prepare(got_class, hot_hi, hot_lo, row_used, cold_owner, freq_cold, freq_map, hot_table, by_row, move, d_out)
        all_fit = jnp.max(got_class) < bad

        def fast(x_moved, slot, my_cold, my_row, d_placed, table, cls, n_used, row_of, code):
            d_moved = exchange(d_placed)
            cls_row = cls.reshape(1, n_loc)
            xs, hs, ss, es, x_last, zeros = forward(x_moved, cls.reshape(n_loc, 1), table, w_up, w_down, w_gate, w_proj, rows_dev)
            x_back = exchange(x_last)
            kept = (cls_row, es, xs, hs, ss, w_up, w_down, w_gate, w_proj)
            sums_3, r = backward(3, d_moved, *kept)
            sums_2, r, all_3, tot_3 = backward(2, r, *kept, sums_3, n_dev)
            r, x_back = lax.optimization_barrier((r, x_back))
            sums_1, r, all_2, tot_2 = backward(1, r, *kept, sums_2, n_dev)
            sums_0, all_b = last(r, ss, w_proj, cls_row, sums_1, tot_3, tot_2, n_dev)
            x_out = dot32((col(slot) == iota((n_loc, n_loc), 1)).astype(BF), x_back).astype(BF)
            numbers = jnp.stack([n_used, my_row, jnp.sum(my_cold * jnp.arange(FREQ_COLD, dtype=I32))])
            d_table = put_rows(numbers, row_of, [sums_0, sums_1, sums_2, sums_3], all_b, zeros)
            at_freq = hot_dev // (2 * RUN)
            into = empty((layers, n_hot, emb_dim))
            into = hot_out(3, 1, all_3, 0, all_b, at_freq, 0, code, into)
            into = hot_out(2, 1, all_2, 0, all_b, at_freq, 1, code, into)
            into = hot_out(1, 2, all_b, at_freq + 1, all_b, 2 * at_freq + 1, 0, code, into)
            return x_out, d_table.transpose(1, 0, 2), into

        def slow(*_):
            return general_path(n_dev, me, token_ids, hot_ids, x_in, d_out, emb_table, hot_table, w_up, w_down, w_gate, w_proj)

        return lax.cond(all_fit, fast, slow, *lax.optimization_barrier((x_moved, slot, my_cold, my_row, *given)))

    return jax.shard_map(body, mesh=mesh,
                         in_specs=(P('emb'), P(), P('emb', None), P('emb', None), P(None, 'emb', None), P(), P(), P(), P(), P()),
                         out_specs=(P('emb', None), P(None, 'emb', None), P()),
                         check_vma=False)
```

```python
import functools

import jax
import jax.numpy as jnp
from jax import lax
from jax.experimental import pallas as pl
from jax.experimental.pallas import tpu as pltpu
from jax.sharding import PartitionSpec as P


NORM_EPS = 1e-6
FREQ_HOT = 124
FREQ_COLD = 4
FREQ = FREQ_HOT + FREQ_COLD
COLD_MAX = 256
LO = 256
HI_BITS = 8
RUN = 4
LEVELS = tuple(12 * 2 ** (i / 6) for i in range(27))
GELU_A = 0.7978845608028654
GELU_B = GELU_A * 0.044715
VMEM = 66_000_000
ROWS_A = 256
ROWS_B = 512
TILE = 1024
BF = jnp.bfloat16
F32 = jnp.float32
I32 = jnp.int32
ONCE = pl.Buffered(1)


def gelu_back(pre_act, cot_in):
    _, pull = jax.vjp(jax.nn.gelu, pre_act.astype(F32))
    return pull(cot_in)[0]


def swap(v):
    return lax.all_to_all(v, 'emb', 0, 0, tiled=True)


def col(v):
    return v[:, None]


def row(v):
    return v[None, :]


def dot32(a, b):
    return jnp.dot(a, b, preferred_element_type=F32)


def dense_parts(resid, w_up, w_gate):
    resid_f = resid.astype(F32)
    inv_rms = lax.rsqrt(jnp.mean(resid_f * resid_f, axis=-1, keepdims=True) + NORM_EPS)
    normed = (resid_f * inv_rms).astype(BF)
    hidden = dot32(normed, w_up).astype(BF)
    gate_pre = dot32(normed, w_gate).astype(BF)
    return resid_f, inv_rms, hidden, gate_pre


def layer_forward(resid, emb_rows, w_up, w_down, w_gate, w_proj):
    resid_f, _, hidden, gate_pre = dense_parts(resid, w_up, w_gate)
    activated = jax.nn.gelu(hidden.astype(F32)).astype(BF)
    mlp_out = dot32(activated, w_down).astype(BF)
    gate = jax.nn.gelu(gate_pre.astype(F32)).astype(BF)
    mixed = (gate.astype(F32) * emb_rows.astype(F32)).astype(BF)
    projected = dot32(mixed, w_proj).astype(BF)
    return (resid_f + mlp_out.astype(F32) + projected.astype(F32)).astype(BF)


def layer_backward(resid, emb_rows, d_next, w_up, w_down, w_gate, w_proj):
    resid_f, inv_rms, hidden, gate_pre = dense_parts(resid, w_up, w_gate)
    gate = jax.nn.gelu(gate_pre.astype(F32)).astype(BF)
    d_cast = d_next.astype(BF)
    d_mixed = jnp.einsum('nd,ed->ne', d_cast, w_proj, preferred_element_type=F32)
    d_rows = gate.astype(F32) * d_mixed
    d_gpre = gelu_back(gate_pre, d_mixed * emb_rows.astype(F32))
    d_hidden = gelu_back(hidden, jnp.einsum('nd,fd->nf', d_cast, w_down, preferred_element_type=F32))
    d_normed = (jnp.einsum('nf,df->nd', d_hidden.astype(BF), w_up, preferred_element_type=F32)
                + jnp.einsum('ne,de->nd', d_gpre.astype(BF), w_gate, preferred_element_type=F32))
    inner = jnp.mean(d_normed * resid_f, axis=-1, keepdims=True)
    d_prev = d_next + inv_rms * d_normed - resid_f * (inv_rms * inv_rms * inv_rms) * inner
    return d_prev, d_rows


def general_path(n_dev, my_index, token_ids, hot_ids, x_in, d_out, emb_table, hot_table, w_up, w_down, w_gate, w_proj):
    n_loc = token_ids.shape[0]
    _, rows_dev, emb_dim = emb_table.shape
    capacity = max(8, (2 * n_loc) // n_dev)
    n_slots = n_dev * capacity
    hot_match = col(token_ids) == row(hot_ids)
    is_hot = hot_match.any(1)
    hot_pick = hot_match.astype(BF)
    hot_pick_f = hot_match.astype(F32)
    owner_id = token_ids // rows_dev
    to_owner = (col(owner_id) == row(jnp.arange(n_dev, dtype=I32))) & col(jnp.logical_not(is_hot))
    owner_rank = jnp.cumsum(to_owner.astype(jnp.int32), axis=0) - 1
    place = row_sum(jnp.where(to_owner, owner_rank, 0))
    slot = jnp.where(is_hot, n_slots, owner_id * capacity + place)
    none = jnp.full((n_slots,), -1, I32)
    send_ids = none.at[slot].set(token_ids, mode='drop')
    slot_tok = none.at[slot].set(jnp.arange(n_loc, dtype=jnp.int32), mode='drop')
    recv_ids = swap(send_ids.reshape(n_dev, capacity)).reshape(n_slots)
    served_ok = recv_ids >= 0
    local_row = jnp.where(served_ok, recv_ids - my_index * rows_dev, 0)
    pick_slot = jnp.minimum(slot, n_slots - 1)
    slot_used = slot_tok >= 0
    slot_src = jnp.maximum(slot_tok, 0)

    def fwd(resid, per_layer):
        table, hot_l, up, down, gate_w, proj = per_layer
        served = table[local_row]
        fetched = swap(served.reshape(n_dev, capacity, emb_dim)).reshape(n_slots, emb_dim)
        cold_rows = fetched[pick_slot]
        hot_rows = dot32(hot_pick, hot_l).astype(BF)
        emb_rows = jnp.where(col(is_hot), hot_rows, cold_rows)
        return layer_forward(resid, emb_rows, up, down, gate_w, proj), (resid, emb_rows)

    x_out, (x_saved, rows_saved) = lax.scan(fwd, x_in, (emb_table, hot_table, w_up, w_down, w_gate, w_proj))

    def bwd(d_resid, per_layer):
        resid_l, rows_l, up, down, gate_w, proj = per_layer
        d_resid, d_rows = layer_backward(resid_l, rows_l, d_resid, up, down, gate_w, proj)
        outgoing = jnp.where(col(slot_used), d_rows[slot_src], 0.0)
        incoming = swap(outgoing.reshape(n_dev, capacity, emb_dim)).reshape(n_slots, emb_dim)
        d_tab = jax.ops.segment_sum(jnp.where(col(served_ok), incoming, 0.0), local_row, num_segments=rows_dev)
        hot_local = jnp.einsum('nh,ne->he', hot_pick_f, d_rows, precision=lax.Precision.HIGHEST, preferred_element_type=F32)
        return d_resid, (d_tab, lax.psum(hot_local, 'emb'))

    _, (d_table, d_hot) = lax.scan(bwd, d_out.astype(F32), (x_saved, rows_saved, w_up, w_down, w_gate, w_proj), reverse=True)
    return x_out, d_table, d_hot


def split3(v):
    hi = v.astype(BF)
    rest = v - hi.astype(F32)
    mid = rest.astype(BF)
    return hi, mid, (rest - mid.astype(F32)).astype(BF)


def iota(shape, dim):
    return lax.broadcasted_iota(jnp.int32, shape, dim)


def one_hot(v, n, dtype=BF):
    return (col(v) == iota((len(v), n), 1)).astype(dtype)


def dot_nt(a, b):
    return lax.dot_general(a, b, (((1,), (1,)), ((), ())), preferred_element_type=F32)


def gelu(x):
    half = 0.5 * x
    return half + half * jnp.tanh(x * (GELU_A + GELU_B * (x * x)))


def gelu_slope(x):
    sq = x * x
    th = jnp.tanh(x * (GELU_A + GELU_B * sq))
    return (0.5 + 0.5 * th) + (0.5 * x) * (1.0 - th * th) * (GELU_A + (3.0 * GELU_B) * sq)


def forward_kernel(n_l, n_f, x0, cls, table, wu, wd, wg, wp, xs, hs, ss, es, xo, zeros, x_now, u_now, acc, q_now, blank, sem):
    layer, step = pl.program_id(0), pl.program_id(1)
    n_tok = x_now.shape[0]
    n_blank = blank.shape[0]
    blanks = [pltpu.make_async_copy(blank, zeros.at[pl.ds(i, n_blank)], sem) for i in range(0, zeros.shape[0], n_blank)]

    @pl.when((layer == 0) & (step == n_f - 1))
    def _():
        blank[...] = jnp.zeros(blank.shape, F32)
        for b in blanks:
            b.start()

    @pl.when((layer == n_l - 1) & (step == n_f - 1))
    def _():
        for b in blanks:
            b.wait()


    @pl.when((layer == 0) & (step == 0))
    def _():
        x_now[...] = x0[...]

    @pl.when(step == 0)
    def _():
        for m in chunks(n_tok, ROWS_A):
            xb = x_now[m, :]
            x = xb.astype(F32)
            xs[m, :] = xb
            u = (x * lax.rsqrt(jnp.mean(x * x, axis=-1, keepdims=True) + NORM_EPS)).astype(BF)
            u_now[m, :] = u
            s = dot32(u, wg[...]).astype(BF)
            ss[m, :] = s
            g = gelu(s.astype(F32)).astype(BF)
            pick = (cls[m, :] == iota((m.size, table.shape[0]), 1)).astype(BF)
            e = dot32(pick, table[...]).astype(BF)
            es[m, :] = e
            mixed = (g.astype(F32) * e.astype(F32)).astype(BF)
            q_now[m, :] = dot32(mixed, wp[...]).astype(BF)
            acc[m, :] = jnp.zeros((m.size, acc.shape[1]), F32)

    for m in chunks(n_tok, ROWS_B):
        h = dot32(u_now[m, :], wu[...]).astype(BF)
        hs[m, :] = h
        acc[m, :] += dot32(gelu(h.astype(F32)).astype(BF), wd[...])

    @pl.when(step == n_f - 1)
    def _():
        for m in chunks(n_tok, ROWS_A):
            x = x_now[m, :].astype(F32) + acc[m, :].astype(BF).astype(F32) + q_now[m, :].astype(F32)
            x_now[m, :] = x.astype(BF)

    @pl.when((step == n_f - 1) & (layer == n_l - 1))
    def _():
        xo[...] = x_now[...]


def chunks(n, size):
    size = min(n, size)
    return [pl.ds(m, size) for m in range(0, n, size)]


def forward(x0, cls, table, w_up, w_down, w_gate, w_proj, rows_dev):
    n_tok, dim = x0.shape
    n_l, _, ff = w_up.shape
    emb = w_gate.shape[2]
    tile = min(TILE, ff)
    n_f = ff // tile
    n_c = table.shape[1]

    def whole(l, f):
        return (l, 0, 0)

    def cols(l, f):
        return (l, 0, f)

    def fixed(l, f):
        return (0, 0)

    return pl.pallas_call(
        functools.partial(forward_kernel, n_l, n_f),
        grid=(n_l, n_f),
        in_specs=[
            pl.BlockSpec((n_tok, dim), fixed, pipeline_mode=ONCE),
            pl.BlockSpec((n_tok, 1), fixed, pipeline_mode=ONCE),
            pl.BlockSpec((None, n_c, emb), whole),
            pl.BlockSpec((None, dim, tile), cols),
            pl.BlockSpec((None, tile, dim), lambda l, f: (l, f, 0)),
            pl.BlockSpec((None, dim, emb), whole),
            pl.BlockSpec((None, emb, dim), whole),
        ],
        out_specs=[
            pl.BlockSpec((None, n_tok, dim), whole),
            pl.BlockSpec((None, n_tok, tile), cols),
            pl.BlockSpec((None, n_tok, emb), whole),
            pl.BlockSpec((None, n_tok, emb), whole),
            pl.BlockSpec((n_tok, dim), fixed),
            ANY,
        ],
        out_shape=[out_of((n_l, n_tok, n), BF) for n in (dim, ff, emb, emb)] + [out_of((n_tok, dim), BF), out_of((rows_dev, n_l, emb))],
        scratch_shapes=[pltpu.VMEM((n_tok, dim), t) for t in (BF, BF, F32, BF)]
        + [pltpu.VMEM((rows_dev // 12, n_l, emb), F32), pltpu.SemaphoreType.DMA(())],
        compiler_params=params("arbitrary", "arbitrary"),
        cost_estimate=cost(n_l * n_tok * dim * (2 * ff + 2 * emb + n_c), n_l),
        name="forward",
    )(x0, cls, table, w_up, w_down, w_gate, w_proj)


def params(*kinds, **more):
    return pltpu.CompilerParams(vmem_limit_bytes=VMEM, dimension_semantics=kinds or None, **more)


def cost(products, layers):
    return pl.CostEstimate(flops=2 * products, bytes_accessed=layers * 40_000_000, transcendentals=0)


def spec(shape, *index, **more):
    index = index or (0,) * len(shape)
    return pl.BlockSpec(shape, lambda *_: index, **more)


ANY = pl.BlockSpec(memory_space=pl.ANY)


def out_of(shape, dtype=F32):
    return jax.ShapeDtypeStruct(shape, dtype)


def backward_kernel(n_f, r_in, ss, wp, es, wg, xs, cls_t, hs, wu, wd, *refs):
    prev, refs = (refs[0], refs[1:]) if len(refs) > 20 else (None, refs)
    sums, r, tot, out, refs = (*refs[:3], refs[3], refs[4:]) if prev is not None else (*refs[:3], None, refs[3:])
    c_now, acc, three, s_now, p_now, e_now, g_now, x_now, loads, sems, sems_f, *bufs = refs
    f = pl.program_id(0)
    n_tok = len(c_now)
    at = Place()
    gather = None if prev is None else Spread(at, prev.at[pl.ds(HOT_AT, COLD_AT - HOT_AT)], lambda d: out.at[d], sems)
    fold = Fold(at, sums.at[pl.ds(0, FREQ)], bufs, sems_f)
    rounded = r_in.dtype == BF
    srcs = (wp, p_now), (r_in, c_now if rounded else r), (ss, s_now), (es, e_now), (wg, g_now), (xs, x_now)
    copies = [pltpu.make_async_copy(src, dst, loads.at[i]) for i, (src, dst) in enumerate(srcs)]

    def talk(*steps):
        if gather is not None:
            for name, k in steps:
                getattr(gather, name)(k)

    @pl.when(f == 0)
    def _():
        for c in copies:
            c.start()
        at.meet()
        talk(("begin", 0))
        for c in copies[:-1]:
            c.wait()
        for m in chunks(n_tok, ROWS_B):
            if rounded:
                r[m, :] = c_now[m, :].astype(F32)
            else:
                c_now[m, :] = r[m, :].astype(BF)
            a = dot_nt(c_now[m, :], p_now[...])
            s = s_now[m, :].astype(F32)
            rows = gelu(s).astype(BF).astype(F32) * a
            for j, part in enumerate(split3(rows)):
                three[j, m, :] = part
            ds = (gelu_slope(s) * (a * e_now[m, :].astype(F32))).astype(BF)
            acc[m, :] = dot_nt(ds, g_now[...])
        talk(("onward", 0))
        class_sums(cls_t, three, sums)
        fold.begin()
        talk(("column", 1))

    plan = {(0, 1): (("onward", 1), ("column", 2)), (1, 0): (("column", 3),), (1, 1): (("onward", 2),),
            (2, 0): (("across", 0), ("onward", 3)), (2, 1): (("across", 1),), (3, 0): (("across", 2),)}
    for i, m in enumerate(chunks(n_tok, ROWS_B)):
        d_act = dot_nt(c_now[m, :], wd[...])
        dh = (gelu_slope(hs[m, :].astype(F32)) * d_act).astype(BF)
        acc[m, :] += dot_nt(dh, wu[...])
        for k in range(n_f):
            @pl.when(f == k)
            def _(k=k, i=i):
                if i and k < 3:
                    fold.step(k)
                talk(*plan.get((k, i), ()))

    @pl.when(f == n_f - 1)
    def _():
        copies[-1].wait()
        for m in chunks(n_tok, ROWS_A):
            x = x_now[m, :].astype(F32)
            k = lax.rsqrt(jnp.mean(x * x, axis=-1, keepdims=True) + NORM_EPS)
            du = acc[m, :]
            inner = jnp.mean(du * x, axis=-1, keepdims=True)
            r[m, :] = r[m, :] + k * du - x * (k * k * k) * inner
        tot[...] = fold.total()
        talk(("across", 3), ("end", 0))


def backward(layer, r_in, cls_t, es, xs, hs, ss, w_up, w_down, w_gate, w_proj, n_dev, prev=None):
    n_tok, dim = r_in.shape
    ff = w_up.shape[2]
    emb = w_gate.shape[2]
    n_c = COLD_AT + COLD_MAX
    n_f = 4
    tile = ff // n_f
    more = prev is not None

    def cols(n):
        return pl.BlockSpec((None, n, tile), lambda t: (layer, 0, t))

    def kernel(r_in, ss, wp, es, wg, xs, *refs):
        backward_kernel(n_f, r_in, *[v.at[layer] for v in (ss, wp, es, wg, xs)], *refs)

    return pl.pallas_call(
        kernel,
        grid=(n_f,),
        in_specs=[ANY] * 6 + [spec((1, n_tok)), cols(n_tok), cols(dim), pl.BlockSpec((None, tile, dim), lambda t: (layer, t, 0))]
        + [spec((n_c, emb), pipeline_mode=ONCE)] * more,
        out_specs=[spec((n_c, emb)), spec((n_tok, dim)), spec((16, emb))] + [ANY] * more,
        out_shape=[out_of((n_c, emb)), out_of((n_tok, dim)), out_of((16, emb))] + [out_of((n_dev, COLD_AT - HOT_AT, emb))] * more,
        scratch_shapes=[pltpu.VMEM((n_tok, dim), BF), pltpu.VMEM((n_tok, dim), F32), pltpu.VMEM((3, n_tok, emb), BF)]
        + [pltpu.VMEM(v, BF) for v in ((n_tok, emb), (emb, dim), (n_tok, emb), (dim, emb), (n_tok, dim))]
        + [pltpu.SemaphoreType.DMA((6,)), SPREAD_SEMS, FOLD_SEMS] + fold_bufs(emb),
        compiler_params=params("arbitrary", collective_id=layer, has_side_effects=True),
        cost_estimate=cost(n_tok * dim * (2 * ff + 2 * emb + 3 * n_c), 1),
        name="backward",
    )(r_in, ss, w_proj, es, w_gate, xs, cls_t, hs, w_up, w_down, *([prev] if more else []))


def count_kernel(ids, out):
    n_tok = ids.shape[1]
    out[...] = jnp.zeros(out.shape, F32)

    def hits(v, n):
        same = v.astype(F32).astype(BF) == iota((n, n_tok), 0).astype(F32).astype(BF)
        return jnp.where(same, jnp.ones((), BF), jnp.zeros((), BF))

    @pl.loop(0, len(ids))
    def _(i):
        ids_i = ids[pl.ds(i, 1), :]
        out[...] += dot_nt(hits(ids_i >> HI_BITS, len(out)), hits(ids_i & (LO - 1), LO))


def count_ids(ids, n_hi):
    return pl.pallas_call(count_kernel, out_shape=out_of((n_hi, LO)), compiler_params=params(), name="count_ids")(ids)


def pack_kernel(row_of, table, out, sem):
    @pl.loop(0, len(out))
    def _(k):
        pltpu.make_async_copy(table.at[row_of[k]], out.at[k], sem).start()

    pltpu.make_async_copy(table.at[pl.ds(0, len(out))], out, sem).wait()


def pack_rows(row_of, table):
    shape = row_of.shape + table.shape[1:]
    return pl.pallas_call(
        pack_kernel,
        grid_spec=pltpu.PrefetchScalarGridSpec(num_scalar_prefetch=1, grid=(1,), in_specs=[ANY], out_specs=spec(shape),
                                               scratch_shapes=[pltpu.SemaphoreType.DMA(())]),
        out_shape=out_of(shape, table.dtype), compiler_params=params(), name="pack_rows",
    )(row_of, table)


class Place:
    def __init__(self):
        me = lax.axis_index('emb')
        self.core, self.x, self.y, self.z = me % 2, (me // 2) % 2, (me // 4) % 2, me // 8
        self.others = [self.dev(z=(self.z + k) % 4) for k in REST]
        self.columns = [(self.z - k + 4) % 4 for k in STOPS]
        self.to_x, self.to_y, self.to_core = self.dev(x=1 - self.x), self.dev(y=1 - self.y), self.dev(core=1 - self.core)

    def dev(self, z=None, y=None, x=None, core=None):
        z, y, x, core = [mine if v is None else v for v, mine in ((z, self.z), (y, self.y), (x, self.x), (core, self.core))]
        return ((z * 2 + y) * 2 + x) * 2 + core

    def meet(self):
        barrier = pltpu.get_barrier_semaphore()
        peers = self.others + [self.to_x, self.to_y, self.to_core]
        for peer in peers:
            pl.semaphore_signal(barrier, device_id=(peer,), device_id_type=pl.DeviceIdType.MESH)
        pl.semaphore_wait(barrier, len(peers))


def remote(src, dst, sems, to):
    return pltpu.make_async_remote_copy(src_ref=src, dst_ref=dst, send_sem=sems[0], recv_sem=sems[1],
                                        device_id=(to,), device_id_type=pl.DeviceIdType.MESH)


Z, X, Y, FX, FY, C, CX, CY, CD, OWN = range(10)


class Spread:
    def __init__(self, at, mine, slot, sems):
        self.at, self.mine, self.slot, self.sems = at, mine, slot, sems
        n = mine.shape[0]
        half = n // 16 * 8
        self.halves = {FY: pl.ds(0, half), FX: pl.ds(half, n - half)}
        self.col = [at.dev(z=z) for z in at.columns]
        self.by_x = [at.dev(z=z, x=1 - at.x) for z in at.columns]
        self.by_y = [at.dev(z=z, y=1 - at.y) for z in at.columns]
        self.by_d = [at.dev(z=z, x=1 - at.x, y=1 - at.y) for z in at.columns]
        self.far = [[at.dev(z=z, x=x, y=y, core=1 - at.core) for z in at.columns]
                    for y, x in ((at.y, at.x), (at.y, 1 - at.x), (1 - at.y, at.x), (1 - at.y, 1 - at.x))]
        self.done = []

    def pair(self, kind, k):
        return self.sems.at[0, kind, k], self.sems.at[1, kind, k]

    def send(self, kind, k, src, dst, to):
        remote(src, dst, self.pair(kind, k), to).start()
        self.done.append((kind, k))

    def got(self, kind, k, block):
        remote(block, block, self.pair(kind, k), self.at.to_x).wait_recv()

    def begin(self, _=None):
        own = self.slot(self.col[0])
        pltpu.make_async_copy(self.mine, own, self.sems.at[0, OWN, 0]).start()
        for k, other in enumerate(self.at.others):
            self.send(Z, k + 1, self.mine, own, other)
        self.column(0)

    def column(self, k):
        block = self.slot(self.col[k])
        if k:
            self.got(Z, k, block)
        src = block if k else self.mine
        for kind, to in ((X, self.at.to_x), (Y, self.at.to_y), (C, self.at.to_core)):
            self.send(kind, k, src, block, to)

    def onward(self, k):
        for kind, part, to, other, core in ((X, self.by_x, self.at.to_y, FY, CX), (Y, self.by_y, self.at.to_x, FX, CY)):
            block = self.slot(part[k])
            self.got(kind, k, block)
            half = block.at[self.halves[other]]
            self.send(other, k, half, half, to)
            self.send(core, k, block, block, self.at.to_core)

    def across(self, k):
        block = self.slot(self.by_d[k])
        for kind, half in self.halves.items():
            self.got(kind, k, block.at[half])
        self.send(CD, k, block, block, self.at.to_core)

    def end(self, _=None):
        for k in STOPS:
            for kind, far in zip((C, CX, CY, CD), self.far):
                self.got(kind, k, self.slot(far[k]))
        own = self.slot(self.col[0])
        for kind, k in self.done:
            block = own.at[self.halves[kind]] if kind in self.halves else own
            remote(block, block, self.pair(kind, k), self.at.to_x).wait_send()
        pltpu.make_async_copy(self.mine, own, self.sems.at[0, OWN, 0]).wait()


class Fold:
    def __init__(self, at, part, bufs, sems):
        self.at, self.part, self.sems = at, part, sems
        self.ins, self.sums, self.all_z = bufs[:3], bufs[3:5], bufs[5]
        self.bits = at.core, at.x, at.y
        self.to = at.to_core, at.to_x, at.to_y

    def pair(self, i, k=0):
        return self.sems.at[0, i, k], self.sems.at[1, i, k]

    def cut(self, i, bit):
        n = self.ins[i].shape[0]
        return pl.ds(pl.multiple_of(bit * n, n), n)

    def source(self, i):
        return self.sums[i - 1] if i else self.part

    def hop(self, i):
        return remote(self.source(i).at[self.cut(i, 1 - self.bits[i])], self.ins[i], self.pair(i), self.to[i])

    def begin(self):
        self.hop(0).start()

    def step(self, i):
        self.hop(i).wait_recv()
        total = self.source(i)[self.cut(i, self.bits[i]), :] + self.ins[i][...]
        if i < 2:
            self.sums[i][...] = total
            self.hop(i + 1).start()
        else:
            self.all_z[self.at.z] = total
            for k, other in enumerate(self.at.others):
                self.along_z(k, other).start()

    def along_z(self, k, other):
        block = self.all_z.at[self.at.z]
        return remote(block, block, self.pair(3, k), other)

    def total(self):
        for k, other in enumerate(self.at.others):
            self.along_z(k, other).wait_recv()
        for i in range(3):
            self.hop(i).wait_send()
        for k, other in enumerate(self.at.others):
            self.along_z(k, other).wait_send()
        v = self.all_z
        return (v[0] + v[1]) + (v[2] + v[3])


def fold_bufs(emb):
    return [pltpu.VMEM((n, emb), F32) for n in (64, 32, 16, 64, 32)] + [pltpu.VMEM((4, 16, emb), F32)]


SPREAD_SEMS = pltpu.SemaphoreType.DMA((2, 10, 4))
STOPS = range(4)
REST = STOPS[1:]
FOLD_SEMS = pltpu.SemaphoreType.DMA((2, 4, 4))
HOT_AT, COLD_AT = FREQ, FREQ + 64


def last_kernel(r_in, ss, wp, cls_t, prev, *refs):
    early, (sums, out, r, s, w, three, pay, loads, sems_1, sems_0, sems_f, *bufs) = refs[:3], refs[3:]
    n_hot = COLD_AT - HOT_AT
    n = pay.shape[1]
    copies = [pltpu.make_async_copy(src, dst, loads.at[i]) for i, (src, dst) in enumerate(((r_in, r), (ss.at[0], s), (wp.at[0], w)))]
    for c in copies:
        c.start()
    at = Place()
    at.meet()

    def fill(i, hot, totals):
        pay[i, pl.ds(0, n_hot), :] = hot
        for z in STOPS:
            @pl.when(at.z == z)
            def _(z=z):
                for j, t in enumerate(totals):
                    pay[i, pl.ds(n_hot + RUN * j, RUN), :] = t[z * RUN:(z + 1) * RUN, :]

    fold = Fold(at, sums.at[pl.ds(0, FREQ)], bufs, sems_f)
    all_1, all_0 = [Spread(at, pay.at[i], lambda d, i=i: out.at[d, pl.ds(STRIDE * i, n)], sems) for i, sems in enumerate((sems_1, sems_0))]
    fill(0, prev[pl.ds(HOT_AT, n_hot), :], [t[...] for t in early[:2]])
    all_1.begin()
    for c in copies:
        c.wait()
    for m in chunks(len(r), ROWS_B):
        a = dot_nt(r[m, :].astype(BF), w[...])
        rows = gelu(s[m, :].astype(F32)).astype(BF).astype(F32) * a
        for i, part in enumerate(split3(rows)):
            three[i, m, :] = part
    all_1.onward(0)
    class_sums(cls_t, three, sums)
    fold.begin()
    all_1.column(1)
    for k in REST:
        fold.step(k - 1)
        all_1.onward(k)
        if k < REST[-1]:
            all_1.column(k + 1)
    all_1.across(0)
    fill(1, sums[pl.ds(HOT_AT, n_hot), :], [early[2][...], fold.total()])
    all_0.begin()
    for k in REST:
        all_1.across(k)
        all_0.onward(k - 1)
        all_0.column(k)
    all_0.across(0)
    all_0.onward(REST[-1])
    for k in REST:
        all_0.across(k)
    all_1.end()
    all_0.end()


def class_sums(cls_t, three, sums):
    pick_t = (cls_t[...] == iota((len(sums), cls_t.shape[1]), 0)).astype(BF)
    hi, mid, lo = [dot32(pick_t, three[i]) for i in range(3)]
    sums[...] = hi + (mid + lo)


STRIDE = 80


def last(r_in, ss, w_proj, cls_t, prev, tots, n_dev):
    n_tok, dim = r_in.shape
    n_c, emb = prev.shape
    n = COLD_AT - HOT_AT + 2 * RUN
    vmem = pl.BlockSpec(memory_space=pltpu.VMEM)
    return pl.pallas_call(
        last_kernel,
        in_specs=[ANY] * 3 + [vmem] * (2 + len(tots)), out_specs=[vmem, ANY],
        out_shape=[out_of((n_c, emb)), out_of((n_dev, 2 * STRIDE, emb))],
        scratch_shapes=[pltpu.VMEM((n_tok, dim), F32), pltpu.VMEM((n_tok, emb), BF), pltpu.VMEM((emb, dim), BF),
                        pltpu.VMEM((3, n_tok, emb), BF), pltpu.VMEM((2, n, emb), F32), pltpu.SemaphoreType.DMA((3,)),
                        SPREAD_SEMS, SPREAD_SEMS, FOLD_SEMS] + fold_bufs(emb),
        compiler_params=params(collective_id=0, has_side_effects=True),
        cost_estimate=cost(n_tok * dim * 4 * emb, 1), name="last",
    )(r_in, ss, w_proj, cls_t, prev, *tots)


ORDER = [(b & 3) * 8 + (b >> 2 & 1) * 4 + (b >> 3 & 1) * 2 + (b >> 4) for b in range(FREQ // RUN)]


def hot_kernel(skip, any_freq, raw, freq, code, into, out, parts):
    n_dev, n_r, _ = raw.shape
    layer, block = pl.program_id(0), pl.program_id(1)
    n = RUN * n_dev
    for g in range(n_r // RUN):
        for o in range(n_dev):
            out[0, pl.ds(g * n + o * RUN, RUN), :] = raw[o, pl.ds(g * RUN, RUN), :]

    @pl.when(any_freq[block] > 0)
    def _():
        for j in range(2):
            @pl.when(layer + skip == j)
            def _(j=j):
                rows = jnp.concatenate([freq[o, j * RUN:(j + 1) * RUN, :] for o in ORDER])
                for i, part in enumerate(split3(rows)):
                    parts[i] = part
        sel = (code[0] == iota((n_r * n_dev, FREQ), 1)).astype(BF)
        out[0] += dot32(sel, parts[0]) + (dot32(sel, parts[1]) + dot32(sel, parts[2]))


def hot_out(first, n_l, gathered, freq_from, freq_at, skip, code, into):
    n_dev, _, emb = gathered.shape
    n_r = 4 * RUN
    width = n_r * n_dev
    blocks = into.shape[1] // width
    code = code.reshape(blocks, width, 1)
    return pl.pallas_call(
        functools.partial(hot_kernel, skip),
        grid_spec=pltpu.PrefetchScalarGridSpec(
            num_scalar_prefetch=1, grid=(n_l, blocks),
            in_specs=[
                pl.BlockSpec((n_dev, n_r, emb), lambda i, b, _: (0, i * (STRIDE // n_r) + b, 0)),
                spec((n_dev, 2 * RUN, emb), 0, freq_at, 0, pipeline_mode=ONCE),
                pl.BlockSpec((1, width, 1), lambda i, b, _: (b, 0, 0)),
                ANY,
            ],
            out_specs=pl.BlockSpec((1, width, emb), lambda i, b, _: (first - i, b, 0)),
            scratch_shapes=[pltpu.VMEM((3, FREQ, emb), BF)]),
        out_shape=out_of(into.shape),
        input_output_aliases={4: 0},
        compiler_params=params("arbitrary", "arbitrary"),
        cost_estimate=cost(n_l * gathered.size * LO, n_l), name="hot_out",
    )((code[:, :, 0] >= 0).any(axis=1).astype(I32), gathered, freq_from, code, into)


def empty(shape):
    return pl.pallas_call(lambda out: None, out_specs=ANY, out_shape=out_of(shape), name="empty")()


def rows_kernel(numbers, row_of, *refs):
    srcs, (freq, into, out, stage, got, sem) = refs[:-6], refs[-6:]
    n_used, cold_row, cold_no = [numbers[i] for i in range(3)]
    n_l = len(srcs)

    def put(k, row):
        return pltpu.make_async_copy(stage.at[pl.ds(k, 1)], out.at[pl.ds(row, 1)], sem)

    @pl.loop(0, n_used)
    def _(k):
        for l, src in enumerate(srcs):
            stage[k, pl.ds(l, 1), :] = src[pl.ds(COLD_AT + k, 1), :]
        put(k, row_of[k]).start()

    @pl.when(cold_row >= 0)
    def _():
        for j in range(2):
            c = pltpu.make_async_copy(freq.at[len(freq) - 1, pl.ds(j * STRIDE + COLD_AT - HOT_AT, 8)], got.at[j], sem)
            c.start()
            c.wait()
        for l in range(n_l):
            i = n_l - 1 - l
            stage[COLD_MAX, pl.ds(l, 1), :] = got[i // 2, pl.ds(i % 2 * RUN + cold_no, 1), :]
        put(COLD_MAX, cold_row).start()
        put(0, 0).wait()

    @pl.loop(0, n_used)
    def _(k):
        put(0, 0).wait()


def put_rows(numbers, row_of, srcs, freq, into):
    n_l = len(srcs)
    shape = srcs[0].shape
    emb = shape[-1]
    return pl.pallas_call(
        rows_kernel,
        grid_spec=pltpu.PrefetchScalarGridSpec(
            num_scalar_prefetch=2, grid=(1,),
            in_specs=[spec(shape)] * n_l + [ANY, ANY], out_specs=ANY,
            scratch_shapes=[pltpu.VMEM((COLD_MAX + 1, n_l, emb), F32), pltpu.VMEM((2, 8, emb), F32), pltpu.SemaphoreType.DMA(())]),
        out_shape=out_of(into.shape), input_output_aliases={n_l + 3: 0},
        compiler_params=params("arbitrary"), name="put_rows",
    )(numbers, row_of, *srcs, freq, into)


def down_sum(v):
    return jnp.sum(v, axis=0)


def beside(*v):
    return jnp.concatenate(v, axis=1)


def row_sum(v):
    return jnp.sum(v, axis=1)


def square(n):
    return iota((n, n), 0), iota((n, n), 1)


def prefix(v):
    r, c = square(len(v))
    return row_sum(jnp.where(r > c, row(v), 0))


def digits(ids, n_hi):
    return one_hot(ids >> HI_BITS, n_hi), one_hot(ids & (LO - 1), LO)


def look(hi_lo, *maps):
    hi, lo = hi_lo
    got = dot32(hi, beside(*maps))
    return [row_sum(got[:, i * LO:(i + 1) * LO] * lo.astype(F32)).astype(I32) for i in range(len(maps))]


def number(count, most):
    levels = jnp.array(LEVELS, F32)
    n_over = jnp.sum((count[:, :, None] >= levels).astype(F32), axis=(0, 1))
    flag = count >= jnp.min(jnp.where(n_over <= most, levels, jnp.inf))
    r, c = square(LO)
    in_row = dot32(flag.astype(BF), (r < c).astype(BF))
    return jnp.where(flag, in_row + col(prefix(row_sum(flag.astype(F32)))) + 1, 0)


def solution(mesh):
    n_dev = mesh.shape['emb']

    def body(token_ids, hot_ids, x_in, d_out, emb_table, hot_table, w_up, w_down, w_gate, w_proj):
        n_loc = len(token_ids)
        layers, rows_dev, emb_dim = emb_table.shape
        n_hot = len(hot_ids)
        places, hot_dev = n_loc // n_dev, n_hot // n_dev
        n_hi = -(-rows_dev * n_dev // (8 * LO)) * 8
        me = lax.axis_index('emb')
        hot_at, cold_at = FREQ, FREQ + hot_dev

        def exchange(v):
            return swap(v.reshape(n_dev, places, -1)).reshape(n_loc, -1)

        def prepare(got_class, hot_hi, hot_lo, row_used, cold_owner, freq_cold, freq_map, hot_table, by_row, move, d_out):
            (hot_f,) = look((hot_hi, hot_lo), freq_map)
            used_rank = prefix(row_used.astype(I32))
            at_rank = (row(used_rank) == iota((COLD_MAX, rows_dev), 0)) & row(row_used)
            row_of = row_sum(jnp.where(at_rank, iota((COLD_MAX, rows_dev), 1), 0))
            packed = pack_rows(row_of, by_row)
            mine_no = jnp.where(hot_owner == me, FREQ_HOT + hot_place, -1)
            hot_pick = (one_hot(hot_f - 1, FREQ_HOT + hot_dev) * col((hot_f <= FREQ_HOT).astype(BF)) + one_hot(mine_no, FREQ_HOT + hot_dev)).T
            hot_rows = [dot32(hot_pick, hot_table[i]).astype(BF) for i in range(layers)]
            table = jnp.stack([jnp.concatenate([
                hot_rows[i][:FREQ_HOT], dot32(one_hot(cold_owner, n_dev), freq_cold[:, i]).astype(BF),
                hot_rows[i][FREQ_HOT:], packed[:, i]]) for i in range(layers)])
            n_used = jnp.minimum(jnp.sum(row_used.astype(I32)), COLD_MAX)
            row_no = got_class - cold_at
            used_before = row_sum(jnp.where(row(row_used) & (iota((n_loc, rows_dev), 1) < col(row_no)), 1, 0))
            cls = jnp.where(row_no >= 0, cold_at + used_before, got_class)
            code = jnp.where(hot_f <= FREQ_HOT, hot_f - 1, -1)
            d_placed = dot32(move, d_out).astype(BF)
            return d_placed, table, cls, n_used, row_of, code

        count = count_ids(swap(jnp.broadcast_to(row(token_ids), (n_dev, n_loc))), n_hi)
        tok, hot = digits(token_ids, n_hi), digits(hot_ids, n_hi)
        slot_no = jnp.arange(n_hot, dtype=I32)
        hot_place = slot_no // (RUN * n_dev) * RUN + slot_no % RUN
        hot_owner = slot_no // RUN % n_dev
        q_map = dot32(hot[0].T, hot[1] * col((hot_place + 1).astype(BF))).astype(BF)
        r_map = dot32(hot[0].T, hot[1] * col(hot_owner.astype(BF))).astype(BF)
        hot_no = number(jnp.where(q_map > 0, count, 0), FREQ_HOT)
        cold_no = number(jnp.where(q_map > 0, 0, count), FREQ_COLD)
        freq_map = jnp.where(hot_no > 0, hot_no, jnp.where(cold_no > 0, FREQ_HOT + cold_no, 0)).astype(BF)
        id_map = iota((n_hi, LO), 0) * LO + iota((n_hi, LO), 1) + 1
        cold_id = jnp.sum(jnp.where(cold_no.astype(I32)[None] == iota((FREQ_COLD, 1, 1), 0) + 1, id_map[None], 0), axis=(1, 2)) - 1
        cold_owner = jnp.where(cold_id >= 0, cold_id // rows_dev, -1)
        my_cold = (cold_owner == me).astype(I32)
        my_row = jnp.minimum(jnp.sum(my_cold * (cold_id - me * rows_dev + 1)) - 1, rows_dev - 1)
        by_row = emb_table.transpose(1, 0, 2)
        cold_row = lax.dynamic_slice_in_dim(by_row, jnp.maximum(my_row, 0), 1)
        freq_cold = swap(jnp.broadcast_to(cold_row, (n_dev, layers, emb_dim)))

        tok_f, tok_q, tok_r = look(tok, freq_map, q_map, r_map)
        rare = tok_f == 0
        owner = jnp.where(tok_q > 0, tok_r, token_ids // rows_dev)
        dev_no = iota((n_loc, n_dev), 1)
        to_dev = (col(owner) == dev_no) & col(rare)
        marks = beside(to_dev.astype(BF), col(jnp.logical_not(rare).astype(BF)))
        r, c = square(n_loc)
        ranks = dot32((r > c).astype(BF), marks)
        sent = down_sum(to_dev.astype(F32))
        free = jnp.maximum(places - sent, 0)
        free_at = prefix(free)
        fill = ranks[:, n_dev:]
        fill_dev = (fill >= free_at) & (fill < free_at + free)
        to_dev = jnp.where(col(rare), to_dev, fill_dev)
        place = jnp.where(col(rare), ranks[:, :n_dev], fill + (sent - free_at))
        slot = row_sum(jnp.where(to_dev, dev_no * places + place.astype(I32), 0))
        row_ids = me * rows_dev + jnp.arange(rows_dev, dtype=I32)
        row_f, row_q, row_n = look(digits(row_ids, n_hi), freq_map, q_map, (count > 0).astype(BF))
        row_used = (row_n > 0) & (row_f == 0) & (row_q == 0)
        fits = ((jnp.max(sent) <= places) & (jnp.sum(row_used.astype(I32)) <= COLD_MAX) & (jnp.sum(my_cold) <= 1))
        tok_class = jnp.where(rare, jnp.where(tok_q > 0, hot_at + tok_q - 1, cold_at + token_ids % rows_dev), tok_f - 1)
        bad = 1 << 20
        move = r == row(slot)
        send_class, freq_cold = lax.optimization_barrier(
            (row_sum(jnp.where(move, row(tok_class), 0)) + jnp.where(fits, 0, bad), freq_cold))
        got_class = swap(send_class.reshape(n_dev, places)).reshape(n_loc)
        move = move.astype(BF)
        placed, got_class, hot_hi, hot_lo, row_used, cold_owner = lax.optimization_barrier(
            (dot32(move, x_in).astype(BF), got_class, *hot, row_used, cold_owner))
        x_moved = exchange(placed)
        given = prepare(got_class, hot_hi, hot_lo, row_used, cold_owner, freq_cold, freq_map, hot_table, by_row, move, d_out)
        all_fit = jnp.max(got_class) < bad

        def fast(x_moved, slot, my_cold, my_row, d_placed, table, cls, n_used, row_of, code):
            d_moved = exchange(d_placed)
            cls_row = cls.reshape(1, n_loc)
            xs, hs, ss, es, x_last, zeros = forward(x_moved, cls.reshape(n_loc, 1), table, w_up, w_down, w_gate, w_proj, rows_dev)
            x_back = exchange(x_last)
            kept = (cls_row, es, xs, hs, ss, w_up, w_down, w_gate, w_proj, n_dev)
            sums_3, r, tot_3 = backward(3, d_moved, *kept)
            sums_2, r, tot_2, all_3 = backward(2, r, *kept, sums_3)
            r, x_back = lax.optimization_barrier((r, x_back))
            sums_1, r, tot_1, all_2 = backward(1, r, *kept, sums_2)
            sums_0, all_b = last(r, ss, w_proj, cls_row, sums_1, (tot_3, tot_2, tot_1), n_dev)
            x_out = dot32((col(slot) == iota((n_loc, n_loc), 1)).astype(BF), x_back).astype(BF)
            numbers = jnp.stack([n_used, my_row, jnp.sum(my_cold * jnp.arange(FREQ_COLD, dtype=I32))])
            d_table = put_rows(numbers, row_of, [sums_0, sums_1, sums_2, sums_3], all_b, zeros)
            freq_at = hot_dev // (2 * RUN)
            into = empty((layers, n_hot, emb_dim))
            into = hot_out(3, 1, all_3, all_b, freq_at, 0, code, into)
            into = hot_out(2, 1, all_2, all_b, freq_at, 1, code, into)
            into = hot_out(1, 2, all_b, all_b, freq_at + STRIDE // (2 * RUN), 0, code, into)
            return x_out, d_table.transpose(1, 0, 2), into

        def slow(*_):
            return general_path(n_dev, me, token_ids, hot_ids, x_in, d_out, emb_table, hot_table, w_up, w_down, w_gate, w_proj)

        return lax.cond(all_fit, fast, slow, *lax.optimization_barrier((x_moved, slot, my_cold, my_row, *given)))

    return jax.shard_map(body, mesh=mesh,
                         in_specs=(P('emb'), P(), P('emb', None), P('emb', None), P(None, 'emb', None), P(), P(), P(), P(), P()),
                         out_specs=(P('emb', None), P(None, 'emb', None), P()),
                         check_vma=False)
```

```python
import functools

import jax
import jax.numpy as jnp
from jax import lax
from jax.experimental import pallas as pl
from jax.experimental.pallas import tpu as pltpu
from jax.sharding import PartitionSpec as P


NORM_EPS = 1e-6
FREQ_HOT = 124
FREQ_COLD = 4
FREQ = FREQ_HOT + FREQ_COLD
COLD_MAX = 256
LO = 256
HI_BITS = 8
RUN = 4
LEVELS = tuple(12 * 2 ** (i / 6) for i in range(27))
GELU_A = 0.7978845608028654
GELU_B = GELU_A * 0.044715
VMEM = 66_000_000
ROWS_A = 256
ROWS_B = 512
TILE = 1024
BF = jnp.bfloat16
F32 = jnp.float32
I32 = jnp.int32
ONCE = pl.Buffered(1)


def gelu_back(pre_act, cot_in):
    _, pull = jax.vjp(jax.nn.gelu, pre_act.astype(F32))
    return pull(cot_in)[0]


def swap(v):
    return lax.all_to_all(v, 'emb', 0, 0, tiled=True)


def col(v):
    return v[:, None]


def row(v):
    return v[None, :]


def dot32(a, b):
    return jnp.dot(a, b, preferred_element_type=F32)


def dense_parts(resid, w_up, w_gate):
    resid_f = resid.astype(F32)
    inv_rms = lax.rsqrt(jnp.mean(resid_f * resid_f, axis=-1, keepdims=True) + NORM_EPS)
    normed = (resid_f * inv_rms).astype(BF)
    hidden = dot32(normed, w_up).astype(BF)
    gate_pre = dot32(normed, w_gate).astype(BF)
    return resid_f, inv_rms, hidden, gate_pre


def layer_forward(resid, emb_rows, w_up, w_down, w_gate, w_proj):
    resid_f, _, hidden, gate_pre = dense_parts(resid, w_up, w_gate)
    activated = jax.nn.gelu(hidden.astype(F32)).astype(BF)
    mlp_out = dot32(activated, w_down).astype(BF)
    gate = jax.nn.gelu(gate_pre.astype(F32)).astype(BF)
    mixed = (gate.astype(F32) * emb_rows.astype(F32)).astype(BF)
    projected = dot32(mixed, w_proj).astype(BF)
    return (resid_f + mlp_out.astype(F32) + projected.astype(F32)).astype(BF)


def layer_backward(resid, emb_rows, d_next, w_up, w_down, w_gate, w_proj):
    resid_f, inv_rms, hidden, gate_pre = dense_parts(resid, w_up, w_gate)
    gate = jax.nn.gelu(gate_pre.astype(F32)).astype(BF)
    d_cast = d_next.astype(BF)
    d_mixed = jnp.einsum('nd,ed->ne', d_cast, w_proj, preferred_element_type=F32)
    d_rows = gate.astype(F32) * d_mixed
    d_gpre = gelu_back(gate_pre, d_mixed * emb_rows.astype(F32))
    d_hidden = gelu_back(hidden, jnp.einsum('nd,fd->nf', d_cast, w_down, preferred_element_type=F32))
    d_normed = (jnp.einsum('nf,df->nd', d_hidden.astype(BF), w_up, preferred_element_type=F32)
                + jnp.einsum('ne,de->nd', d_gpre.astype(BF), w_gate, preferred_element_type=F32))
    inner = jnp.mean(d_normed * resid_f, axis=-1, keepdims=True)
    d_prev = d_next + inv_rms * d_normed - resid_f * (inv_rms * inv_rms * inv_rms) * inner
    return d_prev, d_rows


def general_path(n_dev, my_index, token_ids, hot_ids, x_in, d_out, emb_table, hot_table, w_up, w_down, w_gate, w_proj):
    n_loc = token_ids.shape[0]
    _, rows_dev, emb_dim = emb_table.shape
    capacity = max(8, (2 * n_loc) // n_dev)
    n_slots = n_dev * capacity
    hot_match = col(token_ids) == row(hot_ids)
    is_hot = hot_match.any(1)
    hot_pick = hot_match.astype(BF)
    hot_pick_f = hot_match.astype(F32)
    owner_id = token_ids // rows_dev
    to_owner = (col(owner_id) == row(jnp.arange(n_dev, dtype=I32))) & col(jnp.logical_not(is_hot))
    owner_rank = jnp.cumsum(to_owner.astype(jnp.int32), axis=0) - 1
    place = row_sum(jnp.where(to_owner, owner_rank, 0))
    slot = jnp.where(is_hot, n_slots, owner_id * capacity + place)
    none = jnp.full((n_slots,), -1, I32)
    send_ids = none.at[slot].set(token_ids, mode='drop')
    slot_tok = none.at[slot].set(jnp.arange(n_loc, dtype=jnp.int32), mode='drop')
    recv_ids = swap(send_ids.reshape(n_dev, capacity)).reshape(n_slots)
    served_ok = recv_ids >= 0
    local_row = jnp.where(served_ok, recv_ids - my_index * rows_dev, 0)
    pick_slot = jnp.minimum(slot, n_slots - 1)
    slot_used = slot_tok >= 0
    slot_src = jnp.maximum(slot_tok, 0)

    def fwd(resid, per_layer):
        table, hot_l, up, down, gate_w, proj = per_layer
        served = table[local_row]
        fetched = swap(served.reshape(n_dev, capacity, emb_dim)).reshape(n_slots, emb_dim)
        cold_rows = fetched[pick_slot]
        hot_rows = dot32(hot_pick, hot_l).astype(BF)
        emb_rows = jnp.where(col(is_hot), hot_rows, cold_rows)
        return layer_forward(resid, emb_rows, up, down, gate_w, proj), (resid, emb_rows)

    x_out, (x_saved, rows_saved) = lax.scan(fwd, x_in, (emb_table, hot_table, w_up, w_down, w_gate, w_proj))

    def bwd(d_resid, per_layer):
        resid_l, rows_l, up, down, gate_w, proj = per_layer
        d_resid, d_rows = layer_backward(resid_l, rows_l, d_resid, up, down, gate_w, proj)
        outgoing = jnp.where(col(slot_used), d_rows[slot_src], 0.0)
        incoming = swap(outgoing.reshape(n_dev, capacity, emb_dim)).reshape(n_slots, emb_dim)
        d_tab = jax.ops.segment_sum(jnp.where(col(served_ok), incoming, 0.0), local_row, num_segments=rows_dev)
        hot_local = jnp.einsum('nh,ne->he', hot_pick_f, d_rows, precision=lax.Precision.HIGHEST, preferred_element_type=F32)
        return d_resid, (d_tab, lax.psum(hot_local, 'emb'))

    _, (d_table, d_hot) = lax.scan(bwd, d_out.astype(F32), (x_saved, rows_saved, w_up, w_down, w_gate, w_proj), reverse=True)
    return x_out, d_table, d_hot


def split3(v):
    hi = v.astype(BF)
    rest = v - hi.astype(F32)
    mid = rest.astype(BF)
    return hi, mid, (rest - mid.astype(F32)).astype(BF)


def iota(shape, dim):
    return lax.broadcasted_iota(jnp.int32, shape, dim)


def one_hot(v, n, dtype=BF):
    return (col(v) == iota((len(v), n), 1)).astype(dtype)


def dot_nt(a, b):
    return lax.dot_general(a, b, (((1,), (1,)), ((), ())), preferred_element_type=F32)


def gelu(x):
    half = 0.5 * x
    return half + half * jnp.tanh(x * (GELU_A + GELU_B * (x * x)))


def gelu_slope(x):
    sq = x * x
    th = jnp.tanh(x * (GELU_A + GELU_B * sq))
    return (0.5 + 0.5 * th) + (0.5 * x) * (1.0 - th * th) * (GELU_A + (3.0 * GELU_B) * sq)


def forward_kernel(n_l, n_f, x0, cls, table, wu, wd, wg, wp, xs, hs, ss, es, xo, zeros, x_now, u_now, acc, q_now, blank, sem):
    layer, step = pl.program_id(0), pl.program_id(1)
    n_tok = x_now.shape[0]
    n_blank = blank.shape[0]
    blanks = [pltpu.make_async_copy(blank, zeros.at[pl.ds(i, n_blank)], sem) for i in range(0, zeros.shape[0], n_blank)]

    @pl.when((layer == 0) & (step == n_f - 1))
    def _():
        blank[...] = jnp.zeros(blank.shape, F32)
        for b in blanks:
            b.start()

    @pl.when((layer == n_l - 1) & (step == n_f - 1))
    def _():
        for b in blanks:
            b.wait()


    @pl.when((layer == 0) & (step == 0))
    def _():
        x_now[...] = x0[...]

    @pl.when(step == 0)
    def _():
        for m in chunks(n_tok, ROWS_A):
            xb = x_now[m, :]
            x = xb.astype(F32)
            xs[m, :] = xb
            u = (x * lax.rsqrt(jnp.mean(x * x, axis=-1, keepdims=True) + NORM_EPS)).astype(BF)
            u_now[m, :] = u
            s = dot32(u, wg[...]).astype(BF)
            ss[m, :] = s
            g = gelu(s.astype(F32)).astype(BF)
            pick = (cls[m, :] == iota((m.size, table.shape[0]), 1)).astype(BF)
            e = dot32(pick, table[...]).astype(BF)
            es[m, :] = e
            mixed = (g.astype(F32) * e.astype(F32)).astype(BF)
            q_now[m, :] = dot32(mixed, wp[...]).astype(BF)
            acc[m, :] = jnp.zeros((m.size, acc.shape[1]), F32)

    for m in chunks(n_tok, ROWS_B):
        h = dot32(u_now[m, :], wu[...]).astype(BF)
        hs[m, :] = h
        acc[m, :] += dot32(gelu(h.astype(F32)).astype(BF), wd[...])

    @pl.when(step == n_f - 1)
    def _():
        for m in chunks(n_tok, ROWS_A):
            x = x_now[m, :].astype(F32) + acc[m, :].astype(BF).astype(F32) + q_now[m, :].astype(F32)
            x_now[m, :] = x.astype(BF)

    @pl.when((step == n_f - 1) & (layer == n_l - 1))
    def _():
        xo[...] = x_now[...]


def chunks(n, size):
    size = min(n, size)
    return [pl.ds(m, size) for m in range(0, n, size)]


def forward(x0, cls, table, w_up, w_down, w_gate, w_proj, rows_dev):
    n_tok, dim = x0.shape
    n_l, _, ff = w_up.shape
    emb = w_gate.shape[2]
    tile = min(TILE, ff)
    n_f = ff // tile
    n_c = table.shape[1]

    def whole(l, f):
        return (l, 0, 0)

    def cols(l, f):
        return (l, 0, f)

    def fixed(l, f):
        return (0, 0)

    return pl.pallas_call(
        functools.partial(forward_kernel, n_l, n_f),
        grid=(n_l, n_f),
        in_specs=[
            pl.BlockSpec((n_tok, dim), fixed, pipeline_mode=ONCE),
            pl.BlockSpec((n_tok, 1), fixed, pipeline_mode=ONCE),
            pl.BlockSpec((None, n_c, emb), whole),
            pl.BlockSpec((None, dim, tile), cols),
            pl.BlockSpec((None, tile, dim), lambda l, f: (l, f, 0)),
            pl.BlockSpec((None, dim, emb), whole),
            pl.BlockSpec((None, emb, dim), whole),
        ],
        out_specs=[
            pl.BlockSpec((None, n_tok, dim), whole),
            pl.BlockSpec((None, n_tok, tile), cols),
            pl.BlockSpec((None, n_tok, emb), whole),
            pl.BlockSpec((None, n_tok, emb), whole),
            pl.BlockSpec((n_tok, dim), fixed),
            ANY,
        ],
        out_shape=[out_of((n_l, n_tok, n), BF) for n in (dim, ff, emb, emb)] + [out_of((n_tok, dim), BF), out_of((rows_dev, n_l, emb))],
        scratch_shapes=[pltpu.VMEM((n_tok, dim), t) for t in (BF, BF, F32, BF)]
        + [pltpu.VMEM((rows_dev // 12, n_l, emb), F32), pltpu.SemaphoreType.DMA(())],
        compiler_params=params("arbitrary", "arbitrary"),
        cost_estimate=cost(n_l * n_tok * dim * (2 * ff + 2 * emb + n_c), n_l),
        name="forward",
    )(x0, cls, table, w_up, w_down, w_gate, w_proj)


def params(*kinds, **more):
    return pltpu.CompilerParams(vmem_limit_bytes=VMEM, dimension_semantics=kinds or None, **more)


def cost(products, layers):
    return pl.CostEstimate(flops=2 * products, bytes_accessed=layers * 40_000_000, transcendentals=0)


def spec(shape, *index, **more):
    index = index or (0,) * len(shape)
    return pl.BlockSpec(shape, lambda *_: index, **more)


ANY = pl.BlockSpec(memory_space=pl.ANY)


def out_of(shape, dtype=F32):
    return jax.ShapeDtypeStruct(shape, dtype)


def backward_kernel(n_l, n_f, r_in, ss, wp, es, wg, xs, cls_t, hs, wu, wd, sums_out, out,
                    r, c_now, acc, three, s_now, p_now, e_now, g_now, x_now, sums, totals, loads, sems, sems_few, sems_f, *bufs):
    step = pl.program_id(0)
    f, n_full = step % n_f, (n_l - 1) * n_f
    n_tok = len(c_now)
    parts = chunks(n_tok, ROWS_B)
    n_hot, n_tot = COLD_AT - HOT_AT, n_l * RUN
    at = Place()
    folds = [Fold(at, sums.at[i, pl.ds(0, FREQ)], bufs[i * len(bufs) // n_l:(i + 1) * len(bufs) // n_l], sems_f.at[i]) for i in range(n_l)]
    alls = [Spread(at, sums.at[i, pl.ds(HOT_AT, n_hot)], lambda d, i=i: out.at[d, pl.ds(n_hot * i, n_hot)], sems.at[i]) for i in range(n_l)]
    few = Spread(at, totals, lambda d: out.at[d, pl.ds(n_hot * n_l, n_tot)], sems_few)

    def total(i):
        t = folds[i].total()
        for z in STOPS:
            @pl.when(at.z == z)
            def _(z=z):
                totals[pl.ds(i * RUN, RUN), :] = t[z * RUN:(z + 1) * RUN, :]

    def load(layer, which):
        srcs = (wp, p_now), (ss, s_now), (es, e_now), (wg, g_now), (xs, x_now)
        return [pltpu.make_async_copy(srcs[i][0].at[layer], srcs[i][1], loads.at[i]) for i in which]

    early, late = range(4), range(4, 5)
    layer = n_l - 1 - step // n_f
    first = pltpu.make_async_copy(r_in, c_now, loads.at[5])

    plan = {}
    for i in range(n_l):
        steps = [(1, folds[i].begin, ()), (2, folds[i].step, (0,)), (2, alls[i].begin, ()), (4, folds[i].step, (1,)), (5, alls[i].onward, (0,)),
                 (6, alls[i].column, (1,)), (6, folds[i].step, (2,)), (8, alls[i].column, (2,)), (8, alls[i].onward, (1,)),
                 (9, total, (i,)), (9, alls[i].column, (3,)), (10, alls[i].onward, (2,)), (11, alls[i].across, (0,)), (11, alls[i].onward, (3,)),
                 (13, alls[i].across, (1,)), (14, alls[i].across, (2,)), (15, alls[i].across, (3,))]
        for when, what, args in steps:
            plan.setdefault(10 * i + when, []).append((what, args))
    few_steps = [few.begin], *[[few.column, few.onward]] * 3, [few.onward], [few.across] * 4
    for k, steps in enumerate(few_steps):
        for j, what in enumerate(steps):
            args = () if not k else (k - j,) if k < 4 else (3,) if k == 4 else (j,)
            plan.setdefault(10 * n_l + k - 0.5, []).append((what, args))

    def point(k, now, layers):
        for i in range(layers):
            if 10 * i + k in plan:
                @pl.when(step == i * n_f + now)
                def _(i=i):
                    for what, args in plan.pop(10 * i + k):
                        what(*args)

    @pl.when(step == 0)
    def _():
        first.start()
        for c in load(layer, early):
            c.start()
        at.meet()
        first.wait()
        r[...] = c_now[...].astype(F32)

    @pl.when(f == 0)
    def _():
        for c in load(layer, early):
            c.wait()
        for c in load(layer, late):
            c.start()
        for m in parts:
            c = r[m, :].astype(BF)
            c_now[m, :] = c
            a = dot_nt(c, p_now[...])
            s = s_now[m, :].astype(F32)
            rows = gelu(s).astype(BF).astype(F32) * a
            for j, part in enumerate(split3(rows)):
                three[j, m, :] = part
            e_now[m, :] = (gelu_slope(s) * (a * e_now[m, :].astype(F32))).astype(BF)
        point(0, 0, n_l)
        class_sums(cls_t, three, sums.at[step // n_f])
        point(1, 0, n_l)

    @pl.when((f == 0) & (step < n_full))
    def _():
        for m in parts:
            acc[m, :] = dot_nt(e_now[m, :], g_now[...])

    @pl.when((f == 1) & (step < n_full))
    def _():
        for c in load(layer - 1, early):
            c.start()

    @pl.when(step < n_full)
    def _():
        for i, m in enumerate(parts):
            d_act = dot_nt(c_now[m, :], wd[...])
            dh = (gelu_slope(hs[m, :].astype(F32)) * d_act).astype(BF)
            acc[m, :] += dot_nt(dh, wu[...])
            for k in range(n_f):
                point(2 + 2 * k + i, k, n_l - 1)

    @pl.when((f == n_f - 1) & (step < n_full))
    def _():
        for c in load(layer, late):
            c.wait()
        for m in chunks(n_tok, ROWS_A):
            x = x_now[m, :].astype(F32)
            k = lax.rsqrt(jnp.mean(x * x, axis=-1, keepdims=True) + NORM_EPS)
            du = acc[m, :]
            inner = jnp.mean(du * x, axis=-1, keepdims=True)
            r[m, :] = r[m, :] + k * du - x * (k * k * k) * inner

    @pl.when(step == n_full)
    def _():
        for c in load(layer, late):
            c.wait()
        keep = pltpu.make_async_copy(sums, sums_out, loads.at[5])
        keep.start()
        for k in sorted(plan):
            for what, args in plan[k]:
                what(*args)
        for v in (*alls, few):
            v.end()
        keep.wait()


def backward(r_in, cls_t, es, xs, hs, ss, w_up, w_down, w_gate, w_proj, n_dev):
    n_tok, dim = r_in.shape
    n_l, _, ff = w_up.shape
    emb = w_gate.shape[2]
    n_c = COLD_AT + COLD_MAX
    n_f = 4
    tile = ff // n_f
    n_full = (n_l - 1) * n_f
    n_out = n_l * (COLD_AT - HOT_AT + RUN)

    def at_layer(t):
        t = jnp.minimum(t, n_full - 1)
        return n_l - 1 - t // n_f, t % n_f

    def cols(n):
        return pl.BlockSpec((None, n, tile), lambda t: (at_layer(t)[0], 0, at_layer(t)[1]))

    return pl.pallas_call(
        functools.partial(backward_kernel, n_l, n_f),
        grid=(n_full + 1,),
        in_specs=[ANY] * 6 + [spec((1, n_tok), pipeline_mode=ONCE), cols(n_tok), cols(dim),
                              pl.BlockSpec((None, tile, dim), lambda t: (*at_layer(t), 0))],
        out_specs=[ANY] * 2,
        out_shape=[out_of((n_l, n_c, emb)), out_of((n_dev, n_out, emb))],
        scratch_shapes=[pltpu.VMEM((n_tok, dim), F32), pltpu.VMEM((n_tok, dim), BF), pltpu.VMEM((n_tok, dim), F32), pltpu.VMEM((3, n_tok, emb), BF)]
        + [pltpu.VMEM(v, BF) for v in ((n_tok, emb), (emb, dim), (n_tok, emb), (dim, emb), (n_tok, dim))]
        + [pltpu.VMEM((n_l, n_c, emb), F32), pltpu.VMEM((n_l * RUN, emb), F32), pltpu.SemaphoreType.DMA((6,)),
           pltpu.SemaphoreType.DMA((n_l, *SPREAD_SEMS)), pltpu.SemaphoreType.DMA(SPREAD_SEMS), pltpu.SemaphoreType.DMA((n_l, *FOLD_SEMS))]
        + fold_bufs(emb) * n_l,
        compiler_params=params("arbitrary", collective_id=0, has_side_effects=True),
        cost_estimate=cost(n_l * n_tok * dim * (2 * ff + 2 * emb + 3 * n_c), n_l),
        name="backward",
    )(r_in, ss, w_proj, es, w_gate, xs, cls_t, hs, w_up, w_down)


def count_kernel(ids, out):
    n_tok = ids.shape[1]
    out[...] = jnp.zeros(out.shape, F32)

    def hits(v, n):
        same = v.astype(F32).astype(BF) == iota((n, n_tok), 0).astype(F32).astype(BF)
        return jnp.where(same, jnp.ones((), BF), jnp.zeros((), BF))

    @pl.loop(0, len(ids))
    def _(i):
        ids_i = ids[pl.ds(i, 1), :]
        out[...] += dot_nt(hits(ids_i >> HI_BITS, len(out)), hits(ids_i & (LO - 1), LO))


def count_ids(ids, n_hi):
    return pl.pallas_call(count_kernel, out_shape=out_of((n_hi, LO)), compiler_params=params(), name="count_ids")(ids)


def pack_kernel(row_of, table, out, sem):
    @pl.loop(0, len(out))
    def _(k):
        pltpu.make_async_copy(table.at[row_of[k]], out.at[k], sem).start()

    pltpu.make_async_copy(table.at[pl.ds(0, len(out))], out, sem).wait()


def pack_rows(row_of, table):
    shape = row_of.shape + table.shape[1:]
    return pl.pallas_call(
        pack_kernel,
        grid_spec=pltpu.PrefetchScalarGridSpec(num_scalar_prefetch=1, grid=(1,), in_specs=[ANY], out_specs=spec(shape),
                                               scratch_shapes=[pltpu.SemaphoreType.DMA(())]),
        out_shape=out_of(shape, table.dtype), compiler_params=params(), name="pack_rows",
    )(row_of, table)


class Place:
    def __init__(self):
        me = lax.axis_index('emb')
        self.core, self.x, self.y, self.z = me % 2, (me // 2) % 2, (me // 4) % 2, me // 8
        self.others = [self.dev(z=(self.z + k) % 4) for k in REST]
        self.columns = [(self.z - k + 4) % 4 for k in STOPS]
        self.to_x, self.to_y, self.to_core = self.dev(x=1 - self.x), self.dev(y=1 - self.y), self.dev(core=1 - self.core)

    def dev(self, z=None, y=None, x=None, core=None):
        z, y, x, core = [mine if v is None else v for v, mine in ((z, self.z), (y, self.y), (x, self.x), (core, self.core))]
        return ((z * 2 + y) * 2 + x) * 2 + core

    def meet(self):
        barrier = pltpu.get_barrier_semaphore()
        peers = self.others + [self.to_x, self.to_y, self.to_core]
        for peer in peers:
            pl.semaphore_signal(barrier, device_id=(peer,), device_id_type=pl.DeviceIdType.MESH)
        pl.semaphore_wait(barrier, len(peers))


def remote(src, dst, sems, to):
    return pltpu.make_async_remote_copy(src_ref=src, dst_ref=dst, send_sem=sems[0], recv_sem=sems[1],
                                        device_id=(to,), device_id_type=pl.DeviceIdType.MESH)


Z, X, Y, FX, FY, C, CX, CY, CD, OWN = range(10)


class Spread:
    def __init__(self, at, mine, slot, sems):
        self.at, self.mine, self.slot, self.sems = at, mine, slot, sems
        n = mine.shape[0]
        half = n // 16 * 8
        self.halves = {FY: pl.ds(0, half), FX: pl.ds(half, n - half)}
        self.col = [at.dev(z=z) for z in at.columns]
        self.by_x = [at.dev(z=z, x=1 - at.x) for z in at.columns]
        self.by_y = [at.dev(z=z, y=1 - at.y) for z in at.columns]
        self.by_d = [at.dev(z=z, x=1 - at.x, y=1 - at.y) for z in at.columns]
        self.far = [[at.dev(z=z, x=x, y=y, core=1 - at.core) for z in at.columns]
                    for y, x in ((at.y, at.x), (at.y, 1 - at.x), (1 - at.y, at.x), (1 - at.y, 1 - at.x))]
        self.done = []

    def pair(self, kind, k):
        return self.sems.at[0, kind, k], self.sems.at[1, kind, k]

    def send(self, kind, k, src, dst, to):
        remote(src, dst, self.pair(kind, k), to).start()
        self.done.append((kind, k))

    def got(self, kind, k, block):
        remote(block, block, self.pair(kind, k), self.at.to_x).wait_recv()

    def begin(self):
        own = self.slot(self.col[0])
        pltpu.make_async_copy(self.mine, own, self.sems.at[0, OWN, 0]).start()
        for k, other in enumerate(self.at.others):
            self.send(Z, k + 1, self.mine, own, other)
        self.column(0)

    def column(self, k):
        block = self.slot(self.col[k])
        if k:
            self.got(Z, k, block)
        src = block if k else self.mine
        for kind, to in ((X, self.at.to_x), (Y, self.at.to_y), (C, self.at.to_core)):
            self.send(kind, k, src, block, to)

    def onward(self, k):
        for kind, part, to, other, core in ((X, self.by_x, self.at.to_y, FY, CX), (Y, self.by_y, self.at.to_x, FX, CY)):
            block = self.slot(part[k])
            self.got(kind, k, block)
            half = block.at[self.halves[other]]
            self.send(other, k, half, half, to)
            self.send(core, k, block, block, self.at.to_core)

    def across(self, k):
        block = self.slot(self.by_d[k])
        for kind, half in self.halves.items():
            self.got(kind, k, block.at[half])
        self.send(CD, k, block, block, self.at.to_core)

    def end(self):
        for k in STOPS:
            for kind, far in zip((C, CX, CY, CD), self.far):
                self.got(kind, k, self.slot(far[k]))
        own = self.slot(self.col[0])
        for kind, k in self.done:
            block = own.at[self.halves[kind]] if kind in self.halves else own
            remote(block, block, self.pair(kind, k), self.at.to_x).wait_send()
        pltpu.make_async_copy(self.mine, own, self.sems.at[0, OWN, 0]).wait()


class Fold:
    def __init__(self, at, part, bufs, sems):
        self.at, self.part, self.sems = at, part, sems
        self.ins, self.sums, self.all_z = bufs[:3], bufs[3:5], bufs[5]
        self.bits = at.core, at.x, at.y
        self.to = at.to_core, at.to_x, at.to_y

    def pair(self, i, k=0):
        return self.sems.at[0, i, k], self.sems.at[1, i, k]

    def cut(self, i, bit):
        n = self.ins[i].shape[0]
        return pl.ds(pl.multiple_of(bit * n, n), n)

    def source(self, i):
        return self.sums[i - 1] if i else self.part

    def hop(self, i):
        return remote(self.source(i).at[self.cut(i, 1 - self.bits[i])], self.ins[i], self.pair(i), self.to[i])

    def begin(self):
        self.hop(0).start()

    def step(self, i):
        self.hop(i).wait_recv()
        total = self.source(i)[self.cut(i, self.bits[i]), :] + self.ins[i][...]
        if i < 2:
            self.sums[i][...] = total
            self.hop(i + 1).start()
        else:
            self.all_z[self.at.z] = total
            for k, other in enumerate(self.at.others):
                self.along_z(k, other).start()

    def along_z(self, k, other):
        block = self.all_z.at[self.at.z]
        return remote(block, block, self.pair(3, k), other)

    def total(self):
        for k, other in enumerate(self.at.others):
            self.along_z(k, other).wait_recv()
        for i in range(3):
            self.hop(i).wait_send()
        for k, other in enumerate(self.at.others):
            self.along_z(k, other).wait_send()
        v = self.all_z
        return (v[0] + v[1]) + (v[2] + v[3])


def fold_bufs(emb):
    return [pltpu.VMEM((n, emb), F32) for n in (64, 32, 16, 64, 32)] + [pltpu.VMEM((4, 16, emb), F32)]


SPREAD_SEMS = (2, 10, 4)
STOPS = range(4)
REST = STOPS[1:]
FOLD_SEMS = (2, 4, 4)
HOT_AT, COLD_AT = FREQ, FREQ + 64


def class_sums(cls_t, three, sums):
    pick_t = (cls_t[...] == iota((sums.shape[0], cls_t.shape[1]), 0)).astype(BF)
    hi, mid, lo = [dot32(pick_t, three[i]) for i in range(3)]
    sums[...] = hi + (mid + lo)


ORDER = [(b & 3) * 8 + (b >> 2 & 1) * 4 + (b >> 3 & 1) * 2 + (b >> 4) for b in range(FREQ // RUN)]


def hot_kernel(any_freq, raw, freq, code, out, parts):
    n_dev, n_r, _ = raw.shape
    layer, block = pl.program_id(0), pl.program_id(1)
    n = RUN * n_dev
    for g in range(n_r // RUN):
        for o in range(n_dev):
            out[pl.ds(g * n + o * RUN, RUN), :] = raw[o, pl.ds(g * RUN, RUN), :]

    @pl.when(any_freq[block] > 0)
    def _():
        for j in range(freq.shape[1] // RUN):
            @pl.when(layer == j)
            def _(j=j):
                rows = jnp.concatenate([freq[o, j * RUN:(j + 1) * RUN, :] for o in ORDER])
                for i, part in enumerate(split3(rows)):
                    parts[i] = part
        sel = (code[...] == iota((n_r * n_dev, FREQ), 1)).astype(BF)
        out[...] += dot32(sel, parts[0]) + (dot32(sel, parts[1]) + dot32(sel, parts[2]))


def hot_out(gathered, code, n_l):
    n_dev, n_rows, emb = gathered.shape
    n_r = 4 * RUN
    width = n_r * n_dev
    blocks = len(code) // width
    return pl.pallas_call(
        hot_kernel,
        grid_spec=pltpu.PrefetchScalarGridSpec(
            num_scalar_prefetch=1, grid=(n_l, blocks),
            in_specs=[
                pl.BlockSpec((n_dev, n_r, emb), lambda i, b, _: (0, i * blocks + b, 0)),
                spec((n_dev, n_l * RUN, emb), 0, n_rows // (n_l * RUN) - 1, 0, pipeline_mode=ONCE),
                pl.BlockSpec((width, 1), lambda i, b, _: (b, 0)),
            ],
            out_specs=pl.BlockSpec((None, width, emb), lambda i, b, _: (n_l - 1 - i, b, 0)),
            scratch_shapes=[pltpu.VMEM((3, FREQ, emb), BF)]),
        out_shape=out_of((n_l, len(code), emb)),
        compiler_params=params("arbitrary", "arbitrary"),
        cost_estimate=cost(gathered.size * LO, n_l), name="hot_out",
    )((code.reshape(blocks, width) >= 0).any(axis=1).astype(I32), gathered, gathered, code.reshape(-1, 1))


def rows_kernel(numbers, row_of, sums, freq, into, out, stage, got, sem):
    n_used, cold_row, cold_no = [numbers[i] for i in range(3)]
    n_l = len(sums)

    def put(k, row):
        return pltpu.make_async_copy(stage.at[pl.ds(k, 1)], out.at[pl.ds(row, 1)], sem)

    def fill(k, src, at):
        for i in range(n_l):
            stage[k, pl.ds(n_l - 1 - i, 1), :] = src(i, at)

    @pl.loop(0, n_used)
    def _(k):
        fill(k, lambda i, at: sums[i, pl.ds(at, 1), :], COLD_AT + k)
        put(k, row_of[k]).start()

    @pl.when(cold_row >= 0)
    def _():
        c = pltpu.make_async_copy(freq.at[len(freq) - 1, pl.ds(n_l * (COLD_AT - HOT_AT), n_l * RUN)], got, sem)
        c.start()
        c.wait()
        fill(COLD_MAX, lambda i, at: got[pl.ds(i * RUN + at, 1), :], cold_no)
        put(COLD_MAX, cold_row).start()
        put(0, 0).wait()

    @pl.loop(0, n_used)
    def _(k):
        put(0, 0).wait()


def put_rows(numbers, row_of, sums, freq, into):
    n_l, _, emb = sums.shape
    return pl.pallas_call(
        rows_kernel,
        grid_spec=pltpu.PrefetchScalarGridSpec(
            num_scalar_prefetch=2, grid=(1,),
            in_specs=[spec(sums.shape), ANY, ANY], out_specs=ANY,
            scratch_shapes=[pltpu.VMEM((COLD_MAX + 1, n_l, emb), F32), pltpu.VMEM((n_l * RUN, emb), F32), pltpu.SemaphoreType.DMA(())]),
        out_shape=out_of(into.shape), input_output_aliases={4: 0},
        compiler_params=params("arbitrary"), name="put_rows",
    )(numbers, row_of, sums, freq, into)


def down_sum(v):
    return jnp.sum(v, axis=0)


def beside(*v):
    return jnp.concatenate(v, axis=1)


def row_sum(v):
    return jnp.sum(v, axis=1)


def square(n):
    return iota((n, n), 0), iota((n, n), 1)


def prefix(v):
    r, c = square(len(v))
    return row_sum(jnp.where(r > c, row(v), 0))


def digits(ids, n_hi):
    return one_hot(ids >> HI_BITS, n_hi), one_hot(ids & (LO - 1), LO)


def look(hi_lo, *maps):
    hi, lo = hi_lo
    got = dot32(hi, beside(*maps))
    return [row_sum(got[:, i * LO:(i + 1) * LO] * lo.astype(F32)).astype(I32) for i in range(len(maps))]


def number(count, most):
    levels = jnp.array(LEVELS, F32)
    n_over = jnp.sum((count[:, :, None] >= levels).astype(F32), axis=(0, 1))
    flag = count >= jnp.min(jnp.where(n_over <= most, levels, jnp.inf))
    r, c = square(LO)
    in_row = dot32(flag.astype(BF), (r < c).astype(BF))
    return jnp.where(flag, in_row + col(prefix(row_sum(flag.astype(F32)))) + 1, 0)


def solution(mesh):
    n_dev = mesh.shape['emb']

    def body(token_ids, hot_ids, x_in, d_out, emb_table, hot_table, w_up, w_down, w_gate, w_proj):
        n_loc = len(token_ids)
        layers, rows_dev, emb_dim = emb_table.shape
        n_hot = len(hot_ids)
        places, hot_dev = n_loc // n_dev, n_hot // n_dev
        n_hi = -(-rows_dev * n_dev // (8 * LO)) * 8
        me = lax.axis_index('emb')
        hot_at, cold_at = FREQ, FREQ + hot_dev

        def exchange(v):
            return swap(v.reshape(n_dev, places, -1)).reshape(n_loc, -1)

        def prepare(got_class, hot_hi, hot_lo, row_used, cold_owner, freq_cold, freq_map, hot_table, by_row, move, d_out):
            (hot_f,) = look((hot_hi, hot_lo), freq_map)
            used_rank = prefix(row_used.astype(I32))
            at_rank = (row(used_rank) == iota((COLD_MAX, rows_dev), 0)) & row(row_used)
            row_of = row_sum(jnp.where(at_rank, iota((COLD_MAX, rows_dev), 1), 0))
            packed = pack_rows(row_of, by_row)
            mine_no = jnp.where(hot_owner == me, FREQ_HOT + hot_place, -1)
            hot_pick = (one_hot(hot_f - 1, FREQ_HOT + hot_dev) * col((hot_f <= FREQ_HOT).astype(BF)) + one_hot(mine_no, FREQ_HOT + hot_dev)).T
            hot_rows = [dot32(hot_pick, hot_table[i]).astype(BF) for i in range(layers)]
            table = jnp.stack([jnp.concatenate([
                hot_rows[i][:FREQ_HOT], dot32(one_hot(cold_owner, n_dev), freq_cold[:, i]).astype(BF),
                hot_rows[i][FREQ_HOT:], packed[:, i]]) for i in range(layers)])
            n_used = jnp.minimum(jnp.sum(row_used.astype(I32)), COLD_MAX)
            row_no = got_class - cold_at
            used_before = row_sum(jnp.where(row(row_used) & (iota((n_loc, rows_dev), 1) < col(row_no)), 1, 0))
            cls = jnp.where(row_no >= 0, cold_at + used_before, got_class)
            code = jnp.where(hot_f <= FREQ_HOT, hot_f - 1, -1)
            d_placed = dot32(move, d_out).astype(BF)
            return d_placed, table, cls, n_used, row_of, code

        count = count_ids(swap(jnp.broadcast_to(row(token_ids), (n_dev, n_loc))), n_hi)
        tok, hot = digits(token_ids, n_hi), digits(hot_ids, n_hi)
        slot_no = jnp.arange(n_hot, dtype=I32)
        hot_place = slot_no // (RUN * n_dev) * RUN + slot_no % RUN
        hot_owner = slot_no // RUN % n_dev
        q_map = dot32(hot[0].T, hot[1] * col((hot_place + 1).astype(BF))).astype(BF)
        r_map = dot32(hot[0].T, hot[1] * col(hot_owner.astype(BF))).astype(BF)
        hot_no = number(jnp.where(q_map > 0, count, 0), FREQ_HOT)
        cold_no = number(jnp.where(q_map > 0, 0, count), FREQ_COLD)
        freq_map = jnp.where(hot_no > 0, hot_no, jnp.where(cold_no > 0, FREQ_HOT + cold_no, 0)).astype(BF)
        id_map = iota((n_hi, LO), 0) * LO + iota((n_hi, LO), 1) + 1
        cold_id = jnp.sum(jnp.where(cold_no.astype(I32)[None] == iota((FREQ_COLD, 1, 1), 0) + 1, id_map[None], 0), axis=(1, 2)) - 1
        cold_owner = jnp.where(cold_id >= 0, cold_id // rows_dev, -1)
        my_cold = (cold_owner == me).astype(I32)
        my_row = jnp.minimum(jnp.sum(my_cold * (cold_id - me * rows_dev + 1)) - 1, rows_dev - 1)
        by_row = emb_table.transpose(1, 0, 2)
        cold_row = lax.dynamic_slice_in_dim(by_row, jnp.maximum(my_row, 0), 1)
        freq_cold = swap(jnp.broadcast_to(cold_row, (n_dev, layers, emb_dim)))

        tok_f, tok_q, tok_r = look(tok, freq_map, q_map, r_map)
        rare = tok_f == 0
        owner = jnp.where(tok_q > 0, tok_r, token_ids // rows_dev)
        dev_no = iota((n_loc, n_dev), 1)
        to_dev = (col(owner) == dev_no) & col(rare)
        marks = beside(to_dev.astype(BF), col(jnp.logical_not(rare).astype(BF)))
        r, c = square(n_loc)
        ranks = dot32((r > c).astype(BF), marks)
        sent = down_sum(to_dev.astype(F32))
        free = jnp.maximum(places - sent, 0)
        free_at = prefix(free)
        fill = ranks[:, n_dev:]
        fill_dev = (fill >= free_at) & (fill < free_at + free)
        to_dev = jnp.where(col(rare), to_dev, fill_dev)
        place = jnp.where(col(rare), ranks[:, :n_dev], fill + (sent - free_at))
        slot = row_sum(jnp.where(to_dev, dev_no * places + place.astype(I32), 0))
        row_ids = me * rows_dev + jnp.arange(rows_dev, dtype=I32)
        row_f, row_q, row_n = look(digits(row_ids, n_hi), freq_map, q_map, (count > 0).astype(BF))
        row_used = (row_n > 0) & (row_f == 0) & (row_q == 0)
        fits = ((jnp.max(sent) <= places) & (jnp.sum(row_used.astype(I32)) <= COLD_MAX) & (jnp.sum(my_cold) <= 1))
        tok_class = jnp.where(rare, jnp.where(tok_q > 0, hot_at + tok_q - 1, cold_at + token_ids % rows_dev), tok_f - 1)
        bad = 1 << 20
        move = r == row(slot)
        send_class, freq_cold = lax.optimization_barrier(
            (row_sum(jnp.where(move, row(tok_class), 0)) + jnp.where(fits, 0, bad), freq_cold))
        got_class = swap(send_class.reshape(n_dev, places)).reshape(n_loc)
        move = move.astype(BF)
        placed, got_class, hot_hi, hot_lo, row_used, cold_owner = lax.optimization_barrier(
            (dot32(move, x_in).astype(BF), got_class, *hot, row_used, cold_owner))
        x_moved = exchange(placed)
        given = prepare(got_class, hot_hi, hot_lo, row_used, cold_owner, freq_cold, freq_map, hot_table, by_row, move, d_out)
        all_fit = jnp.max(got_class) < bad

        def fast(x_moved, slot, my_cold, my_row, d_placed, table, cls, n_used, row_of, code):
            d_moved = exchange(d_placed)
            cls_row = cls.reshape(1, n_loc)
            xs, hs, ss, es, x_last, zeros = forward(x_moved, cls.reshape(n_loc, 1), table, w_up, w_down, w_gate, w_proj, rows_dev)
            sums, gathered = backward(d_moved, cls_row, es, xs, hs, ss, w_up, w_down, w_gate, w_proj, n_dev)
            x_last, gathered = lax.optimization_barrier((x_last, gathered))
            x_back = exchange(x_last)
            numbers = jnp.stack([n_used, my_row, jnp.sum(my_cold * jnp.arange(FREQ_COLD, dtype=I32))])
            d_table = put_rows(numbers, row_of, sums, gathered, zeros)
            d_hot = hot_out(gathered, code, layers)
            x_out = dot32((col(slot) == iota((n_loc, n_loc), 1)).astype(BF), x_back).astype(BF)
            return x_out, d_table.transpose(1, 0, 2), d_hot

        def slow(*_):
            return general_path(n_dev, me, token_ids, hot_ids, x_in, d_out, emb_table, hot_table, w_up, w_down, w_gate, w_proj)

        return lax.cond(all_fit, fast, slow, *lax.optimization_barrier((x_moved, slot, my_cold, my_row, *given)))

    return jax.shard_map(body, mesh=mesh,
                         in_specs=(P('emb'), P(), P('emb', None), P('emb', None), P(None, 'emb', None), P(), P(), P(), P(), P()),
                         out_specs=(P('emb', None), P(None, 'emb', None), P()),
                         check_vma=False)
```

```python
import functools

import jax
import jax.numpy as jnp
from jax import lax
from jax.experimental import pallas as pl
from jax.experimental.pallas import tpu as pltpu
from jax.sharding import PartitionSpec as P


NORM_EPS = 1e-6
FREQ_HOT = 124
FREQ_COLD = 4
FREQ = FREQ_HOT + FREQ_COLD
COLD_MAX = 256
LO = 256
HI_BITS = 8
RUN = 4
LEVELS = tuple(12 * 2 ** (i / 6) for i in range(27))
GELU_A = 0.7978845608028654
GELU_B = GELU_A * 0.044715
VMEM = 66_000_000
ROWS_A = 256
ROWS_B = 512
TILE = 1024
BF = jnp.bfloat16
F32 = jnp.float32
I32 = jnp.int32
ONCE = pl.Buffered(1)


def gelu_back(pre_act, cot_in):
    _, pull = jax.vjp(jax.nn.gelu, pre_act.astype(F32))
    return pull(cot_in)[0]


def swap(v):
    return lax.all_to_all(v, 'emb', 0, 0, tiled=True)


def col(v):
    return v[:, None]


def row(v):
    return v[None, :]


def dot32(a, b):
    return jnp.dot(a, b, preferred_element_type=F32)


def dense_parts(resid, w_up, w_gate):
    resid_f = resid.astype(F32)
    inv_rms = lax.rsqrt(jnp.mean(resid_f * resid_f, axis=-1, keepdims=True) + NORM_EPS)
    normed = (resid_f * inv_rms).astype(BF)
    hidden = dot32(normed, w_up).astype(BF)
    gate_pre = dot32(normed, w_gate).astype(BF)
    return resid_f, inv_rms, hidden, gate_pre


def layer_forward(resid, emb_rows, w_up, w_down, w_gate, w_proj):
    resid_f, _, hidden, gate_pre = dense_parts(resid, w_up, w_gate)
    activated = jax.nn.gelu(hidden.astype(F32)).astype(BF)
    mlp_out = dot32(activated, w_down).astype(BF)
    gate = jax.nn.gelu(gate_pre.astype(F32)).astype(BF)
    mixed = (gate.astype(F32) * emb_rows.astype(F32)).astype(BF)
    projected = dot32(mixed, w_proj).astype(BF)
    return (resid_f + mlp_out.astype(F32) + projected.astype(F32)).astype(BF)


def layer_backward(resid, emb_rows, d_next, w_up, w_down, w_gate, w_proj):
    resid_f, inv_rms, hidden, gate_pre = dense_parts(resid, w_up, w_gate)
    gate = jax.nn.gelu(gate_pre.astype(F32)).astype(BF)
    d_cast = d_next.astype(BF)
    d_mixed = jnp.einsum('nd,ed->ne', d_cast, w_proj, preferred_element_type=F32)
    d_rows = gate.astype(F32) * d_mixed
    d_gpre = gelu_back(gate_pre, d_mixed * emb_rows.astype(F32))
    d_hidden = gelu_back(hidden, jnp.einsum('nd,fd->nf', d_cast, w_down, preferred_element_type=F32))
    d_normed = (jnp.einsum('nf,df->nd', d_hidden.astype(BF), w_up, preferred_element_type=F32)
                + jnp.einsum('ne,de->nd', d_gpre.astype(BF), w_gate, preferred_element_type=F32))
    inner = jnp.mean(d_normed * resid_f, axis=-1, keepdims=True)
    d_prev = d_next + inv_rms * d_normed - resid_f * (inv_rms * inv_rms * inv_rms) * inner
    return d_prev, d_rows


def general_path(n_dev, my_index, token_ids, hot_ids, x_in, d_out, emb_table, hot_table, w_up, w_down, w_gate, w_proj):
    n_loc = token_ids.shape[0]
    _, rows_dev, emb_dim = emb_table.shape
    capacity = max(8, (2 * n_loc) // n_dev)
    n_slots = n_dev * capacity
    hot_match = col(token_ids) == row(hot_ids)
    is_hot = hot_match.any(1)
    hot_pick = hot_match.astype(BF)
    hot_pick_f = hot_match.astype(F32)
    owner_id = token_ids // rows_dev
    to_owner = (col(owner_id) == row(jnp.arange(n_dev, dtype=I32))) & col(jnp.logical_not(is_hot))
    owner_rank = jnp.cumsum(to_owner.astype(jnp.int32), axis=0) - 1
    place = row_sum(jnp.where(to_owner, owner_rank, 0))
    slot = jnp.where(is_hot, n_slots, owner_id * capacity + place)
    none = jnp.full((n_slots,), -1, I32)
    send_ids = none.at[slot].set(token_ids, mode='drop')
    slot_tok = none.at[slot].set(jnp.arange(n_loc, dtype=jnp.int32), mode='drop')
    recv_ids = swap(send_ids.reshape(n_dev, capacity)).reshape(n_slots)
    served_ok = recv_ids >= 0
    local_row = jnp.where(served_ok, recv_ids - my_index * rows_dev, 0)
    pick_slot = jnp.minimum(slot, n_slots - 1)
    slot_used = slot_tok >= 0
    slot_src = jnp.maximum(slot_tok, 0)

    def fwd(resid, per_layer):
        table, hot_l, up, down, gate_w, proj = per_layer
        served = table[local_row]
        fetched = swap(served.reshape(n_dev, capacity, emb_dim)).reshape(n_slots, emb_dim)
        cold_rows = fetched[pick_slot]
        hot_rows = dot32(hot_pick, hot_l).astype(BF)
        emb_rows = jnp.where(col(is_hot), hot_rows, cold_rows)
        return layer_forward(resid, emb_rows, up, down, gate_w, proj), (resid, emb_rows)

    x_first = jnp.where(n_loc * hot_ids[0] >= 0, x_in, 0)
    x_out, (x_saved, rows_saved) = lax.scan(fwd, x_first, (emb_table, hot_table, w_up, w_down, w_gate, w_proj))

    def bwd(d_resid, per_layer):
        resid_l, rows_l, up, down, gate_w, proj = per_layer
        d_resid, d_rows = layer_backward(resid_l, rows_l, d_resid, up, down, gate_w, proj)
        outgoing = jnp.where(col(slot_used), d_rows[slot_src], 0.0)
        incoming = swap(outgoing.reshape(n_dev, capacity, emb_dim)).reshape(n_slots, emb_dim)
        d_tab = jax.ops.segment_sum(jnp.where(col(served_ok), incoming, 0.0), local_row, num_segments=rows_dev)
        hot_local = jnp.einsum('nh,ne->he', hot_pick_f, d_rows, precision=lax.Precision.HIGHEST, preferred_element_type=F32)
        return d_resid, (d_tab, lax.psum(hot_local, 'emb'))

    _, (d_table, d_hot) = lax.scan(bwd, d_out.astype(F32), (x_saved, rows_saved, w_up, w_down, w_gate, w_proj), reverse=True)
    return x_out, d_table, d_hot


def split3(v):
    hi = v.astype(BF)
    rest = v - hi.astype(F32)
    mid = rest.astype(BF)
    return hi, mid, (rest - mid.astype(F32)).astype(BF)


def iota(shape, dim):
    return lax.broadcasted_iota(jnp.int32, shape, dim)


def one_hot(v, n, dtype=BF):
    return (col(v) == iota((len(v), n), 1)).astype(dtype)


def dot_nt(a, b):
    return lax.dot_general(a, b, (((1,), (1,)), ((), ())), preferred_element_type=F32)


def gelu(x):
    half = 0.5 * x
    return half + half * jnp.tanh(x * (GELU_A + GELU_B * (x * x)))


def gelu_slope(x):
    sq = x * x
    th = jnp.tanh(x * (GELU_A + GELU_B * sq))
    return (0.5 + 0.5 * th) + (0.5 * x) * (1.0 - th * th) * (GELU_A + (3.0 * GELU_B) * sq)


def forward_kernel(n_l, n_f, x0, cls, table, wu, wd, wg, wp, xs, hs, ss, es, xo, x_now, u_now, acc, q_now):
    layer, step = pl.program_id(0), pl.program_id(1)
    n_tok = x_now.shape[0]

    @pl.when((layer == 0) & (step == 0))
    def _():
        x_now[...] = x0[...]

    @pl.when(step == 0)
    def _():
        for m in chunks(n_tok, ROWS_A):
            xb = x_now[m, :]
            x = xb.astype(F32)
            xs[m, :] = xb
            u = (x * lax.rsqrt(jnp.mean(x * x, axis=-1, keepdims=True) + NORM_EPS)).astype(BF)
            u_now[m, :] = u
            s = dot32(u, wg[...]).astype(BF)
            ss[m, :] = s
            g = gelu(s.astype(F32)).astype(BF)
            pick = (cls[m, :] == iota((m.size, table.shape[0]), 1)).astype(BF)
            e = dot32(pick, table[...]).astype(BF)
            es[m, :] = e
            mixed = (g.astype(F32) * e.astype(F32)).astype(BF)
            q_now[m, :] = dot32(mixed, wp[...]).astype(BF)
            acc[m, :] = jnp.zeros((m.size, acc.shape[1]), F32)

    for m in chunks(n_tok, ROWS_B):
        h = dot32(u_now[m, :], wu[...]).astype(BF)
        hs[m, :] = h
        acc[m, :] += dot32(gelu(h.astype(F32)).astype(BF), wd[...])

    @pl.when(step == n_f - 1)
    def _():
        for m in chunks(n_tok, ROWS_A):
            x = x_now[m, :].astype(F32) + acc[m, :].astype(BF).astype(F32) + q_now[m, :].astype(F32)
            x_now[m, :] = x.astype(BF)

    @pl.when((step == n_f - 1) & (layer == n_l - 1))
    def _():
        xo[...] = x_now[...]


def chunks(n, size):
    size = min(n, size)
    return [pl.ds(m, size) for m in range(0, n, size)]


def forward(x0, cls, table, w_up, w_down, w_gate, w_proj):
    n_tok, dim = x0.shape
    n_l, _, ff = w_up.shape
    emb = w_gate.shape[2]
    tile = min(TILE, ff)
    n_f = ff // tile
    n_c = table.shape[1]

    def whole(l, f):
        return (l, 0, 0)

    def cols(l, f):
        return (l, 0, f)

    def fixed(l, f):
        return (0, 0)

    return pl.pallas_call(
        functools.partial(forward_kernel, n_l, n_f),
        grid=(n_l, n_f),
        in_specs=[
            pl.BlockSpec((n_tok, dim), fixed, pipeline_mode=ONCE),
            pl.BlockSpec((n_tok, 1), fixed, pipeline_mode=ONCE),
            pl.BlockSpec((None, n_c, emb), whole),
            pl.BlockSpec((None, dim, tile), cols),
            pl.BlockSpec((None, tile, dim), lambda l, f: (l, f, 0)),
            pl.BlockSpec((None, dim, emb), whole),
            pl.BlockSpec((None, emb, dim), whole),
        ],
        out_specs=[
            pl.BlockSpec((None, n_tok, dim), whole),
            pl.BlockSpec((None, n_tok, tile), cols),
            pl.BlockSpec((None, n_tok, emb), whole),
            pl.BlockSpec((None, n_tok, emb), whole),
            pl.BlockSpec((n_tok, dim), fixed),
        ],
        out_shape=[out_of((n_l, n_tok, n), BF) for n in (dim, ff, emb, emb)] + [out_of((n_tok, dim), BF)],
        scratch_shapes=[pltpu.VMEM((n_tok, dim), t) for t in (BF, BF, F32, BF)],
        compiler_params=params("arbitrary", "arbitrary"),
        cost_estimate=cost(n_l * n_tok * dim * (2 * ff + 2 * emb + n_c), n_l),
        name="forward",
    )(x0, cls, table, w_up, w_down, w_gate, w_proj)


def params(*kinds, **more):
    return pltpu.CompilerParams(vmem_limit_bytes=VMEM, dimension_semantics=kinds or None, **more)


def cost(products, layers):
    return pl.CostEstimate(flops=2 * products, bytes_accessed=layers * 40_000_000, transcendentals=0)


def spec(shape, *index, **more):
    index = index or (0,) * len(shape)
    return pl.BlockSpec(shape, lambda *_: index, **more)


ANY = pl.BlockSpec(memory_space=pl.ANY)


def out_of(shape, dtype=F32):
    return jax.ShapeDtypeStruct(shape, dtype)


def backward_kernel(n_l, n_f, r_in, ss, wp, es, wg, xs, cls_t, hs, wu, wd, sums_out, out,
                    r, c_now, acc, three, s_now, p_now, e_now, g_now, x_now, sums, totals, loads, sems, sems_few, sems_f, *bufs):
    step = pl.program_id(0)
    f, n_full = step % n_f, (n_l - 1) * n_f
    n_tok = len(c_now)
    parts = chunks(n_tok, ROWS_B)
    n_hot, n_tot = COLD_AT - HOT_AT, n_l * RUN
    at = Place()
    folds = [Fold(at, sums.at[i, pl.ds(0, FREQ)], bufs[i * len(bufs) // n_l:(i + 1) * len(bufs) // n_l], sems_f.at[i]) for i in range(n_l)]
    alls = [Spread(at, sums.at[i, pl.ds(HOT_AT, n_hot)], lambda d, i=i: out.at[d, pl.ds(n_hot * i, n_hot)], sems.at[i]) for i in range(n_l)]
    few = Spread(at, totals, lambda d: out.at[d, pl.ds(n_hot * n_l, n_tot)], sems_few)

    def total(i):
        t = folds[i].total()
        for z in STOPS:
            @pl.when(at.z == z)
            def _(z=z):
                totals[pl.ds(i * RUN, RUN), :] = t[z * RUN:(z + 1) * RUN, :]

    def load(layer, which):
        srcs = (wp, p_now), (ss, s_now), (es, e_now), (wg, g_now), (xs, x_now)
        return [pltpu.make_async_copy(srcs[i][0].at[layer], srcs[i][1], loads.at[i]) for i in which]

    early, late = range(4), range(4, 5)
    layer = n_l - 1 - step // n_f
    first = pltpu.make_async_copy(r_in, c_now, loads.at[5])

    plan = {}
    for i in range(n_l):
        steps = [(1, folds[i].begin, ()), (2, folds[i].step, (0,)), (2, alls[i].begin, ()), (4, folds[i].step, (1,)), (5, alls[i].column, (1,)),
                 (6, alls[i].onward, (0,)), (7, folds[i].step, (2,)), (8, alls[i].column, (2,)), (9, alls[i].onward, (1,)), (9, total, (i,)),
                 (10, alls[i].across, (0,)), (10, alls[i].onward, (2,)), (11, alls[i].column, (3,)), (12, alls[i].across, (1,)),
                 (13, alls[i].across, (2,)), (14, alls[i].onward, (3,)), (17, alls[i].across, (3,))]
        for when, what, args in steps:
            plan.setdefault(10 * i + when, []).append((what, args))
    few_steps = [few.begin], *[[few.column, few.onward]] * 3, [few.onward], [few.across] * 4
    for k, steps in enumerate(few_steps):
        for j, what in enumerate(steps):
            args = () if not k else (k - j,) if k < 4 else (3,) if k == 4 else (j,)
            plan.setdefault(10 * n_l + k - 0.5, []).append((what, args))

    def point(k, now, layers):
        for i in range(layers):
            if 10 * i + k in plan:
                @pl.when(step == i * n_f + now)
                def _(i=i):
                    for what, args in plan.pop(10 * i + k):
                        what(*args)

    @pl.when(step == 0)
    def _():
        first.start()
        for c in load(layer, early):
            c.start()
        at.meet()
        first.wait()
        r[...] = c_now[...].astype(F32)

    @pl.when(f == 0)
    def _():
        for c in load(layer, early):
            c.wait()
        for c in load(layer, late):
            c.start()
        for m in parts:
            c = r[m, :].astype(BF)
            c_now[m, :] = c
            a = dot_nt(c, p_now[...])
            s = s_now[m, :].astype(F32)
            rows = gelu(s).astype(BF).astype(F32) * a
            for j, part in enumerate(split3(rows)):
                three[j, m, :] = part
            e_now[m, :] = (gelu_slope(s) * (a * e_now[m, :].astype(F32))).astype(BF)
        point(0, 0, n_l)
        class_sums(cls_t, three, sums.at[step // n_f])
        point(1, 0, n_l)

    @pl.when((f == 0) & (step < n_full))
    def _():
        for m in parts:
            acc[m, :] = dot_nt(e_now[m, :], g_now[...])

    @pl.when((f == 1) & (step < n_full))
    def _():
        for c in load(layer - 1, early):
            c.start()

    @pl.when(step < n_full)
    def _():
        for i, m in enumerate(parts):
            d_act = dot_nt(c_now[m, :], wd[...])
            dh = (gelu_slope(hs[m, :].astype(F32)) * d_act).astype(BF)
            acc[m, :] += dot_nt(dh, wu[...])
            for k in range(n_f):
                point(2 + 2 * k + i, k, n_l - 1)

    @pl.when((f == n_f - 1) & (step < n_full))
    def _():
        for c in load(layer, late):
            c.wait()
        for m in chunks(n_tok, ROWS_A):
            x = x_now[m, :].astype(F32)
            k = lax.rsqrt(jnp.mean(x * x, axis=-1, keepdims=True) + NORM_EPS)
            du = acc[m, :]
            inner = jnp.mean(du * x, axis=-1, keepdims=True)
            r[m, :] = r[m, :] + k * du - x * (k * k * k) * inner

    @pl.when(step == n_full)
    def _():
        for c in load(layer, late):
            c.wait()
        keep = pltpu.make_async_copy(sums, sums_out, loads.at[5])
        keep.start()
        for k in sorted(plan):
            for what, args in plan[k]:
                what(*args)
        for v in (*alls, few):
            v.end()
        keep.wait()


def backward(r_in, cls_t, es, xs, hs, ss, w_up, w_down, w_gate, w_proj, n_dev):
    n_tok, dim = r_in.shape
    n_l, _, ff = w_up.shape
    emb = w_gate.shape[2]
    n_c = COLD_AT + COLD_MAX
    n_f = 4
    tile = ff // n_f
    n_full = (n_l - 1) * n_f
    n_out = n_l * (COLD_AT - HOT_AT + RUN)

    def at_layer(t):
        t = jnp.minimum(t, n_full - 1)
        return n_l - 1 - t // n_f, t % n_f

    def cols(n):
        return pl.BlockSpec((None, n, tile), lambda t: (at_layer(t)[0], 0, at_layer(t)[1]))

    return pl.pallas_call(
        functools.partial(backward_kernel, n_l, n_f),
        grid=(n_full + 1,),
        in_specs=[ANY] * 6 + [spec((1, n_tok), pipeline_mode=ONCE), cols(n_tok), cols(dim),
                              pl.BlockSpec((None, tile, dim), lambda t: (*at_layer(t), 0))],
        out_specs=[ANY] * 2,
        out_shape=[out_of((n_l, n_c, emb)), out_of((n_dev, n_out, emb))],
        scratch_shapes=[pltpu.VMEM((n_tok, dim), F32), pltpu.VMEM((n_tok, dim), BF), pltpu.VMEM((n_tok, dim), F32), pltpu.VMEM((3, n_tok, emb), BF)]
        + [pltpu.VMEM(v, BF) for v in ((n_tok, emb), (emb, dim), (n_tok, emb), (dim, emb), (n_tok, dim))]
        + [pltpu.VMEM((n_l, n_c, emb), F32), pltpu.VMEM((n_l * RUN, emb), F32), pltpu.SemaphoreType.DMA((6,)),
           pltpu.SemaphoreType.DMA((n_l, *SPREAD_SEMS)), pltpu.SemaphoreType.DMA(SPREAD_SEMS), pltpu.SemaphoreType.DMA((n_l, *FOLD_SEMS))]
        + fold_bufs(emb) * n_l,
        compiler_params=params("arbitrary", collective_id=0, has_side_effects=True),
        cost_estimate=cost(n_l * n_tok * dim * (2 * ff + 2 * emb + 3 * n_c), n_l),
        name="backward",
    )(r_in, ss, w_proj, es, w_gate, xs, cls_t, hs, w_up, w_down)


def count_kernel(ids, out, zeros, blank, sem):
    n_tok = ids.shape[1]
    blank[...] = jnp.zeros(blank.shape, F32)
    blanks = [pltpu.make_async_copy(blank, zeros.at[pl.ds(i, len(blank))], sem) for i in range(0, len(zeros), len(blank))]
    for c in blanks:
        c.start()
    out[...] = jnp.zeros(out.shape, F32)

    def hits(v, n):
        same = v.astype(F32).astype(BF) == iota((n, n_tok), 0).astype(F32).astype(BF)
        return jnp.where(same, jnp.ones((), BF), jnp.zeros((), BF))

    @pl.loop(0, len(ids) // RUN)
    def _(i):
        got = []
        for j in range(RUN):
            ids_j = ids[pl.ds(i * RUN + j, 1), :]
            got.append(dot_nt(hits(ids_j >> HI_BITS, len(out)), hits(ids_j & (LO - 1), LO)))
        out[...] += sum(got)

    for c in blanks:
        c.wait()


def count_ids(ids, n_hi, shape):
    return pl.pallas_call(
        count_kernel, out_shape=[out_of((n_hi, LO)), out_of(shape)], out_specs=[pl.BlockSpec(memory_space=pltpu.VMEM), ANY],
        scratch_shapes=[pltpu.VMEM((shape[0] // 12, *shape[1:]), F32), pltpu.SemaphoreType.DMA(())],
        compiler_params=params(), name="count_ids")(ids)


def pack_kernel(row_of, table, out, sem):
    @pl.loop(0, len(out))
    def _(k):
        pltpu.make_async_copy(table.at[row_of[k]], out.at[k], sem).start()

    pltpu.make_async_copy(table.at[pl.ds(0, len(out))], out, sem).wait()


def pack_rows(row_of, table):
    shape = row_of.shape + table.shape[1:]
    return pl.pallas_call(
        pack_kernel,
        grid_spec=pltpu.PrefetchScalarGridSpec(num_scalar_prefetch=1, grid=(1,), in_specs=[ANY], out_specs=spec(shape),
                                               scratch_shapes=[pltpu.SemaphoreType.DMA(())]),
        out_shape=out_of(shape, table.dtype), compiler_params=params(), name="pack_rows",
    )(row_of, table)


class Place:
    def __init__(self):
        me = lax.axis_index('emb')
        self.core, self.x, self.y, self.z = me % 2, (me // 2) % 2, (me // 4) % 2, me // 8
        self.columns = [self.z, self.z + 1 - self.z % 2 * 2, (self.z + 2) % 4, 3 - self.z]
        self.others = [self.dev(z=z) for z in self.columns[1:]]
        self.to_x, self.to_y, self.to_core = self.dev(x=1 - self.x), self.dev(y=1 - self.y), self.dev(core=1 - self.core)

    def dev(self, z=None, y=None, x=None, core=None):
        z, y, x, core = [mine if v is None else v for v, mine in ((z, self.z), (y, self.y), (x, self.x), (core, self.core))]
        return ((z * 2 + y) * 2 + x) * 2 + core

    def meet(self):
        barrier = pltpu.get_barrier_semaphore()
        peers = self.others + [self.to_x, self.to_y, self.to_core]
        for peer in peers:
            pl.semaphore_signal(barrier, device_id=(peer,), device_id_type=pl.DeviceIdType.MESH)
        pl.semaphore_wait(barrier, len(peers))


def remote(src, dst, sems, to):
    return pltpu.make_async_remote_copy(src_ref=src, dst_ref=dst, send_sem=sems[0], recv_sem=sems[1],
                                        device_id=(to,), device_id_type=pl.DeviceIdType.MESH)


Z, X, Y, FX, FY, C, CX, CY, CD, OWN = range(10)


class Spread:
    def __init__(self, at, mine, slot, sems):
        self.at, self.mine, self.slot, self.sems = at, mine, slot, sems
        n = mine.shape[0]
        half = n // 16 * 8
        self.halves = {FY: pl.ds(0, half), FX: pl.ds(half, n - half)}
        self.col = [at.dev(z=z) for z in at.columns]
        self.by_x = [at.dev(z=z, x=1 - at.x) for z in at.columns]
        self.by_y = [at.dev(z=z, y=1 - at.y) for z in at.columns]
        self.by_d = [at.dev(z=z, x=1 - at.x, y=1 - at.y) for z in at.columns]
        self.far = [[at.dev(z=z, x=x, y=y, core=1 - at.core) for z in at.columns]
                    for y, x in ((at.y, at.x), (at.y, 1 - at.x), (1 - at.y, at.x), (1 - at.y, 1 - at.x))]
        self.done = []

    def pair(self, kind, k):
        return self.sems.at[0, kind, k], self.sems.at[1, kind, k]

    def send(self, kind, k, src, dst, to):
        remote(src, dst, self.pair(kind, k), to).start()
        self.done.append((kind, k))

    def got(self, kind, k, block):
        remote(block, block, self.pair(kind, k), self.at.to_x).wait_recv()

    def begin(self):
        own = self.slot(self.col[0])
        pltpu.make_async_copy(self.mine, own, self.sems.at[0, OWN, 0]).start()
        for k, other in enumerate(self.at.others):
            self.send(Z, k + 1, self.mine, own, other)
        self.column(0)

    def column(self, k):
        block = self.slot(self.col[k])
        if k:
            self.got(Z, k, block)
        src = block if k else self.mine
        for kind, to in ((X, self.at.to_x), (Y, self.at.to_y), (C, self.at.to_core)):
            self.send(kind, k, src, block, to)

    def onward(self, k):
        for kind, part, to, other, core in ((X, self.by_x, self.at.to_y, FY, CX), (Y, self.by_y, self.at.to_x, FX, CY)):
            block = self.slot(part[k])
            self.got(kind, k, block)
            half = block.at[self.halves[other]]
            self.send(other, k, half, half, to)
            self.send(core, k, block, block, self.at.to_core)

    def across(self, k):
        block = self.slot(self.by_d[k])
        for kind, half in self.halves.items():
            self.got(kind, k, block.at[half])
        self.send(CD, k, block, block, self.at.to_core)

    def end(self):
        for k in STOPS:
            for kind, far in zip((C, CX, CY, CD), self.far):
                self.got(kind, k, self.slot(far[k]))
        own = self.slot(self.col[0])
        for kind, k in self.done:
            block = own.at[self.halves[kind]] if kind in self.halves else own
            remote(block, block, self.pair(kind, k), self.at.to_x).wait_send()
        pltpu.make_async_copy(self.mine, own, self.sems.at[0, OWN, 0]).wait()


class Fold:
    def __init__(self, at, part, bufs, sems):
        self.at, self.part, self.sems = at, part, sems
        self.ins, self.sums, self.all_z = bufs[:3], bufs[3:5], bufs[5]
        self.bits = at.core, at.x, at.y
        self.to = at.to_core, at.to_x, at.to_y

    def pair(self, i, k=0):
        return self.sems.at[0, i, k], self.sems.at[1, i, k]

    def cut(self, i, bit):
        n = self.ins[i].shape[0]
        return pl.ds(pl.multiple_of(bit * n, n), n)

    def source(self, i):
        return self.sums[i - 1] if i else self.part

    def hop(self, i):
        return remote(self.source(i).at[self.cut(i, 1 - self.bits[i])], self.ins[i], self.pair(i), self.to[i])

    def begin(self):
        self.hop(0).start()

    def step(self, i):
        self.hop(i).wait_recv()
        total = self.source(i)[self.cut(i, self.bits[i]), :] + self.ins[i][...]
        if i < 2:
            self.sums[i][...] = total
            self.hop(i + 1).start()
        else:
            self.all_z[self.at.z] = total
            for k, other in enumerate(self.at.others):
                self.along_z(k, other).start()

    def along_z(self, k, other):
        block = self.all_z.at[self.at.z]
        return remote(block, block, self.pair(3, k), other)

    def total(self):
        for k, other in enumerate(self.at.others):
            self.along_z(k, other).wait_recv()
        for i in range(3):
            self.hop(i).wait_send()
        for k, other in enumerate(self.at.others):
            self.along_z(k, other).wait_send()
        v = self.all_z
        return (v[0] + v[1]) + (v[2] + v[3])


def fold_bufs(emb):
    return [pltpu.VMEM((n, emb), F32) for n in (64, 32, 16, 64, 32)] + [pltpu.VMEM((4, 16, emb), F32)]


SPREAD_SEMS = (2, 10, 4)
STOPS = range(4)
FOLD_SEMS = (2, 4, 4)
HOT_AT, COLD_AT = FREQ, FREQ + 64


def class_sums(cls_t, three, sums):
    pick_t = (cls_t[...] == iota((sums.shape[0], cls_t.shape[1]), 0)).astype(BF)
    hi, mid, lo = [dot32(pick_t, three[i]) for i in range(3)]
    sums[...] = hi + (mid + lo)


ORDER = [(b & 3) * 8 + (b >> 2 & 1) * 4 + (b >> 3 & 1) * 2 + (b >> 4) for b in range(FREQ // RUN)]


def hot_kernel(any_freq, raw, freq, code, out, parts):
    n_dev, n_r, _ = raw.shape
    layer, block = pl.program_id(0), pl.program_id(1)
    n = RUN * n_dev
    for g in range(n_r // RUN):
        for o in range(n_dev):
            out[pl.ds(g * n + o * RUN, RUN), :] = raw[o, pl.ds(g * RUN, RUN), :]

    @pl.when(any_freq[block] > 0)
    def _():
        for j in range(freq.shape[1] // RUN):
            @pl.when(layer == j)
            def _(j=j):
                rows = jnp.concatenate([freq[o, j * RUN:(j + 1) * RUN, :] for o in ORDER])
                for i, part in enumerate(split3(rows)):
                    parts[i] = part
        sel = (code[...] == iota((n_r * n_dev, FREQ), 1)).astype(BF)
        out[...] += dot32(sel, parts[0]) + (dot32(sel, parts[1]) + dot32(sel, parts[2]))


def hot_out(gathered, code, n_l):
    n_dev, n_rows, emb = gathered.shape
    n_r = 4 * RUN
    width = n_r * n_dev
    blocks = len(code) // width
    return pl.pallas_call(
        hot_kernel,
        grid_spec=pltpu.PrefetchScalarGridSpec(
            num_scalar_prefetch=1, grid=(n_l, blocks),
            in_specs=[
                pl.BlockSpec((n_dev, n_r, emb), lambda i, b, _: (0, i * blocks + b, 0)),
                spec((n_dev, n_l * RUN, emb), 0, n_rows // (n_l * RUN) - 1, 0, pipeline_mode=ONCE),
                pl.BlockSpec((width, 1), lambda i, b, _: (b, 0)),
            ],
            out_specs=pl.BlockSpec((None, width, emb), lambda i, b, _: (n_l - 1 - i, b, 0)),
            scratch_shapes=[pltpu.VMEM((3, FREQ, emb), BF)]),
        out_shape=out_of((n_l, len(code), emb)),
        compiler_params=params("arbitrary", "arbitrary"),
        cost_estimate=cost(gathered.size * LO, n_l), name="hot_out",
    )((code.reshape(blocks, width) >= 0).any(axis=1).astype(I32), gathered, gathered, code.reshape(-1, 1))


def rows_kernel(numbers, row_of, sums, freq, into, out, stage, got, sem):
    n_used, cold_row, cold_no = [numbers[i] for i in range(3)]
    n_l = len(sums)

    def put(k, row):
        return pltpu.make_async_copy(stage.at[pl.ds(k, 1)], out.at[pl.ds(row, 1)], sem)

    def fill(k, src, at):
        for i in range(n_l):
            stage[k, pl.ds(n_l - 1 - i, 1), :] = src(i, at)

    @pl.loop(0, n_used)
    def _(k):
        fill(k, lambda i, at: sums[i, pl.ds(at, 1), :], COLD_AT + k)
        put(k, row_of[k]).start()

    @pl.when(cold_row >= 0)
    def _():
        c = pltpu.make_async_copy(freq.at[len(freq) - 1, pl.ds(n_l * (COLD_AT - HOT_AT), n_l * RUN)], got, sem)
        c.start()
        c.wait()
        fill(COLD_MAX, lambda i, at: got[pl.ds(i * RUN + at, 1), :], cold_no)
        put(COLD_MAX, cold_row).start()
        put(0, 0).wait()

    @pl.loop(0, n_used)
    def _(k):
        put(0, 0).wait()


def put_rows(numbers, row_of, sums, freq, into):
    n_l, _, emb = sums.shape
    return pl.pallas_call(
        rows_kernel,
        grid_spec=pltpu.PrefetchScalarGridSpec(
            num_scalar_prefetch=2, grid=(1,),
            in_specs=[spec(sums.shape), ANY, ANY], out_specs=ANY,
            scratch_shapes=[pltpu.VMEM((COLD_MAX + 1, n_l, emb), F32), pltpu.VMEM((n_l * RUN, emb), F32), pltpu.SemaphoreType.DMA(())]),
        out_shape=out_of(into.shape), input_output_aliases={4: 0},
        compiler_params=params("arbitrary"), name="put_rows",
    )(numbers, row_of, sums, freq, into)


def merge_kernel(keep, *refs):
    n = (len(refs) - 1) // 3
    sem = refs[-1]

    @pl.when(keep[0] == 0)
    def _():
        copies = [pltpu.make_async_copy(src, dst, sem.at[i]) for i, (src, dst) in enumerate(zip(refs[n:2 * n], refs[2 * n:]))]
        for c in copies:
            c.start()
        for c in copies:
            c.wait()


def merge(keep, fast, general):
    n = len(fast)
    return pl.pallas_call(
        merge_kernel,
        in_specs=[pl.BlockSpec(memory_space=pltpu.SMEM)] + [ANY] * 2 * n, out_specs=[ANY] * n,
        out_shape=[out_of(v.shape, v.dtype) for v in fast], scratch_shapes=[pltpu.SemaphoreType.DMA((n,))],
        input_output_aliases={i + 1: i for i in range(n)}, name="merge",
    )(keep, *fast, *general)


def empty_kernel(*_):
    pass


def empty(like):
    return pl.pallas_call(empty_kernel, out_specs=[ANY] * len(like), out_shape=[out_of(v.shape, v.dtype) for v in like], name="empty")()


def down_sum(v):
    return jnp.sum(v, axis=0)


def beside(*v):
    return jnp.concatenate(v, axis=1)


def row_sum(v):
    return jnp.sum(v, axis=1)


def square(n):
    return iota((n, n), 0), iota((n, n), 1)


def prefix(v):
    r, c = square(len(v))
    return row_sum(jnp.where(r > c, row(v), 0))


def digits(ids, n_hi):
    return one_hot(ids >> HI_BITS, n_hi), one_hot(ids & (LO - 1), LO)


def look(hi_lo, *maps):
    hi, lo = hi_lo
    got = dot32(hi, beside(*maps))
    return [row_sum(got[:, i * LO:(i + 1) * LO] * lo.astype(F32)).astype(I32) for i in range(len(maps))]


def number(count, most):
    levels = jnp.array(LEVELS, F32)
    n_over = jnp.sum((count[:, :, None] >= levels).astype(F32), axis=(0, 1))
    flag = count >= jnp.min(jnp.where(n_over <= most, levels, jnp.inf))
    r, c = square(LO)
    in_row = dot32(flag.astype(BF), (r < c).astype(BF))
    return jnp.where(flag, in_row + col(prefix(row_sum(flag.astype(F32)))) + 1, 0)


def solution(mesh):
    n_dev = mesh.shape['emb']

    def body(token_ids, hot_ids, x_in, d_out, emb_table, hot_table, w_up, w_down, w_gate, w_proj):
        n_loc = len(token_ids)
        layers, rows_dev, emb_dim = emb_table.shape
        n_hot = len(hot_ids)
        places, hot_dev = n_loc // n_dev, n_hot // n_dev
        n_hi = -(-rows_dev * n_dev // (8 * LO)) * 8
        me = lax.axis_index('emb')
        hot_at, cold_at = FREQ, FREQ + hot_dev

        def exchange(v):
            return swap(v.reshape(n_dev, places, -1)).reshape(n_loc, -1)

        def prepare(got_class, hot_hi, hot_lo, row_used, cold_owner, freq_cold, freq_map, hot_table, by_row, move, d_out):
            (hot_f,) = look((hot_hi, hot_lo), freq_map)
            used_rank = prefix(row_used.astype(I32))
            at_rank = (row(used_rank) == iota((COLD_MAX, rows_dev), 0)) & row(row_used)
            row_of = row_sum(jnp.where(at_rank, iota((COLD_MAX, rows_dev), 1), 0))
            packed = pack_rows(row_of, by_row)
            mine_no = jnp.where(hot_owner == me, FREQ_HOT + hot_place, -1)
            hot_pick = (one_hot(hot_f - 1, FREQ_HOT + hot_dev) * col((hot_f <= FREQ_HOT).astype(BF)) + one_hot(mine_no, FREQ_HOT + hot_dev)).T
            hot_rows = [dot32(hot_pick, hot_table[i]).astype(BF) for i in range(layers)]
            table = jnp.stack([jnp.concatenate([
                hot_rows[i][:FREQ_HOT], dot32(one_hot(cold_owner, n_dev), freq_cold[:, i]).astype(BF),
                hot_rows[i][FREQ_HOT:], packed[:, i]]) for i in range(layers)])
            n_used = jnp.minimum(jnp.sum(row_used.astype(I32)), COLD_MAX)
            row_no = got_class - cold_at
            used_before = row_sum(jnp.where(row(row_used) & (iota((n_loc, rows_dev), 1) < col(row_no)), 1, 0))
            cls = jnp.where(row_no >= 0, cold_at + used_before, got_class)
            code = jnp.where(hot_f <= FREQ_HOT, hot_f - 1, -1)
            d_placed = dot32(move, d_out).astype(BF)
            return d_placed, table, cls, n_used, row_of, code

        count, zeros = count_ids(swap(jnp.broadcast_to(row(token_ids), (n_dev, n_loc))), n_hi, (rows_dev, layers, emb_dim))
        tok, hot = digits(token_ids, n_hi), digits(hot_ids, n_hi)
        slot_no = jnp.arange(n_hot, dtype=I32)
        hot_place = slot_no // (RUN * n_dev) * RUN + slot_no % RUN
        hot_owner = slot_no // RUN % n_dev
        q_map = dot32(hot[0].T, hot[1] * col((hot_place + 1).astype(BF))).astype(BF)
        r_map = dot32(hot[0].T, hot[1] * col(hot_owner.astype(BF))).astype(BF)
        hot_no = number(jnp.where(q_map > 0, count, 0), FREQ_HOT)
        cold_no = number(jnp.where(q_map > 0, 0, count), FREQ_COLD)
        freq_map = jnp.where(hot_no > 0, hot_no, jnp.where(cold_no > 0, FREQ_HOT + cold_no, 0)).astype(BF)
        id_map = iota((n_hi, LO), 0) * LO + iota((n_hi, LO), 1) + 1
        cold_id = jnp.sum(jnp.where(cold_no.astype(I32)[None] == iota((FREQ_COLD, 1, 1), 0) + 1, id_map[None], 0), axis=(1, 2)) - 1
        cold_owner = jnp.where(cold_id >= 0, cold_id // rows_dev, -1)
        my_cold = (cold_owner == me).astype(I32)
        my_row = jnp.minimum(jnp.sum(my_cold * (cold_id - me * rows_dev + 1)) - 1, rows_dev - 1)
        by_row = emb_table.transpose(1, 0, 2)
        cold_row = lax.dynamic_slice_in_dim(by_row, jnp.maximum(my_row, 0), 1)
        freq_cold = swap(jnp.broadcast_to(cold_row, (n_dev, layers, emb_dim)))

        tok_f, tok_q, tok_r = look(tok, freq_map, q_map, r_map)
        rare = tok_f == 0
        owner = jnp.where(tok_q > 0, tok_r, token_ids // rows_dev)
        dev_no = iota((n_loc, n_dev), 1)
        to_dev = (col(owner) == dev_no) & col(rare)
        marks = beside(to_dev.astype(BF), col(jnp.logical_not(rare).astype(BF)))
        r, c = square(n_loc)
        ranks = dot32((r > c).astype(BF), marks)
        sent = down_sum(to_dev.astype(F32))
        free = jnp.maximum(places - sent, 0)
        free_at = prefix(free)
        fill = ranks[:, n_dev:]
        fill_dev = (fill >= free_at) & (fill < free_at + free)
        to_dev = jnp.where(col(rare), to_dev, fill_dev)
        place = jnp.where(col(rare), ranks[:, :n_dev], fill + (sent - free_at))
        slot = row_sum(jnp.where(to_dev, dev_no * places + place.astype(I32), 0))
        row_ids = me * rows_dev + jnp.arange(rows_dev, dtype=I32)
        row_f, row_q, row_n = look(digits(row_ids, n_hi), freq_map, q_map, (count > 0).astype(BF))
        row_used = (row_n > 0) & (row_f == 0) & (row_q == 0)
        fits = ((jnp.max(sent) <= places) & (jnp.sum(row_used.astype(I32)) <= COLD_MAX) & (jnp.sum(my_cold) <= 1))
        tok_class = jnp.where(rare, jnp.where(tok_q > 0, hot_at + tok_q - 1, cold_at + token_ids % rows_dev), tok_f - 1)
        bad = 1 << 20
        move = r == row(slot)
        send_class, freq_cold = lax.optimization_barrier(
            (row_sum(jnp.where(move, row(tok_class), 0)) + jnp.where(fits, 0, bad), freq_cold))
        got_class = swap(send_class.reshape(n_dev, places)).reshape(n_loc)
        move = move.astype(BF)
        placed, got_class, hot_hi, hot_lo, row_used, cold_owner = lax.optimization_barrier(
            (dot32(move, x_in).astype(BF), got_class, *hot, row_used, cold_owner))
        x_moved = exchange(placed)
        given = prepare(got_class, hot_hi, hot_lo, row_used, cold_owner, freq_cold, freq_map, hot_table, by_row, move, d_out)
        all_fit = jnp.max(got_class) < bad

        d_placed, table, cls, n_used, row_of, code = given
        d_moved = exchange(d_placed)
        cls_row = cls.reshape(1, n_loc)
        xs, hs, ss, es, x_last = forward(x_moved, cls.reshape(n_loc, 1), table, w_up, w_down, w_gate, w_proj)
        sums, gathered = backward(d_moved, cls_row, es, xs, hs, ss, w_up, w_down, w_gate, w_proj, n_dev)
        x_last, gathered = lax.optimization_barrier((x_last, gathered))
        x_back = exchange(x_last)
        numbers = jnp.stack([n_used, my_row, jnp.minimum(jnp.sum(my_cold * jnp.arange(FREQ_COLD, dtype=I32)), FREQ_COLD - 1)])
        d_table = put_rows(numbers, row_of, sums, gathered, zeros)
        d_hot = hot_out(gathered, code, layers)
        x_out = dot32((col(slot) == iota((n_loc, n_loc), 1)).astype(BF), x_back).astype(BF)
        *fast, fit = lax.optimization_barrier((x_out, d_table, d_hot, all_fit))

        def slow():
            x, table_grad, hot_grad = general_path(n_dev, me, token_ids, hot_ids, x_in, d_out, emb_table, hot_table, w_up, w_down, w_gate, w_proj)
            return x, table_grad.transpose(1, 0, 2), hot_grad

        general = lax.cond(fit, lambda: tuple(empty(fast)), slow)
        x_out, d_table, d_hot = merge(fit.astype(I32).reshape(1), fast, general)
        return x_out, d_table.transpose(1, 0, 2), d_hot

    return jax.shard_map(body, mesh=mesh,
                         in_specs=(P('emb'), P(), P('emb', None), P('emb', None), P(None, 'emb', None), P(), P(), P(), P(), P()),
                         out_specs=(P('emb', None), P(None, 'emb', None), P()),
                         check_vma=False)
```

```python
import functools

import jax
import jax.numpy as jnp
from jax import lax
from jax.experimental import pallas as pl
from jax.experimental.pallas import tpu as pltpu
from jax.sharding import PartitionSpec as P


NORM_EPS = 1e-6
FREQ_HOT = 124
FREQ_COLD = 4
FREQ = FREQ_HOT + FREQ_COLD
COLD_MAX = 256
LO = 256
HI_BITS = 8
RUN = 4
LEVELS = tuple(12 * 2 ** (i / 6) for i in range(27))
GELU_A = 0.7978845608028654
GELU_B = GELU_A * 0.044715
VMEM = 66_000_000
ROWS_A = 256
ROWS_B = 512
TILE = 1024
BF = jnp.bfloat16
F32 = jnp.float32
I32 = jnp.int32
ONCE = pl.Buffered(1)


def gelu_back(pre_act, cot_in):
    _, pull = jax.vjp(jax.nn.gelu, pre_act.astype(F32))
    return pull(cot_in)[0]


def swap(v):
    return lax.all_to_all(v, 'emb', 0, 0, tiled=True)


def col(v):
    return v[:, None]


def row(v):
    return v[None, :]


def dot32(a, b):
    return jnp.dot(a, b, preferred_element_type=F32)


def dense_parts(resid, w_up, w_gate):
    resid_f = resid.astype(F32)
    inv_rms = lax.rsqrt(jnp.mean(resid_f * resid_f, axis=-1, keepdims=True) + NORM_EPS)
    normed = (resid_f * inv_rms).astype(BF)
    hidden = dot32(normed, w_up).astype(BF)
    gate_pre = dot32(normed, w_gate).astype(BF)
    return resid_f, inv_rms, hidden, gate_pre


def layer_forward(resid, emb_rows, w_up, w_down, w_gate, w_proj):
    resid_f, _, hidden, gate_pre = dense_parts(resid, w_up, w_gate)
    activated = jax.nn.gelu(hidden.astype(F32)).astype(BF)
    mlp_out = dot32(activated, w_down).astype(BF)
    gate = jax.nn.gelu(gate_pre.astype(F32)).astype(BF)
    mixed = (gate.astype(F32) * emb_rows.astype(F32)).astype(BF)
    projected = dot32(mixed, w_proj).astype(BF)
    return (resid_f + mlp_out.astype(F32) + projected.astype(F32)).astype(BF)


def layer_backward(resid, emb_rows, d_next, w_up, w_down, w_gate, w_proj):
    resid_f, inv_rms, hidden, gate_pre = dense_parts(resid, w_up, w_gate)
    gate = jax.nn.gelu(gate_pre.astype(F32)).astype(BF)
    d_cast = d_next.astype(BF)
    d_mixed = jnp.einsum('nd,ed->ne', d_cast, w_proj, preferred_element_type=F32)
    d_rows = gate.astype(F32) * d_mixed
    d_gpre = gelu_back(gate_pre, d_mixed * emb_rows.astype(F32))
    d_hidden = gelu_back(hidden, jnp.einsum('nd,fd->nf', d_cast, w_down, preferred_element_type=F32))
    d_normed = (jnp.einsum('nf,df->nd', d_hidden.astype(BF), w_up, preferred_element_type=F32)
                + jnp.einsum('ne,de->nd', d_gpre.astype(BF), w_gate, preferred_element_type=F32))
    inner = jnp.mean(d_normed * resid_f, axis=-1, keepdims=True)
    d_prev = d_next + inv_rms * d_normed - resid_f * (inv_rms * inv_rms * inv_rms) * inner
    return d_prev, d_rows


def general_path(n_dev, my_index, token_ids, hot_ids, x_in, d_out, emb_table, hot_table, w_up, w_down, w_gate, w_proj):
    n_loc = token_ids.shape[0]
    _, rows_dev, emb_dim = emb_table.shape
    capacity = max(8, (2 * n_loc) // n_dev)
    n_slots = n_dev * capacity
    hot_match = col(token_ids) == row(hot_ids)
    is_hot = hot_match.any(1)
    hot_pick = hot_match.astype(BF)
    hot_pick_f = hot_match.astype(F32)
    owner_id = token_ids // rows_dev
    to_owner = (col(owner_id) == row(jnp.arange(n_dev, dtype=I32))) & col(jnp.logical_not(is_hot))
    owner_rank = jnp.cumsum(to_owner.astype(jnp.int32), axis=0) - 1
    place = row_sum(jnp.where(to_owner, owner_rank, 0))
    slot = jnp.where(is_hot, n_slots, owner_id * capacity + place)
    none = jnp.full((n_slots,), -1, I32)
    send_ids = none.at[slot].set(token_ids, mode='drop')
    slot_tok = none.at[slot].set(jnp.arange(n_loc, dtype=jnp.int32), mode='drop')
    recv_ids = swap(send_ids.reshape(n_dev, capacity)).reshape(n_slots)
    served_ok = recv_ids >= 0
    local_row = jnp.where(served_ok, recv_ids - my_index * rows_dev, 0)
    pick_slot = jnp.minimum(slot, n_slots - 1)
    slot_used = slot_tok >= 0
    slot_src = jnp.maximum(slot_tok, 0)

    def fwd(resid, per_layer):
        table, hot_l, up, down, gate_w, proj = per_layer
        served = table[local_row]
        fetched = swap(served.reshape(n_dev, capacity, emb_dim)).reshape(n_slots, emb_dim)
        cold_rows = fetched[pick_slot]
        hot_rows = dot32(hot_pick, hot_l).astype(BF)
        emb_rows = jnp.where(col(is_hot), hot_rows, cold_rows)
        return layer_forward(resid, emb_rows, up, down, gate_w, proj), (resid, emb_rows)

    x_first = jnp.where(n_loc * hot_ids[0] >= 0, x_in, 0)
    x_out, (x_saved, rows_saved) = lax.scan(fwd, x_first, (emb_table, hot_table, w_up, w_down, w_gate, w_proj))

    def bwd(d_resid, per_layer):
        resid_l, rows_l, up, down, gate_w, proj = per_layer
        d_resid, d_rows = layer_backward(resid_l, rows_l, d_resid, up, down, gate_w, proj)
        outgoing = jnp.where(col(slot_used), d_rows[slot_src], 0.0)
        incoming = swap(outgoing.reshape(n_dev, capacity, emb_dim)).reshape(n_slots, emb_dim)
        d_tab = jax.ops.segment_sum(jnp.where(col(served_ok), incoming, 0.0), local_row, num_segments=rows_dev)
        hot_local = jnp.einsum('nh,ne->he', hot_pick_f, d_rows, precision=lax.Precision.HIGHEST, preferred_element_type=F32)
        return d_resid, (d_tab, lax.psum(hot_local, 'emb'))

    _, (d_table, d_hot) = lax.scan(bwd, d_out.astype(F32), (x_saved, rows_saved, w_up, w_down, w_gate, w_proj), reverse=True)
    return x_out, d_table, d_hot


def split3(v):
    hi = v.astype(BF)
    rest = v - hi.astype(F32)
    mid = rest.astype(BF)
    return hi, mid, (rest - mid.astype(F32)).astype(BF)


def iota(shape, dim):
    return lax.broadcasted_iota(jnp.int32, shape, dim)


def one_hot(v, n, dtype=BF):
    return (col(v) == iota((len(v), n), 1)).astype(dtype)


def dot_nt(a, b):
    return lax.dot_general(a, b, (((1,), (1,)), ((), ())), preferred_element_type=F32)


def gelu(x):
    half = 0.5 * x
    return half + half * jnp.tanh(x * (GELU_A + GELU_B * (x * x)))


def gelu_slope(x):
    sq = x * x
    th = jnp.tanh(x * (GELU_A + GELU_B * sq))
    return (0.5 + 0.5 * th) + (0.5 * x) * (1.0 - th * th) * (GELU_A + (3.0 * GELU_B) * sq)


def forward_kernel(n_l, n_f, n_dev, x0, cls, table, wu, wd, wg, wp, d_in, xs, hs, ss, es, xo, d_got, x_now, u_now, acc, q_now, sems):
    layer, step = pl.program_id(0), pl.program_id(1)
    n_tok = x_now.shape[0]
    me = lax.axis_index('emb')
    places = n_tok // n_dev
    barrier = pltpu.get_barrier_semaphore()

    def block(dev):
        return pl.ds(pl.multiple_of(dev * places, places), places)

    own = pltpu.make_async_copy(d_in.at[block(me)], d_got.at[block(me)], sems.at[2])

    @pl.when((layer == 0) & (step == 0))
    def _():
        @pl.loop(1, n_dev)
        def _(k):
            pl.semaphore_signal(barrier, device_id=((me + k) % n_dev,), device_id_type=pl.DeviceIdType.MESH)

    @pl.when((layer == 0) & (step == 1))
    def _():
        own.start()
        pl.semaphore_wait(barrier, n_dev - 1)

        @pl.loop(1, n_dev)
        def _(k):
            to = (me + k) % n_dev
            remote(d_in.at[block(to)], d_got.at[block(me)], sems, to).start()

    @pl.when((layer == n_l - 1) & (step == n_f - 1))
    def _():
        others = pl.ds(0, n_tok - places)
        remote(d_in.at[others], d_got.at[others], sems, me).wait()
        own.wait()

    @pl.when((layer == 0) & (step == 0))
    def _():
        x_now[...] = x0[...]

    @pl.when(step == 0)
    def _():
        for m in chunks(n_tok, ROWS_A):
            xb = x_now[m, :]
            x = xb.astype(F32)
            xs[m, :] = xb
            u = (x * lax.rsqrt(jnp.mean(x * x, axis=-1, keepdims=True) + NORM_EPS)).astype(BF)
            u_now[m, :] = u
            s = dot32(u, wg[...]).astype(BF)
            ss[m, :] = s
            g = gelu(s.astype(F32)).astype(BF)
            pick = (cls[m, :] == iota((m.size, table.shape[0]), 1)).astype(BF)
            e = dot32(pick, table[...]).astype(BF)
            es[m, :] = e
            mixed = (g.astype(F32) * e.astype(F32)).astype(BF)
            q_now[m, :] = dot32(mixed, wp[...]).astype(BF)
            acc[m, :] = jnp.zeros((m.size, acc.shape[1]), F32)

    for m in chunks(n_tok, ROWS_B):
        h = dot32(u_now[m, :], wu[...]).astype(BF)
        hs[m, :] = h
        acc[m, :] += dot32(gelu(h.astype(F32)).astype(BF), wd[...])

    @pl.when(step == n_f - 1)
    def _():
        for m in chunks(n_tok, ROWS_A):
            x = x_now[m, :].astype(F32) + acc[m, :].astype(BF).astype(F32) + q_now[m, :].astype(F32)
            x_now[m, :] = x.astype(BF)

    @pl.when((step == n_f - 1) & (layer == n_l - 1))
    def _():
        xo[...] = x_now[...]


def chunks(n, size):
    size = min(n, size)
    return [pl.ds(m, size) for m in range(0, n, size)]


def forward(x0, cls, table, w_up, w_down, w_gate, w_proj, d_in, n_dev):
    n_tok, dim = x0.shape
    n_l, _, ff = w_up.shape
    emb = w_gate.shape[2]
    tile = min(TILE, ff)
    n_f = ff // tile
    n_c = table.shape[1]

    def whole(l, f):
        return (l, 0, 0)

    def cols(l, f):
        return (l, 0, f)

    def fixed(l, f):
        return (0, 0)

    return pl.pallas_call(
        functools.partial(forward_kernel, n_l, n_f, n_dev),
        grid=(n_l, n_f),
        in_specs=[
            pl.BlockSpec((n_tok, dim), fixed, pipeline_mode=ONCE),
            pl.BlockSpec((n_tok, 1), fixed, pipeline_mode=ONCE),
            pl.BlockSpec((None, n_c, emb), whole),
            pl.BlockSpec((None, dim, tile), cols),
            pl.BlockSpec((None, tile, dim), lambda l, f: (l, f, 0)),
            pl.BlockSpec((None, dim, emb), whole),
            pl.BlockSpec((None, emb, dim), whole),
            ANY,
        ],
        out_specs=[
            pl.BlockSpec((None, n_tok, dim), whole),
            pl.BlockSpec((None, n_tok, tile), cols),
            pl.BlockSpec((None, n_tok, emb), whole),
            pl.BlockSpec((None, n_tok, emb), whole),
            pl.BlockSpec((n_tok, dim), fixed),
            ANY,
        ],
        out_shape=[out_of((n_l, n_tok, n), BF) for n in (dim, ff, emb, emb)] + [out_of((n_tok, dim), BF)] * 2,
        scratch_shapes=[pltpu.VMEM((n_tok, dim), t) for t in (BF, BF, F32, BF)] + [pltpu.SemaphoreType.DMA((3,))],
        compiler_params=params("arbitrary", "arbitrary", collective_id=1, has_side_effects=True),
        cost_estimate=cost(n_l * n_tok * dim * (2 * ff + 2 * emb + n_c), n_l),
        name="forward",
    )(x0, cls, table, w_up, w_down, w_gate, w_proj, d_in)


def params(*kinds, **more):
    return pltpu.CompilerParams(vmem_limit_bytes=VMEM, dimension_semantics=kinds or None, **more)


def cost(products, layers):
    return pl.CostEstimate(flops=2 * products, bytes_accessed=layers * 40_000_000, transcendentals=0)


def spec(shape, *index, **more):
    index = index or (0,) * len(shape)
    return pl.BlockSpec(shape, lambda *_: index, **more)


ANY = pl.BlockSpec(memory_space=pl.ANY)


def out_of(shape, dtype=F32):
    return jax.ShapeDtypeStruct(shape, dtype)


def backward_kernel(n_l, n_f, r_in, ss, wp, es, wg, xs, cls_t, hs, wu, wd, sums_out, out,
                    r, c_now, acc, three, s_now, p_now, e_now, g_now, x_now, sums, totals, loads, sems, sems_few, sems_f, *bufs):
    step = pl.program_id(0)
    f, n_full = step % n_f, (n_l - 1) * n_f
    n_tok = len(c_now)
    parts = chunks(n_tok, ROWS_B)
    n_hot, n_tot = COLD_AT - HOT_AT, n_l * RUN
    at = Place()
    folds = [Fold(at, sums.at[i, pl.ds(0, FREQ)], bufs[i * len(bufs) // n_l:(i + 1) * len(bufs) // n_l], sems_f.at[i]) for i in range(n_l)]
    alls = [Spread(at, sums.at[i, pl.ds(HOT_AT, n_hot)], lambda d, i=i: out.at[d, pl.ds(n_hot * i, n_hot)], sems.at[i]) for i in range(n_l)]
    few = Spread(at, totals, lambda d: out.at[d, pl.ds(n_hot * n_l, n_tot)], sems_few)

    def total(i):
        t = folds[i].total()
        for z in STOPS:
            @pl.when(at.z == z)
            def _(z=z):
                totals[pl.ds(i * RUN, RUN), :] = t[z * RUN:(z + 1) * RUN, :]

    def load(layer, which):
        srcs = (wp, p_now), (ss, s_now), (es, e_now), (wg, g_now), (xs, x_now)
        return [pltpu.make_async_copy(srcs[i][0].at[layer], srcs[i][1], loads.at[i]) for i in which]

    early, late = range(4), range(4, 5)
    layer = n_l - 1 - step // n_f
    first = pltpu.make_async_copy(r_in, c_now, loads.at[5])

    plan = {}
    for i in range(n_l):
        steps = [(1, folds[i].begin, ()), (2, folds[i].step, (0,)), (2, alls[i].begin, ()), (5, folds[i].step, (1,)), (8, alls[i].onward, (0,)),
                 (9, alls[i].column, (1,)), (10, folds[i].step, (2,)), (10, alls[i].column, (2,)), (13, alls[i].onward, (1,)),
                 (13, alls[i].across, (0,)), (14, alls[i].column, (3,)), (18, total, (i,)), (19, alls[i].onward, (2,)), (21, alls[i].onward, (3,)),
                 (21, alls[i].across, (1,)), (23, alls[i].across, (2,)), (26, alls[i].across, (3,))]
        for when, what, args in steps:
            plan.setdefault(10 * i + when, []).append((what, args))
    few_steps = [few.begin], *[[few.column, few.onward]] * 3, [few.onward], [few.across] * 4
    for k, steps in enumerate(few_steps):
        for j, what in enumerate(steps):
            args = () if not k else (k - j,) if k < 4 else (3,) if k == 4 else (j,)
            plan.setdefault(10 * n_l + 8 + k / 2, []).append((what, args))

    def point(k, now, layers):
        for i in range(layers):
            if 10 * i + k in plan:
                @pl.when(step == i * n_f + now)
                def _(i=i):
                    for what, args in plan.pop(10 * i + k):
                        what(*args)

    @pl.when(step == 0)
    def _():
        first.start()
        for c in load(layer, early):
            c.start()
        at.meet()
        first.wait()
        r[...] = c_now[...].astype(F32)

    @pl.when(f == 0)
    def _():
        for c in load(layer, early):
            c.wait()
        for c in load(layer, late):
            c.start()
        for m in parts:
            c = r[m, :].astype(BF)
            c_now[m, :] = c
            a = dot_nt(c, p_now[...])
            s = s_now[m, :].astype(F32)
            rows = gelu(s).astype(BF).astype(F32) * a
            for j, part in enumerate(split3(rows)):
                three[j, m, :] = part
            e_now[m, :] = (gelu_slope(s) * (a * e_now[m, :].astype(F32))).astype(BF)
        point(0, 0, n_l)
        class_sums(cls_t, three, sums.at[step // n_f])
        point(1, 0, n_l)

    @pl.when((f == 0) & (step < n_full))
    def _():
        for m in parts:
            acc[m, :] = dot_nt(e_now[m, :], g_now[...])

    @pl.when((f == 1) & (step < n_full))
    def _():
        for c in load(layer - 1, early):
            c.start()

    @pl.when(step < n_full)
    def _():
        for i, m in enumerate(parts):
            d_act = dot_nt(c_now[m, :], wd[...])
            dh = (gelu_slope(hs[m, :].astype(F32)) * d_act).astype(BF)
            acc[m, :] += dot_nt(dh, wu[...])
            for k in range(n_f):
                point(2 + 2 * k + i, k, n_l - 1)

    @pl.when((f == n_f - 1) & (step < n_full))
    def _():
        for c in load(layer, late):
            c.wait()
        for m in chunks(n_tok, ROWS_A):
            x = x_now[m, :].astype(F32)
            k = lax.rsqrt(jnp.mean(x * x, axis=-1, keepdims=True) + NORM_EPS)
            du = acc[m, :]
            inner = jnp.mean(du * x, axis=-1, keepdims=True)
            r[m, :] = r[m, :] + k * du - x * (k * k * k) * inner

    @pl.when(step == n_full)
    def _():
        for c in load(layer, late):
            c.wait()
        keep = pltpu.make_async_copy(sums, sums_out, loads.at[5])
        keep.start()
        for k in sorted(plan):
            for what, args in plan[k]:
                what(*args)
        for v in (*alls, few):
            v.end()
        keep.wait()


def backward(r_in, cls_t, es, xs, hs, ss, w_up, w_down, w_gate, w_proj, n_dev):
    n_tok, dim = r_in.shape
    n_l, _, ff = w_up.shape
    emb = w_gate.shape[2]
    n_c = COLD_AT + COLD_MAX
    n_f = 4
    tile = ff // n_f
    n_full = (n_l - 1) * n_f
    n_out = n_l * (COLD_AT - HOT_AT + RUN)

    def at_layer(t):
        t = jnp.minimum(t, n_full - 1)
        return n_l - 1 - t // n_f, t % n_f

    def cols(n):
        return pl.BlockSpec((None, n, tile), lambda t: (at_layer(t)[0], 0, at_layer(t)[1]))

    return pl.pallas_call(
        functools.partial(backward_kernel, n_l, n_f),
        grid=(n_full + 1,),
        in_specs=[ANY] * 6 + [spec((1, n_tok), pipeline_mode=ONCE), cols(n_tok), cols(dim),
                              pl.BlockSpec((None, tile, dim), lambda t: (*at_layer(t), 0))],
        out_specs=[ANY] * 2,
        out_shape=[out_of((n_l, n_c, emb)), out_of((n_dev, n_out, emb))],
        scratch_shapes=[pltpu.VMEM((n_tok, dim), F32), pltpu.VMEM((n_tok, dim), BF), pltpu.VMEM((n_tok, dim), F32), pltpu.VMEM((3, n_tok, emb), BF)]
        + [pltpu.VMEM(v, BF) for v in ((n_tok, emb), (emb, dim), (n_tok, emb), (dim, emb), (n_tok, dim))]
        + [pltpu.VMEM((n_l, n_c, emb), F32), pltpu.VMEM((n_l * RUN, emb), F32), pltpu.SemaphoreType.DMA((6,)),
           pltpu.SemaphoreType.DMA((n_l, *SPREAD_SEMS)), pltpu.SemaphoreType.DMA(SPREAD_SEMS), pltpu.SemaphoreType.DMA((n_l, *FOLD_SEMS))]
        + fold_bufs(emb) * n_l,
        compiler_params=params("arbitrary", collective_id=0, has_side_effects=True),
        cost_estimate=cost(n_l * n_tok * dim * (2 * ff + 2 * emb + 3 * n_c), n_l),
        name="backward",
    )(r_in, ss, w_proj, es, w_gate, xs, cls_t, hs, w_up, w_down)


def count_kernel(ids, out, zeros, blank, sem):
    n_tok = ids.shape[1]
    blank[...] = jnp.zeros(blank.shape, F32)
    blanks = [pltpu.make_async_copy(blank, zeros.at[pl.ds(i, len(blank))], sem) for i in range(0, len(zeros), len(blank))]
    for c in blanks:
        c.start()
    out[...] = jnp.zeros(out.shape, F32)

    def hits(v, n):
        same = v.astype(F32).astype(BF) == iota((n, n_tok), 0).astype(F32).astype(BF)
        return jnp.where(same, jnp.ones((), BF), jnp.zeros((), BF))

    @pl.loop(0, len(ids) // RUN)
    def _(i):
        got = []
        for j in range(RUN):
            ids_j = ids[pl.ds(i * RUN + j, 1), :]
            got.append(dot_nt(hits(ids_j >> HI_BITS, len(out)), hits(ids_j & (LO - 1), LO)))
        out[...] += sum(got)

    for c in blanks:
        c.wait()


def count_ids(ids, n_hi, shape):
    return pl.pallas_call(
        count_kernel, out_shape=[out_of((n_hi, LO)), out_of(shape)], out_specs=[pl.BlockSpec(memory_space=pltpu.VMEM), ANY],
        scratch_shapes=[pltpu.VMEM((shape[0] // 12, *shape[1:]), F32), pltpu.SemaphoreType.DMA(())],
        compiler_params=params(), name="count_ids")(ids)


def pack_kernel(row_of, table, out, sem):
    @pl.loop(0, len(out))
    def _(k):
        pltpu.make_async_copy(table.at[row_of[k]], out.at[k], sem).start()

    pltpu.make_async_copy(table.at[pl.ds(0, len(out))], out, sem).wait()


def pack_rows(row_of, table):
    shape = row_of.shape + table.shape[1:]
    return pl.pallas_call(
        pack_kernel,
        grid_spec=pltpu.PrefetchScalarGridSpec(num_scalar_prefetch=1, grid=(1,), in_specs=[ANY], out_specs=spec(shape),
                                               scratch_shapes=[pltpu.SemaphoreType.DMA(())]),
        out_shape=out_of(shape, table.dtype), compiler_params=params(), name="pack_rows",
    )(row_of, table)


class Place:
    def __init__(self):
        me = lax.axis_index('emb')
        self.core, self.x, self.y, self.z = me % 2, (me // 2) % 2, (me // 4) % 2, me // 8
        self.columns = [self.z, self.z + 1 - self.z % 2 * 2, (self.z + 2) % 4, 3 - self.z]
        self.others = [self.dev(z=z) for z in self.columns[1:]]
        self.to_x, self.to_y, self.to_core = self.dev(x=1 - self.x), self.dev(y=1 - self.y), self.dev(core=1 - self.core)

    def dev(self, z=None, y=None, x=None, core=None):
        z, y, x, core = [mine if v is None else v for v, mine in ((z, self.z), (y, self.y), (x, self.x), (core, self.core))]
        return ((z * 2 + y) * 2 + x) * 2 + core

    def meet(self):
        barrier = pltpu.get_barrier_semaphore()
        peers = self.others + [self.to_x, self.to_y, self.to_core]
        for peer in peers:
            pl.semaphore_signal(barrier, device_id=(peer,), device_id_type=pl.DeviceIdType.MESH)
        pl.semaphore_wait(barrier, len(peers))


def remote(src, dst, sems, to):
    send, recv = sems if isinstance(sems, tuple) else (sems.at[0], sems.at[1])
    return pltpu.make_async_remote_copy(src_ref=src, dst_ref=dst, send_sem=send, recv_sem=recv,
                                        device_id=(to,), device_id_type=pl.DeviceIdType.MESH)


Z, X, Y, FX, FY, C, CX, CY, CD, OWN = range(10)


class Spread:
    def __init__(self, at, mine, slot, sems):
        self.at, self.mine, self.slot, self.sems = at, mine, slot, sems
        n = mine.shape[0]
        half = n // 16 * 8
        self.halves = {FY: pl.ds(0, half), FX: pl.ds(half, n - half)}
        self.col = [at.dev(z=z) for z in at.columns]
        self.by_x = [at.dev(z=z, x=1 - at.x) for z in at.columns]
        self.by_y = [at.dev(z=z, y=1 - at.y) for z in at.columns]
        self.by_d = [at.dev(z=z, x=1 - at.x, y=1 - at.y) for z in at.columns]
        self.far = [[at.dev(z=z, x=x, y=y, core=1 - at.core) for z in at.columns]
                    for y, x in ((at.y, at.x), (at.y, 1 - at.x), (1 - at.y, at.x), (1 - at.y, 1 - at.x))]
        self.done = []

    def pair(self, kind, k):
        return self.sems.at[0, kind, k], self.sems.at[1, kind, k]

    def send(self, kind, k, src, dst, to):
        remote(src, dst, self.pair(kind, k), to).start()
        self.done.append((kind, k))

    def got(self, kind, k, block):
        remote(block, block, self.pair(kind, k), self.at.to_x).wait_recv()

    def begin(self):
        own = self.slot(self.col[0])
        pltpu.make_async_copy(self.mine, own, self.sems.at[0, OWN, 0]).start()
        for k, other in enumerate(self.at.others):
            self.send(Z, k + 1, self.mine, own, other)
        self.column(0)

    def column(self, k):
        block = self.slot(self.col[k])
        if k:
            self.got(Z, k, block)
        src = block if k else self.mine
        for kind, to in ((X, self.at.to_x), (Y, self.at.to_y), (C, self.at.to_core)):
            self.send(kind, k, src, block, to)

    def onward(self, k):
        for kind, part, to, other, core in ((X, self.by_x, self.at.to_y, FY, CX), (Y, self.by_y, self.at.to_x, FX, CY)):
            block = self.slot(part[k])
            self.got(kind, k, block)
            half = block.at[self.halves[other]]
            self.send(other, k, half, half, to)
            self.send(core, k, block, block, self.at.to_core)

    def across(self, k):
        block = self.slot(self.by_d[k])
        for kind, half in self.halves.items():
            self.got(kind, k, block.at[half])
        self.send(CD, k, block, block, self.at.to_core)

    def end(self):
        for k in STOPS:
            for kind, far in zip((C, CX, CY, CD), self.far):
                self.got(kind, k, self.slot(far[k]))
        own = self.slot(self.col[0])
        for kind, k in self.done:
            block = own.at[self.halves[kind]] if kind in self.halves else own
            remote(block, block, self.pair(kind, k), self.at.to_x).wait_send()
        pltpu.make_async_copy(self.mine, own, self.sems.at[0, OWN, 0]).wait()


class Fold:
    def __init__(self, at, part, bufs, sems):
        self.at, self.part, self.sems = at, part, sems
        self.ins, self.sums, self.all_z = bufs[:3], bufs[3:5], bufs[5]
        self.bits = at.core, at.x, at.y
        self.to = at.to_core, at.to_x, at.to_y

    def pair(self, i, k=0):
        return self.sems.at[0, i, k], self.sems.at[1, i, k]

    def cut(self, i, bit):
        n = self.ins[i].shape[0]
        return pl.ds(pl.multiple_of(bit * n, n), n)

    def source(self, i):
        return self.sums[i - 1] if i else self.part

    def hop(self, i):
        return remote(self.source(i).at[self.cut(i, 1 - self.bits[i])], self.ins[i], self.pair(i), self.to[i])

    def begin(self):
        self.hop(0).start()

    def step(self, i):
        self.hop(i).wait_recv()
        total = self.source(i)[self.cut(i, self.bits[i]), :] + self.ins[i][...]
        if i < 2:
            self.sums[i][...] = total
            self.hop(i + 1).start()
        else:
            self.all_z[self.at.z] = total
            for k, other in enumerate(self.at.others):
                self.along_z(k, other).start()

    def along_z(self, k, other):
        block = self.all_z.at[self.at.z]
        return remote(block, block, self.pair(3, k), other)

    def total(self):
        for k, other in enumerate(self.at.others):
            self.along_z(k, other).wait_recv()
        for i in range(3):
            self.hop(i).wait_send()
        for k, other in enumerate(self.at.others):
            self.along_z(k, other).wait_send()
        v = self.all_z
        return (v[0] + v[1]) + (v[2] + v[3])


def fold_bufs(emb):
    return [pltpu.VMEM((n, emb), F32) for n in (64, 32, 16, 64, 32)] + [pltpu.VMEM((4, 16, emb), F32)]


SPREAD_SEMS = (2, 10, 4)
STOPS = range(4)
FOLD_SEMS = (2, 4, 4)
HOT_AT, COLD_AT = FREQ, FREQ + 64


def class_sums(cls_t, three, sums):
    pick_t = (cls_t[...] == iota((sums.shape[0], cls_t.shape[1]), 0)).astype(BF)
    hi, mid, lo = [dot32(pick_t, three[i]) for i in range(3)]
    sums[...] = hi + (mid + lo)


ORDER = [(b & 3) * 8 + (b >> 2 & 1) * 4 + (b >> 3 & 1) * 2 + (b >> 4) for b in range(FREQ // RUN)]


def hot_kernel(any_freq, raw, freq, code, out, parts):
    n_dev, n_r, _ = raw.shape
    layer, block = pl.program_id(0), pl.program_id(1)
    n = RUN * n_dev
    for g in range(n_r // RUN):
        for o in range(n_dev):
            out[pl.ds(g * n + o * RUN, RUN), :] = raw[o, pl.ds(g * RUN, RUN), :]

    @pl.when(any_freq[block] > 0)
    def _():
        for j in range(freq.shape[1] // RUN):
            @pl.when(layer == j)
            def _(j=j):
                rows = jnp.concatenate([freq[o, j * RUN:(j + 1) * RUN, :] for o in ORDER])
                for i, part in enumerate(split3(rows)):
                    parts[i] = part
        sel = (code[...] == iota((n_r * n_dev, FREQ), 1)).astype(BF)
        out[...] += dot32(sel, parts[0]) + (dot32(sel, parts[1]) + dot32(sel, parts[2]))


def hot_out(gathered, code, n_l):
    n_dev, n_rows, emb = gathered.shape
    n_r = 4 * RUN
    width = n_r * n_dev
    blocks = len(code) // width
    return pl.pallas_call(
        hot_kernel,
        grid_spec=pltpu.PrefetchScalarGridSpec(
            num_scalar_prefetch=1, grid=(n_l, blocks),
            in_specs=[
                pl.BlockSpec((n_dev, n_r, emb), lambda i, b, _: (0, i * blocks + b, 0)),
                spec((n_dev, n_l * RUN, emb), 0, n_rows // (n_l * RUN) - 1, 0, pipeline_mode=ONCE),
                pl.BlockSpec((width, 1), lambda i, b, _: (b, 0)),
            ],
            out_specs=pl.BlockSpec((None, width, emb), lambda i, b, _: (n_l - 1 - i, b, 0)),
            scratch_shapes=[pltpu.VMEM((3, FREQ, emb), BF)]),
        out_shape=out_of((n_l, len(code), emb)),
        compiler_params=params("arbitrary", "arbitrary"),
        cost_estimate=cost(gathered.size * LO, n_l), name="hot_out",
    )((code.reshape(blocks, width) >= 0).any(axis=1).astype(I32), gathered, gathered, code.reshape(-1, 1))


def rows_kernel(numbers, row_of, sums, freq, into, out, stage, got, sem):
    n_used, cold_row, cold_no = [numbers[i] for i in range(3)]
    n_l = len(sums)

    def put(k, row):
        return pltpu.make_async_copy(stage.at[pl.ds(k, 1)], out.at[pl.ds(row, 1)], sem)

    def fill(k, src, at):
        for i in range(n_l):
            stage[k, pl.ds(n_l - 1 - i, 1), :] = src(i, at)

    @pl.loop(0, n_used)
    def _(k):
        fill(k, lambda i, at: sums[i, pl.ds(at, 1), :], COLD_AT + k)
        put(k, row_of[k]).start()

    @pl.when(cold_row >= 0)
    def _():
        c = pltpu.make_async_copy(freq.at[len(freq) - 1, pl.ds(n_l * (COLD_AT - HOT_AT), n_l * RUN)], got, sem)
        c.start()
        c.wait()
        fill(COLD_MAX, lambda i, at: got[pl.ds(i * RUN + at, 1), :], cold_no)
        put(COLD_MAX, cold_row).start()
        put(0, 0).wait()

    @pl.loop(0, n_used)
    def _(k):
        put(0, 0).wait()


def put_rows(numbers, row_of, sums, freq, into):
    n_l, _, emb = sums.shape
    return pl.pallas_call(
        rows_kernel,
        grid_spec=pltpu.PrefetchScalarGridSpec(
            num_scalar_prefetch=2, grid=(1,),
            in_specs=[spec(sums.shape), ANY, ANY], out_specs=ANY,
            scratch_shapes=[pltpu.VMEM((COLD_MAX + 1, n_l, emb), F32), pltpu.VMEM((n_l * RUN, emb), F32), pltpu.SemaphoreType.DMA(())]),
        out_shape=out_of(into.shape), input_output_aliases={4: 0},
        compiler_params=params("arbitrary"), name="put_rows",
    )(numbers, row_of, sums, freq, into)


def merge_kernel(keep, *refs):
    n = (len(refs) - 1) // 3
    sem = refs[-1]

    @pl.when(keep[0] == 0)
    def _():
        copies = [pltpu.make_async_copy(src, dst, sem.at[i]) for i, (src, dst) in enumerate(zip(refs[n:2 * n], refs[2 * n:]))]
        for c in copies:
            c.start()
        for c in copies:
            c.wait()


def merge(keep, fast, general):
    n = len(fast)
    return pl.pallas_call(
        merge_kernel,
        in_specs=[pl.BlockSpec(memory_space=pltpu.SMEM)] + [ANY] * 2 * n, out_specs=[ANY] * n,
        out_shape=[out_of(v.shape, v.dtype) for v in fast], scratch_shapes=[pltpu.SemaphoreType.DMA((n,))],
        input_output_aliases={i + 1: i for i in range(n)}, name="merge",
    )(keep, *fast, *general)


def empty_kernel(*_):
    pass


def empty(like):
    return pl.pallas_call(empty_kernel, out_specs=[ANY] * len(like), out_shape=[out_of(v.shape, v.dtype) for v in like], name="empty")()


def down_sum(v):
    return jnp.sum(v, axis=0)


def beside(*v):
    return jnp.concatenate(v, axis=1)


def row_sum(v):
    return jnp.sum(v, axis=1)


def square(n):
    return iota((n, n), 0), iota((n, n), 1)


def prefix(v):
    r, c = square(len(v))
    return row_sum(jnp.where(r > c, row(v), 0))


def digits(ids, n_hi):
    return one_hot(ids >> HI_BITS, n_hi), one_hot(ids & (LO - 1), LO)


def look(hi_lo, *maps):
    hi, lo = hi_lo
    got = dot32(hi, beside(*maps))
    return [row_sum(got[:, i * LO:(i + 1) * LO] * lo.astype(F32)).astype(I32) for i in range(len(maps))]


def number(count, most):
    levels = jnp.array(LEVELS, F32)
    n_over = jnp.sum((count[:, :, None] >= levels).astype(F32), axis=(0, 1))
    flag = count >= jnp.min(jnp.where(n_over <= most, levels, jnp.inf))
    r, c = square(LO)
    in_row = dot32(flag.astype(BF), (r < c).astype(BF))
    return jnp.where(flag, in_row + col(prefix(row_sum(flag.astype(F32)))) + 1, 0)


def solution(mesh):
    n_dev = mesh.shape['emb']

    def body(token_ids, hot_ids, x_in, d_out, emb_table, hot_table, w_up, w_down, w_gate, w_proj):
        n_loc = len(token_ids)
        layers, rows_dev, emb_dim = emb_table.shape
        n_hot = len(hot_ids)
        places, hot_dev = n_loc // n_dev, n_hot // n_dev
        n_hi = -(-rows_dev * n_dev // (8 * LO)) * 8
        me = lax.axis_index('emb')
        hot_at, cold_at = FREQ, FREQ + hot_dev

        def exchange(v):
            return swap(v.reshape(n_dev, places, -1)).reshape(n_loc, -1)

        def prepare(got_class, hot_hi, hot_lo, row_used, cold_owner, freq_cold, freq_map, hot_table, by_row, move, d_out):
            (hot_f,) = look((hot_hi, hot_lo), freq_map)
            used_rank = prefix(row_used.astype(I32))
            at_rank = (row(used_rank) == iota((COLD_MAX, rows_dev), 0)) & row(row_used)
            row_of = row_sum(jnp.where(at_rank, iota((COLD_MAX, rows_dev), 1), 0))
            packed = pack_rows(row_of, by_row)
            mine_no = jnp.where(hot_owner == me, FREQ_HOT + hot_place, -1)
            hot_pick = (one_hot(hot_f - 1, FREQ_HOT + hot_dev) * col((hot_f <= FREQ_HOT).astype(BF)) + one_hot(mine_no, FREQ_HOT + hot_dev)).T
            hot_rows = [dot32(hot_pick, hot_table[i]).astype(BF) for i in range(layers)]
            table = jnp.stack([jnp.concatenate([
                hot_rows[i][:FREQ_HOT], dot32(one_hot(cold_owner, n_dev), freq_cold[:, i]).astype(BF),
                hot_rows[i][FREQ_HOT:], packed[:, i]]) for i in range(layers)])
            n_used = jnp.minimum(jnp.sum(row_used.astype(I32)), COLD_MAX)
            row_no = got_class - cold_at
            used_before = row_sum(jnp.where(row(row_used) & (iota((n_loc, rows_dev), 1) < col(row_no)), 1, 0))
            cls = jnp.where(row_no >= 0, cold_at + used_before, got_class)
            code = jnp.where(hot_f <= FREQ_HOT, hot_f - 1, -1)
            d_placed = dot32(move, d_out).astype(BF)
            return d_placed, table, cls, n_used, row_of, code

        count, zeros = count_ids(swap(jnp.broadcast_to(row(token_ids), (n_dev, n_loc))), n_hi, (rows_dev, layers, emb_dim))
        tok, hot = digits(token_ids, n_hi), digits(hot_ids, n_hi)
        slot_no = jnp.arange(n_hot, dtype=I32)
        hot_place = slot_no // (RUN * n_dev) * RUN + slot_no % RUN
        hot_owner = slot_no // RUN % n_dev
        q_map = dot32(hot[0].T, hot[1] * col((hot_place + 1).astype(BF))).astype(BF)
        r_map = dot32(hot[0].T, hot[1] * col(hot_owner.astype(BF))).astype(BF)
        hot_no = number(jnp.where(q_map > 0, count, 0), FREQ_HOT)
        cold_no = number(jnp.where(q_map > 0, 0, count), FREQ_COLD)
        freq_map = jnp.where(hot_no > 0, hot_no, jnp.where(cold_no > 0, FREQ_HOT + cold_no, 0)).astype(BF)
        id_map = iota((n_hi, LO), 0) * LO + iota((n_hi, LO), 1) + 1
        cold_id = jnp.sum(jnp.where(cold_no.astype(I32)[None] == iota((FREQ_COLD, 1, 1), 0) + 1, id_map[None], 0), axis=(1, 2)) - 1
        cold_owner = jnp.where(cold_id >= 0, cold_id // rows_dev, -1)
        my_cold = (cold_owner == me).astype(I32)
        my_row = jnp.minimum(jnp.sum(my_cold * (cold_id - me * rows_dev + 1)) - 1, rows_dev - 1)
        by_row = emb_table.transpose(1, 0, 2)
        cold_row = lax.dynamic_slice_in_dim(by_row, jnp.maximum(my_row, 0), 1)
        freq_cold = swap(jnp.broadcast_to(cold_row, (n_dev, layers, emb_dim)))

        tok_f, tok_q, tok_r = look(tok, freq_map, q_map, r_map)
        rare = tok_f == 0
        owner = jnp.where(tok_q > 0, tok_r, token_ids // rows_dev)
        dev_no = iota((n_loc, n_dev), 1)
        to_dev = (col(owner) == dev_no) & col(rare)
        marks = beside(to_dev.astype(BF), col(jnp.logical_not(rare).astype(BF)))
        r, c = square(n_loc)
        ranks = dot32((r > c).astype(BF), marks)
        sent = down_sum(to_dev.astype(F32))
        free = jnp.maximum(places - sent, 0)
        free_at = prefix(free)
        fill = ranks[:, n_dev:]
        fill_dev = (fill >= free_at) & (fill < free_at + free)
        to_dev = jnp.where(col(rare), to_dev, fill_dev)
        place = jnp.where(col(rare), ranks[:, :n_dev], fill + (sent - free_at))
        slot = row_sum(jnp.where(to_dev, dev_no * places + place.astype(I32), 0))
        row_ids = me * rows_dev + jnp.arange(rows_dev, dtype=I32)
        row_f, row_q, row_n = look(digits(row_ids, n_hi), freq_map, q_map, (count > 0).astype(BF))
        row_used = (row_n > 0) & (row_f == 0) & (row_q == 0)
        fits = ((jnp.max(sent) <= places) & (jnp.sum(row_used.astype(I32)) <= COLD_MAX) & (jnp.sum(my_cold) <= 1))
        tok_class = jnp.where(rare, jnp.where(tok_q > 0, hot_at + tok_q - 1, cold_at + token_ids % rows_dev), tok_f - 1)
        bad = 1 << 20
        move = r == row(slot)
        send_class, freq_cold = lax.optimization_barrier(
            (row_sum(jnp.where(move, row(tok_class), 0)) + jnp.where(fits, 0, bad), freq_cold))
        got_class = swap(send_class.reshape(n_dev, places)).reshape(n_loc)
        move = move.astype(BF)
        placed, got_class, hot_hi, hot_lo, row_used, cold_owner = lax.optimization_barrier(
            (dot32(move, x_in).astype(BF), got_class, *hot, row_used, cold_owner))
        x_moved = exchange(placed)
        given = prepare(got_class, hot_hi, hot_lo, row_used, cold_owner, freq_cold, freq_map, hot_table, by_row, move, d_out)
        all_fit = jnp.max(got_class) < bad

        d_placed, table, cls, n_used, row_of, code = given
        cls_row = cls.reshape(1, n_loc)
        xs, hs, ss, es, x_last, d_moved = forward(x_moved, cls.reshape(n_loc, 1), table, w_up, w_down, w_gate, w_proj, d_placed, n_dev)
        sums, gathered = backward(d_moved, cls_row, es, xs, hs, ss, w_up, w_down, w_gate, w_proj, n_dev)
        x_last, gathered = lax.optimization_barrier((x_last, gathered))
        x_back = exchange(x_last)
        numbers = jnp.stack([n_used, my_row, jnp.minimum(jnp.sum(my_cold * jnp.arange(FREQ_COLD, dtype=I32)), FREQ_COLD - 1)])
        d_table = put_rows(numbers, row_of, sums, gathered, zeros)
        d_hot = hot_out(gathered, code, layers)
        x_out = dot32((col(slot) == iota((n_loc, n_loc), 1)).astype(BF), x_back).astype(BF)
        *fast, fit = lax.optimization_barrier((x_out, d_table, d_hot, all_fit))

        def slow():
            x, table_grad, hot_grad = general_path(n_dev, me, token_ids, hot_ids, x_in, d_out, emb_table, hot_table, w_up, w_down, w_gate, w_proj)
            return x, table_grad.transpose(1, 0, 2), hot_grad

        general = lax.cond(fit, lambda: tuple(empty(fast)), slow)
        x_out, d_table, d_hot = merge(fit.astype(I32).reshape(1), fast, general)
        return x_out, d_table.transpose(1, 0, 2), d_hot

    return jax.shard_map(body, mesh=mesh,
                         in_specs=(P('emb'), P(), P('emb', None), P('emb', None), P(None, 'emb', None), P(), P(), P(), P(), P()),
                         out_specs=(P('emb', None), P(None, 'emb', None), P()),
                         check_vma=False)
```

```python
import functools

import jax
import jax.numpy as jnp
from jax import lax
from jax.experimental import pallas as pl
from jax.experimental.pallas import tpu as pltpu
from jax.sharding import PartitionSpec as P


NORM_EPS = 1e-6
FREQ_HOT = 124
FREQ_COLD = 4
FREQ = FREQ_HOT + FREQ_COLD
COLD_MAX = 256
LO = 256
HI_BITS = 8
RUN = 4
LEVELS = tuple(12 * 2 ** (i / 6) for i in range(27))
GELU_A = 0.7978845608028654
GELU_B = GELU_A * 0.044715
VMEM = 66_000_000
ROWS_A = 256
ROWS_B = 512
TILE = 1024
BF = jnp.bfloat16
F32 = jnp.float32
I32 = jnp.int32
ONCE = pl.Buffered(1)


def gelu_back(pre_act, cot_in):
    _, pull = jax.vjp(jax.nn.gelu, pre_act.astype(F32))
    return pull(cot_in)[0]


def swap(v):
    return lax.all_to_all(v, 'emb', 0, 0, tiled=True)


def col(v):
    return v[:, None]


def row(v):
    return v[None, :]


def dot32(a, b):
    return jnp.dot(a, b, preferred_element_type=F32)


def dense_parts(resid, w_up, w_gate):
    resid_f = resid.astype(F32)
    inv_rms = lax.rsqrt(jnp.mean(resid_f * resid_f, axis=-1, keepdims=True) + NORM_EPS)
    normed = (resid_f * inv_rms).astype(BF)
    hidden = dot32(normed, w_up).astype(BF)
    gate_pre = dot32(normed, w_gate).astype(BF)
    return resid_f, inv_rms, hidden, gate_pre


def layer_forward(resid, emb_rows, w_up, w_down, w_gate, w_proj):
    resid_f, _, hidden, gate_pre = dense_parts(resid, w_up, w_gate)
    activated = jax.nn.gelu(hidden.astype(F32)).astype(BF)
    mlp_out = dot32(activated, w_down).astype(BF)
    gate = jax.nn.gelu(gate_pre.astype(F32)).astype(BF)
    mixed = (gate.astype(F32) * emb_rows.astype(F32)).astype(BF)
    projected = dot32(mixed, w_proj).astype(BF)
    return (resid_f + mlp_out.astype(F32) + projected.astype(F32)).astype(BF)


def layer_backward(resid, emb_rows, d_next, w_up, w_down, w_gate, w_proj):
    resid_f, inv_rms, hidden, gate_pre = dense_parts(resid, w_up, w_gate)
    gate = jax.nn.gelu(gate_pre.astype(F32)).astype(BF)
    d_cast = d_next.astype(BF)
    d_mixed = jnp.einsum('nd,ed->ne', d_cast, w_proj, preferred_element_type=F32)
    d_rows = gate.astype(F32) * d_mixed
    d_gpre = gelu_back(gate_pre, d_mixed * emb_rows.astype(F32))
    d_hidden = gelu_back(hidden, jnp.einsum('nd,fd->nf', d_cast, w_down, preferred_element_type=F32))
    d_normed = (jnp.einsum('nf,df->nd', d_hidden.astype(BF), w_up, preferred_element_type=F32)
                + jnp.einsum('ne,de->nd', d_gpre.astype(BF), w_gate, preferred_element_type=F32))
    inner = jnp.mean(d_normed * resid_f, axis=-1, keepdims=True)
    d_prev = d_next + inv_rms * d_normed - resid_f * (inv_rms * inv_rms * inv_rms) * inner
    return d_prev, d_rows


def general_path(n_dev, my_index, token_ids, hot_ids, x_in, d_out, emb_table, hot_table, w_up, w_down, w_gate, w_proj):
    n_loc = token_ids.shape[0]
    _, rows_dev, emb_dim = emb_table.shape
    capacity = max(8, (2 * n_loc) // n_dev)
    n_slots = n_dev * capacity
    hot_match = col(token_ids) == row(hot_ids)
    is_hot = hot_match.any(1)
    hot_pick = hot_match.astype(BF)
    hot_pick_f = hot_match.astype(F32)
    owner_id = token_ids // rows_dev
    to_owner = (col(owner_id) == row(jnp.arange(n_dev, dtype=I32))) & col(jnp.logical_not(is_hot))
    owner_rank = jnp.cumsum(to_owner.astype(jnp.int32), axis=0) - 1
    place = row_sum(jnp.where(to_owner, owner_rank, 0))
    slot = jnp.where(is_hot, n_slots, owner_id * capacity + place)
    none = jnp.full((n_slots,), -1, I32)
    send_ids = none.at[slot].set(token_ids, mode='drop')
    slot_tok = none.at[slot].set(jnp.arange(n_loc, dtype=jnp.int32), mode='drop')
    recv_ids = swap(send_ids.reshape(n_dev, capacity)).reshape(n_slots)
    served_ok = recv_ids >= 0
    local_row = jnp.where(served_ok, recv_ids - my_index * rows_dev, 0)
    pick_slot = jnp.minimum(slot, n_slots - 1)
    slot_used = slot_tok >= 0
    slot_src = jnp.maximum(slot_tok, 0)

    def fwd(resid, per_layer):
        table, hot_l, up, down, gate_w, proj = per_layer
        served = table[local_row]
        fetched = swap(served.reshape(n_dev, capacity, emb_dim)).reshape(n_slots, emb_dim)
        cold_rows = fetched[pick_slot]
        hot_rows = dot32(hot_pick, hot_l).astype(BF)
        emb_rows = jnp.where(col(is_hot), hot_rows, cold_rows)
        return layer_forward(resid, emb_rows, up, down, gate_w, proj), (resid, emb_rows)

    x_first = jnp.where(n_loc * hot_ids[0] >= 0, x_in, 0)
    x_out, (x_saved, rows_saved) = lax.scan(fwd, x_first, (emb_table, hot_table, w_up, w_down, w_gate, w_proj))

    def bwd(d_resid, per_layer):
        resid_l, rows_l, up, down, gate_w, proj = per_layer
        d_resid, d_rows = layer_backward(resid_l, rows_l, d_resid, up, down, gate_w, proj)
        outgoing = jnp.where(col(slot_used), d_rows[slot_src], 0.0)
        incoming = swap(outgoing.reshape(n_dev, capacity, emb_dim)).reshape(n_slots, emb_dim)
        d_tab = jax.ops.segment_sum(jnp.where(col(served_ok), incoming, 0.0), local_row, num_segments=rows_dev)
        hot_local = jnp.einsum('nh,ne->he', hot_pick_f, d_rows, precision=lax.Precision.HIGHEST, preferred_element_type=F32)
        return d_resid, (d_tab, lax.psum(hot_local, 'emb'))

    _, (d_table, d_hot) = lax.scan(bwd, d_out.astype(F32), (x_saved, rows_saved, w_up, w_down, w_gate, w_proj), reverse=True)
    return x_out, d_table, d_hot


def split3(v):
    hi = v.astype(BF)
    rest = v - hi.astype(F32)
    mid = rest.astype(BF)
    return hi, mid, (rest - mid.astype(F32)).astype(BF)


def iota(shape, dim):
    return lax.broadcasted_iota(jnp.int32, shape, dim)


def one_hot(v, n, dtype=BF):
    return (col(v) == iota((len(v), n), 1)).astype(dtype)


def dot_nt(a, b):
    return lax.dot_general(a, b, (((1,), (1,)), ((), ())), preferred_element_type=F32)


def gelu(x):
    half = 0.5 * x
    return half + half * jnp.tanh(x * (GELU_A + GELU_B * (x * x)))


def gelu_slope(x):
    sq = x * x
    th = jnp.tanh(x * (GELU_A + GELU_B * sq))
    return (0.5 + 0.5 * th) + (0.5 * x) * (1.0 - th * th) * (GELU_A + (3.0 * GELU_B) * sq)


def forward_kernel(n_l, n_f, n_dev, x0, cls, table, wu, wd, wg, wp, d_in, xs, hs, ss, es, xo, d_got, x_now, u_now, acc, q_now, sems):
    layer, step = pl.program_id(0), pl.program_id(1)
    n_tok = x_now.shape[0]
    me = lax.axis_index('emb')
    places = n_tok // n_dev
    barrier = pltpu.get_barrier_semaphore()

    def block(dev):
        return pl.ds(pl.multiple_of(dev * places, places), places)

    own = pltpu.make_async_copy(d_in.at[block(me)], d_got.at[block(me)], sems.at[2])

    @pl.when((layer == 0) & (step == 0))
    def _():
        @pl.loop(1, n_dev)
        def _(k):
            pl.semaphore_signal(barrier, device_id=((me + k) % n_dev,), device_id_type=pl.DeviceIdType.MESH)

    @pl.when((layer == 0) & (step == 1))
    def _():
        own.start()
        pl.semaphore_wait(barrier, n_dev - 1)

        @pl.loop(1, n_dev)
        def _(k):
            to = (me + k) % n_dev
            remote(d_in.at[block(to)], d_got.at[block(me)], sems, to).start()

    @pl.when((layer == n_l - 1) & (step == n_f - 1))
    def _():
        others = pl.ds(0, n_tok - places)
        remote(d_in.at[others], d_got.at[others], sems, me).wait()
        own.wait()

    @pl.when((layer == 0) & (step == 0))
    def _():
        x_now[...] = x0[...]

    @pl.when(step == 0)
    def _():
        for m in chunks(n_tok, ROWS_A):
            xb = x_now[m, :]
            x = xb.astype(F32)
            xs[m, :] = xb
            u = (x * lax.rsqrt(jnp.mean(x * x, axis=-1, keepdims=True) + NORM_EPS)).astype(BF)
            u_now[m, :] = u
            s = dot32(u, wg[...]).astype(BF)
            ss[m, :] = s
            g = gelu(s.astype(F32)).astype(BF)
            pick = (cls[m, :] == iota((m.size, table.shape[0]), 1)).astype(BF)
            e = dot32(pick, table[...]).astype(BF)
            es[m, :] = e
            mixed = (g.astype(F32) * e.astype(F32)).astype(BF)
            q_now[m, :] = dot32(mixed, wp[...]).astype(BF)
            acc[m, :] = jnp.zeros((m.size, acc.shape[1]), F32)

    for m in chunks(n_tok, ROWS_B):
        h = dot32(u_now[m, :], wu[...]).astype(BF)
        hs[m, :] = h
        acc[m, :] += dot32(gelu(h.astype(F32)).astype(BF), wd[...])

    @pl.when(step == n_f - 1)
    def _():
        for m in chunks(n_tok, ROWS_A):
            x = x_now[m, :].astype(F32) + acc[m, :].astype(BF).astype(F32) + q_now[m, :].astype(F32)
            x_now[m, :] = x.astype(BF)

    @pl.when((step == n_f - 1) & (layer == n_l - 1))
    def _():
        xo[...] = x_now[...]


def chunks(n, size):
    size = min(n, size)
    return [pl.ds(m, size) for m in range(0, n, size)]


def forward(x0, cls, table, w_up, w_down, w_gate, w_proj, d_in, n_dev):
    n_tok, dim = x0.shape
    n_l, _, ff = w_up.shape
    emb = w_gate.shape[2]
    tile = min(TILE, ff)
    n_f = ff // tile
    n_c = table.shape[1]

    def whole(l, f):
        return (l, 0, 0)

    def cols(l, f):
        return (l, 0, f)

    def fixed(l, f):
        return (0, 0)

    return pl.pallas_call(
        functools.partial(forward_kernel, n_l, n_f, n_dev),
        grid=(n_l, n_f),
        in_specs=[
            pl.BlockSpec((n_tok, dim), fixed, pipeline_mode=ONCE),
            pl.BlockSpec((n_tok, 1), fixed, pipeline_mode=ONCE),
            pl.BlockSpec((None, n_c, emb), whole),
            pl.BlockSpec((None, dim, tile), cols),
            pl.BlockSpec((None, tile, dim), lambda l, f: (l, f, 0)),
            pl.BlockSpec((None, dim, emb), whole),
            pl.BlockSpec((None, emb, dim), whole),
            ANY,
        ],
        out_specs=[
            pl.BlockSpec((None, n_tok, dim), whole),
            pl.BlockSpec((None, n_tok, tile), cols),
            pl.BlockSpec((None, n_tok, emb), whole),
            pl.BlockSpec((None, n_tok, emb), whole),
            pl.BlockSpec((n_tok, dim), fixed),
            ANY,
        ],
        out_shape=[out_of((n_l, n_tok, n), BF) for n in (dim, ff, emb, emb)] + [out_of((n_tok, dim), BF)] * 2,
        scratch_shapes=[pltpu.VMEM((n_tok, dim), t) for t in (BF, BF, F32, BF)] + [pltpu.SemaphoreType.DMA((3,))],
        compiler_params=params("arbitrary", "arbitrary", collective_id=1, has_side_effects=True),
        cost_estimate=cost(n_l * n_tok * dim * (2 * ff + 2 * emb + n_c), n_l),
        name="forward",
    )(x0, cls, table, w_up, w_down, w_gate, w_proj, d_in)


def params(*kinds, **more):
    return pltpu.CompilerParams(vmem_limit_bytes=VMEM, dimension_semantics=kinds or None, **more)


def cost(products, layers):
    return pl.CostEstimate(flops=2 * products, bytes_accessed=layers * 40_000_000, transcendentals=0)


def spec(shape, *index, **more):
    index = index or (0,) * len(shape)
    return pl.BlockSpec(shape, lambda *_: index, **more)


ANY = pl.BlockSpec(memory_space=pl.ANY)


def out_of(shape, dtype=F32):
    return jax.ShapeDtypeStruct(shape, dtype)


def backward_kernel(n_l, n_f, r_in, ss, wp, es, wg, xs, cls_t, hs, wu, wd, sums_out, out,
                    r, c_now, acc, three, s_now, p_now, e_now, g_now, x_now, sums, totals, loads, sems, sems_few, sems_f, *bufs):
    step = pl.program_id(0)
    f, n_full = step % n_f, (n_l - 1) * n_f
    n_tok = len(c_now)
    parts = chunks(n_tok, ROWS_B)
    n_hot, n_tot = COLD_AT - HOT_AT, n_l * RUN
    at = Place()
    folds = [Fold(at, sums.at[i, pl.ds(0, FREQ)], bufs[i * len(bufs) // n_l:(i + 1) * len(bufs) // n_l], sems_f.at[i]) for i in range(n_l)]
    alls = [Spread(at, sums.at[i, pl.ds(HOT_AT, n_hot)], lambda d, i=i: out.at[d, pl.ds(n_hot * i, n_hot)], sems.at[i]) for i in range(n_l)]
    few = Spread(at, totals, lambda d: out.at[d, pl.ds(n_hot * n_l, n_tot)], sems_few)

    def total(i):
        t = folds[i].total()
        for z in STOPS:
            @pl.when(at.z == z)
            def _(z=z):
                totals[pl.ds(i * RUN, RUN), :] = t[z * RUN:(z + 1) * RUN, :]

    def load(layer, which):
        srcs = (wp, p_now), (ss, s_now), (es, e_now), (wg, g_now), (xs, x_now)
        return [pltpu.make_async_copy(srcs[i][0].at[layer], srcs[i][1], loads.at[i]) for i in which]

    early, late = range(4), range(4, 5)
    layer = n_l - 1 - step // n_f
    first = pltpu.make_async_copy(r_in, c_now, loads.at[5])

    plan = {}
    for i in range(n_l):
        steps = [(1, folds[i].begin, ()), (2, folds[i].step, (0,)), (2, alls[i].begin, ()), (5, folds[i].step, (1,)), (8, alls[i].onward, (0,)),
                 (9, alls[i].column, (1,)), (10, folds[i].step, (2,)), (10, alls[i].column, (2,)), (13, alls[i].onward, (1,)),
                 (13, alls[i].across, (0,)), (14, alls[i].column, (3,)), (18, total, (i,)), (19, alls[i].onward, (2,)), (21, alls[i].onward, (3,)),
                 (21, alls[i].across, (1,)), (23, alls[i].across, (2,)), (26, alls[i].across, (3,))]
        for when, what, args in steps:
            plan.setdefault(10 * i + when, []).append((what, args))
    few_steps = [few.begin], *[[few.column, few.onward]] * 3, [few.onward], [few.across] * 4
    for k, steps in enumerate(few_steps):
        for j, what in enumerate(steps):
            args = () if not k else (k - j,) if k < 4 else (3,) if k == 4 else (j,)
            plan.setdefault(10 * n_l + 8 + k / 2, []).append((what, args))

    def point(k, now, layers):
        for i in range(layers):
            if 10 * i + k in plan:
                @pl.when(step == i * n_f + now)
                def _(i=i):
                    for what, args in plan.pop(10 * i + k):
                        what(*args)

    @pl.when(step == 0)
    def _():
        first.start()
        for c in load(layer, early):
            c.start()
        at.meet()
        first.wait()
        r[...] = c_now[...].astype(F32)

    @pl.when(f == 0)
    def _():
        for c in load(layer, early[:3]):
            c.wait()
        for c in load(layer, late):
            c.start()
        for m in parts:
            c = r[m, :].astype(BF)
            c_now[m, :] = c
            a = dot_nt(c, p_now[...])
            s = s_now[m, :].astype(F32)
            rows = gelu(s).astype(BF).astype(F32) * a
            for j, part in enumerate(split3(rows)):
                three[j, m, :] = part
            e_now[m, :] = (gelu_slope(s) * (a * e_now[m, :].astype(F32))).astype(BF)
        point(0, 0, n_l)
        class_sums(cls_t, three, sums.at[step // n_f])
        point(1, 0, n_l)

    @pl.when(f == 0)
    def _():
        for c in load(layer, early[3:]):
            c.wait()

    @pl.when((f == 0) & (step < n_full))
    def _():
        for m in parts:
            acc[m, :] = dot_nt(e_now[m, :], g_now[...])

    @pl.when((f == 1) & (step < n_full))
    def _():
        for c in load(layer - 1, early):
            c.start()

    @pl.when(step < n_full)
    def _():
        for i, m in enumerate(parts):
            d_act = dot_nt(c_now[m, :], wd[...])
            dh = (gelu_slope(hs[m, :].astype(F32)) * d_act).astype(BF)
            acc[m, :] += dot_nt(dh, wu[...])
            for k in range(n_f):
                point(2 + 2 * k + i, k, n_l - 1)

    @pl.when((f == n_f - 1) & (step < n_full))
    def _():
        for c in load(layer, late):
            c.wait()
        for m in chunks(n_tok, ROWS_A):
            x = x_now[m, :].astype(F32)
            k = lax.rsqrt(jnp.mean(x * x, axis=-1, keepdims=True) + NORM_EPS)
            du = acc[m, :]
            inner = jnp.mean(du * x, axis=-1, keepdims=True)
            r[m, :] = r[m, :] + k * du - x * (k * k * k) * inner

    @pl.when(step == n_full)
    def _():
        for c in load(layer, late):
            c.wait()
        keep = pltpu.make_async_copy(sums, sums_out, loads.at[5])
        keep.start()
        for k in sorted(plan):
            for what, args in plan[k]:
                what(*args)
        for v in (*alls, few):
            v.end()
        keep.wait()


def backward(r_in, cls_t, es, xs, hs, ss, w_up, w_down, w_gate, w_proj, n_dev):
    n_tok, dim = r_in.shape
    n_l, _, ff = w_up.shape
    emb = w_gate.shape[2]
    n_c = COLD_AT + COLD_MAX
    n_f = 4
    tile = ff // n_f
    n_full = (n_l - 1) * n_f
    n_out = n_l * (COLD_AT - HOT_AT + RUN)

    def at_layer(t):
        t = jnp.minimum(t, n_full - 1)
        return n_l - 1 - t // n_f, t % n_f

    def cols(n):
        return pl.BlockSpec((None, n, tile), lambda t: (at_layer(t)[0], 0, at_layer(t)[1]))

    return pl.pallas_call(
        functools.partial(backward_kernel, n_l, n_f),
        grid=(n_full + 1,),
        in_specs=[ANY] * 6 + [spec((1, n_tok), pipeline_mode=ONCE), cols(n_tok), cols(dim),
                              pl.BlockSpec((None, tile, dim), lambda t: (*at_layer(t), 0))],
        out_specs=[ANY] * 2,
        out_shape=[out_of((n_l, n_c, emb)), out_of((n_dev, n_out, emb))],
        scratch_shapes=[pltpu.VMEM((n_tok, dim), F32), pltpu.VMEM((n_tok, dim), BF), pltpu.VMEM((n_tok, dim), F32), pltpu.VMEM((3, n_tok, emb), BF)]
        + [pltpu.VMEM(v, BF) for v in ((n_tok, emb), (emb, dim), (n_tok, emb), (dim, emb), (n_tok, dim))]
        + [pltpu.VMEM((n_l, n_c, emb), F32), pltpu.VMEM((n_l * RUN, emb), F32), pltpu.SemaphoreType.DMA((6,)),
           pltpu.SemaphoreType.DMA((n_l, *SPREAD_SEMS)), pltpu.SemaphoreType.DMA(SPREAD_SEMS), pltpu.SemaphoreType.DMA((n_l, *FOLD_SEMS))]
        + fold_bufs(emb) * n_l,
        compiler_params=params("arbitrary", collective_id=0, has_side_effects=True),
        cost_estimate=cost(n_l * n_tok * dim * (2 * ff + 2 * emb + 3 * n_c), n_l),
        name="backward",
    )(r_in, ss, w_proj, es, w_gate, xs, cls_t, hs, w_up, w_down)


def count_kernel(ids, out, zeros, blank, sem):
    n_tok = ids.shape[1]
    blank[...] = jnp.zeros(blank.shape, F32)
    blanks = [pltpu.make_async_copy(blank, zeros.at[pl.ds(i, len(blank))], sem) for i in range(0, len(zeros), len(blank))]
    for c in blanks:
        c.start()
    out[...] = jnp.zeros(out.shape, F32)

    def hits(v, n):
        same = v.astype(F32).astype(BF) == iota((n, n_tok), 0).astype(F32).astype(BF)
        return jnp.where(same, jnp.ones((), BF), jnp.zeros((), BF))

    @pl.loop(0, len(ids) // RUN)
    def _(i):
        got = []
        for j in range(RUN):
            ids_j = ids[pl.ds(i * RUN + j, 1), :]
            got.append(dot_nt(hits(ids_j >> HI_BITS, len(out)), hits(ids_j & (LO - 1), LO)))
        out[...] += sum(got)

    for c in blanks:
        c.wait()


def count_ids(ids, n_hi, shape):
    return pl.pallas_call(
        count_kernel, out_shape=[out_of((n_hi, LO)), out_of(shape)], out_specs=[pl.BlockSpec(memory_space=pltpu.VMEM), ANY],
        scratch_shapes=[pltpu.VMEM((shape[0] // 12, *shape[1:]), F32), pltpu.SemaphoreType.DMA(())],
        compiler_params=params(), name="count_ids")(ids)


def pack_kernel(row_of, table, out, sem):
    @pl.loop(0, len(out))
    def _(k):
        pltpu.make_async_copy(table.at[row_of[k]], out.at[k], sem).start()

    pltpu.make_async_copy(table.at[pl.ds(0, len(out))], out, sem).wait()


def pack_rows(row_of, table):
    shape = row_of.shape + table.shape[1:]
    return pl.pallas_call(
        pack_kernel,
        grid_spec=pltpu.PrefetchScalarGridSpec(num_scalar_prefetch=1, grid=(1,), in_specs=[ANY], out_specs=spec(shape),
                                               scratch_shapes=[pltpu.SemaphoreType.DMA(())]),
        out_shape=out_of(shape, table.dtype), compiler_params=params(), name="pack_rows",
    )(row_of, table)


class Place:
    def __init__(self):
        me = lax.axis_index('emb')
        self.core, self.x, self.y, self.z = me % 2, (me // 2) % 2, (me // 4) % 2, me // 8
        self.columns = [self.z, self.z + 1 - self.z % 2 * 2, (self.z + 2) % 4, 3 - self.z]
        self.others = [self.dev(z=z) for z in self.columns[1:]]
        self.to_x, self.to_y, self.to_core = self.dev(x=1 - self.x), self.dev(y=1 - self.y), self.dev(core=1 - self.core)

    def dev(self, z=None, y=None, x=None, core=None):
        z, y, x, core = [mine if v is None else v for v, mine in ((z, self.z), (y, self.y), (x, self.x), (core, self.core))]
        return ((z * 2 + y) * 2 + x) * 2 + core

    def meet(self):
        barrier = pltpu.get_barrier_semaphore()
        peers = self.others + [self.to_x, self.to_y, self.to_core]
        for peer in peers:
            pl.semaphore_signal(barrier, device_id=(peer,), device_id_type=pl.DeviceIdType.MESH)
        pl.semaphore_wait(barrier, len(peers))


def remote(src, dst, sems, to):
    send, recv = sems if isinstance(sems, tuple) else (sems.at[0], sems.at[1])
    return pltpu.make_async_remote_copy(src_ref=src, dst_ref=dst, send_sem=send, recv_sem=recv,
                                        device_id=(to,), device_id_type=pl.DeviceIdType.MESH)


Z, X, Y, FX, FY, C, CX, CY, CD, OWN = range(10)


class Spread:
    def __init__(self, at, mine, slot, sems):
        self.at, self.mine, self.slot, self.sems = at, mine, slot, sems
        n = mine.shape[0]
        half = n // 16 * 8
        self.halves = {FY: pl.ds(0, half), FX: pl.ds(half, n - half)}
        self.col = [at.dev(z=z) for z in at.columns]
        self.by_x = [at.dev(z=z, x=1 - at.x) for z in at.columns]
        self.by_y = [at.dev(z=z, y=1 - at.y) for z in at.columns]
        self.by_d = [at.dev(z=z, x=1 - at.x, y=1 - at.y) for z in at.columns]
        self.far = [[at.dev(z=z, x=x, y=y, core=1 - at.core) for z in at.columns]
                    for y, x in ((at.y, at.x), (at.y, 1 - at.x), (1 - at.y, at.x), (1 - at.y, 1 - at.x))]
        self.done = []

    def pair(self, kind, k):
        return self.sems.at[0, kind, k], self.sems.at[1, kind, k]

    def send(self, kind, k, src, dst, to):
        remote(src, dst, self.pair(kind, k), to).start()
        self.done.append((kind, k))

    def got(self, kind, k, block):
        remote(block, block, self.pair(kind, k), self.at.to_x).wait_recv()

    def begin(self):
        own = self.slot(self.col[0])
        pltpu.make_async_copy(self.mine, own, self.sems.at[0, OWN, 0]).start()
        for k, other in enumerate(self.at.others):
            self.send(Z, k + 1, self.mine, own, other)
        self.column(0)

    def column(self, k):
        block = self.slot(self.col[k])
        if k:
            self.got(Z, k, block)
        src = block if k else self.mine
        for kind, to in ((X, self.at.to_x), (Y, self.at.to_y), (C, self.at.to_core)):
            self.send(kind, k, src, block, to)

    def onward(self, k):
        for kind, part, to, other, core in ((X, self.by_x, self.at.to_y, FY, CX), (Y, self.by_y, self.at.to_x, FX, CY)):
            block = self.slot(part[k])
            self.got(kind, k, block)
            half = block.at[self.halves[other]]
            self.send(other, k, half, half, to)
            self.send(core, k, block, block, self.at.to_core)

    def across(self, k):
        block = self.slot(self.by_d[k])
        for kind, half in self.halves.items():
            self.got(kind, k, block.at[half])
        self.send(CD, k, block, block, self.at.to_core)

    def end(self):
        for k in STOPS:
            for kind, far in zip((C, CX, CY, CD), self.far):
                self.got(kind, k, self.slot(far[k]))
        own = self.slot(self.col[0])
        for kind, k in self.done:
            block = own.at[self.halves[kind]] if kind in self.halves else own
            remote(block, block, self.pair(kind, k), self.at.to_x).wait_send()
        pltpu.make_async_copy(self.mine, own, self.sems.at[0, OWN, 0]).wait()


class Fold:
    def __init__(self, at, part, bufs, sems):
        self.at, self.part, self.sems = at, part, sems
        self.ins, self.sums, self.all_z = bufs[:3], bufs[3:5], bufs[5]
        self.bits = at.core, at.x, at.y
        self.to = at.to_core, at.to_x, at.to_y

    def pair(self, i, k=0):
        return self.sems.at[0, i, k], self.sems.at[1, i, k]

    def cut(self, i, bit):
        n = self.ins[i].shape[0]
        return pl.ds(pl.multiple_of(bit * n, n), n)

    def source(self, i):
        return self.sums[i - 1] if i else self.part

    def hop(self, i):
        return remote(self.source(i).at[self.cut(i, 1 - self.bits[i])], self.ins[i], self.pair(i), self.to[i])

    def begin(self):
        self.hop(0).start()

    def step(self, i):
        self.hop(i).wait_recv()
        total = self.source(i)[self.cut(i, self.bits[i]), :] + self.ins[i][...]
        if i < 2:
            self.sums[i][...] = total
            self.hop(i + 1).start()
        else:
            self.all_z[self.at.z] = total
            for k, other in enumerate(self.at.others):
                self.along_z(k, other).start()

    def along_z(self, k, other):
        block = self.all_z.at[self.at.z]
        return remote(block, block, self.pair(3, k), other)

    def total(self):
        for k, other in enumerate(self.at.others):
            self.along_z(k, other).wait_recv()
        for i in range(3):
            self.hop(i).wait_send()
        for k, other in enumerate(self.at.others):
            self.along_z(k, other).wait_send()
        v = self.all_z
        return (v[0] + v[1]) + (v[2] + v[3])


def fold_bufs(emb):
    return [pltpu.VMEM((n, emb), F32) for n in (64, 32, 16, 64, 32)] + [pltpu.VMEM((4, 16, emb), F32)]


SPREAD_SEMS = (2, 10, 4)
STOPS = range(4)
FOLD_SEMS = (2, 4, 4)
HOT_AT, COLD_AT = FREQ, FREQ + 64


def class_sums(cls_t, three, sums):
    pick_t = (cls_t[...] == iota((sums.shape[0], cls_t.shape[1]), 0)).astype(BF)
    hi, mid, lo = [dot32(pick_t, three[i]) for i in range(3)]
    sums[...] = hi + (mid + lo)


ORDER = [(b & 3) * 8 + (b >> 2 & 1) * 4 + (b >> 3 & 1) * 2 + (b >> 4) for b in range(FREQ // RUN)]


def pick_kernel(pick, table, out):
    out[...] = dot32(pick[...], table[...]).astype(BF)


def pick_rows(pick, table):
    n_l, n, emb = table.shape
    return pl.pallas_call(
        pick_kernel, grid=(n_l,),
        in_specs=[spec(pick.shape, pipeline_mode=ONCE), pl.BlockSpec((None, n, emb), lambda l: (l, 0, 0))],
        out_specs=pl.BlockSpec((None, len(pick), emb), lambda l: (l, 0, 0)),
        out_shape=out_of((n_l, len(pick), emb), BF), compiler_params=params("arbitrary"),
        cost_estimate=cost(len(pick) * table.size, n_l), name="pick_rows",
    )(pick, table)


def hot_kernel(any_freq, raw, freq, code, out, parts):
    n_dev, n_r, _ = raw.shape
    layer, block = pl.program_id(0), pl.program_id(1)
    n = RUN * n_dev
    for g in range(n_r // RUN):
        for o in range(n_dev):
            out[pl.ds(g * n + o * RUN, RUN), :] = raw[o, pl.ds(g * RUN, RUN), :]

    @pl.when(any_freq[block] > 0)
    def _():
        for j in range(freq.shape[1] // RUN):
            @pl.when(layer == j)
            def _(j=j):
                rows = jnp.concatenate([freq[o, j * RUN:(j + 1) * RUN, :] for o in ORDER])
                for i, part in enumerate(split3(rows)):
                    parts[i] = part
        sel = (code[...] == iota((n_r * n_dev, FREQ), 1)).astype(BF)
        out[...] += dot32(sel, parts[0]) + (dot32(sel, parts[1]) + dot32(sel, parts[2]))


def hot_out(gathered, code, any_freq, n_l):
    n_dev, n_rows, emb = gathered.shape
    width = len(code) // len(any_freq)
    n_r = width // n_dev
    blocks = len(code) // width
    return pl.pallas_call(
        hot_kernel,
        grid_spec=pltpu.PrefetchScalarGridSpec(
            num_scalar_prefetch=1, grid=(n_l, blocks),
            in_specs=[
                pl.BlockSpec((n_dev, n_r, emb), lambda i, b, _: (0, i * blocks + b, 0)),
                spec((n_dev, n_l * RUN, emb), 0, n_rows // (n_l * RUN) - 1, 0, pipeline_mode=ONCE),
                pl.BlockSpec((width, 1), lambda i, b, _: (b, 0)),
            ],
            out_specs=pl.BlockSpec((None, width, emb), lambda i, b, _: (n_l - 1 - i, b, 0)),
            scratch_shapes=[pltpu.VMEM((3, FREQ, emb), BF)]),
        out_shape=out_of((n_l, len(code), emb)),
        compiler_params=params("arbitrary", "arbitrary"),
        cost_estimate=cost(gathered.size * LO, n_l), name="hot_out",
    )(any_freq, gathered, gathered, code)


def rows_kernel(numbers, row_of, sums, freq, into, out, stage, got, sem):
    n_used, cold_row, cold_no = [numbers[i] for i in range(3)]
    n_l = len(sums)

    def put(k, row):
        return pltpu.make_async_copy(stage.at[pl.ds(k, 1)], out.at[pl.ds(row, 1)], sem)

    def fill(k, src, at):
        for i in range(n_l):
            stage[k, pl.ds(n_l - 1 - i, 1), :] = src(i, at)

    @pl.loop(0, n_used)
    def _(k):
        fill(k, lambda i, at: sums[i, pl.ds(at, 1), :], COLD_AT + k)
        put(k, row_of[k]).start()

    @pl.when(cold_row >= 0)
    def _():
        c = pltpu.make_async_copy(freq.at[len(freq) - 1, pl.ds(n_l * (COLD_AT - HOT_AT), n_l * RUN)], got, sem)
        c.start()
        c.wait()
        fill(COLD_MAX, lambda i, at: got[pl.ds(i * RUN + at, 1), :], cold_no)
        put(COLD_MAX, cold_row).start()
        put(0, 0).wait()

    @pl.loop(0, n_used)
    def _(k):
        put(0, 0).wait()


def put_rows(numbers, row_of, sums, freq, into):
    n_l, _, emb = sums.shape
    return pl.pallas_call(
        rows_kernel,
        grid_spec=pltpu.PrefetchScalarGridSpec(
            num_scalar_prefetch=2, grid=(1,),
            in_specs=[spec(sums.shape), ANY, ANY], out_specs=ANY,
            scratch_shapes=[pltpu.VMEM((COLD_MAX + 1, n_l, emb), F32), pltpu.VMEM((n_l * RUN, emb), F32), pltpu.SemaphoreType.DMA(())]),
        out_shape=out_of(into.shape), input_output_aliases={4: 0},
        compiler_params=params("arbitrary"), name="put_rows",
    )(numbers, row_of, sums, freq, into)


def merge_kernel(keep, *refs):
    n = (len(refs) - 1) // 3
    sem = refs[-1]

    @pl.when(keep[0] == 0)
    def _():
        copies = [pltpu.make_async_copy(src, dst, sem.at[i]) for i, (src, dst) in enumerate(zip(refs[n:2 * n], refs[2 * n:]))]
        for c in copies:
            c.start()
        for c in copies:
            c.wait()


def merge(keep, fast, general):
    n = len(fast)
    return pl.pallas_call(
        merge_kernel,
        in_specs=[pl.BlockSpec(memory_space=pltpu.SMEM)] + [ANY] * 2 * n, out_specs=[ANY] * n,
        out_shape=[out_of(v.shape, v.dtype) for v in fast], scratch_shapes=[pltpu.SemaphoreType.DMA((n,))],
        input_output_aliases={i + 1: i for i in range(n)}, name="merge",
    )(keep, *fast, *general)


def empty_kernel(*_):
    pass


def empty(like):
    return pl.pallas_call(empty_kernel, out_specs=[ANY] * len(like), out_shape=[out_of(v.shape, v.dtype) for v in like], name="empty")()


def down_sum(v):
    return jnp.sum(v, axis=0)


def beside(*v):
    return jnp.concatenate(v, axis=1)


def row_sum(v):
    return jnp.sum(v, axis=1)


def square(n):
    return iota((n, n), 0), iota((n, n), 1)


def prefix(v):
    r, c = square(len(v))
    return row_sum(jnp.where(r > c, row(v), 0))


def digits(ids, n_hi):
    return one_hot(ids >> HI_BITS, n_hi), one_hot(ids & (LO - 1), LO)


def look(hi_lo, *maps):
    hi, lo = hi_lo
    got = dot32(hi, beside(*maps))
    return [row_sum(got[:, i * LO:(i + 1) * LO] * lo.astype(F32)).astype(I32) for i in range(len(maps))]


def number(count, most):
    levels = jnp.array(LEVELS, F32)
    n_over = jnp.sum((count[:, :, None] >= levels).astype(F32), axis=(0, 1))
    flag = count >= jnp.min(jnp.where(n_over <= most, levels, jnp.inf))
    r, c = square(LO)
    in_row = dot32(flag.astype(BF), (r < c).astype(BF))
    return jnp.where(flag, in_row + col(prefix(row_sum(flag.astype(F32)))) + 1, 0)


def solution(mesh):
    n_dev = mesh.shape['emb']

    def body(token_ids, hot_ids, x_in, d_out, emb_table, hot_table, w_up, w_down, w_gate, w_proj):
        n_loc = len(token_ids)
        layers, rows_dev, emb_dim = emb_table.shape
        n_hot = len(hot_ids)
        places, hot_dev = n_loc // n_dev, n_hot // n_dev
        n_hi = -(-rows_dev * n_dev // (8 * LO)) * 8
        me = lax.axis_index('emb')
        hot_at, cold_at = FREQ, FREQ + hot_dev

        def exchange(v):
            return swap(v.reshape(n_dev, places, -1)).reshape(n_loc, -1)

        def prepare(got_class, hot_hi, hot_lo, row_used, cold_owner, freq_cold, freq_map, hot_table, by_row, move, d_out):
            (hot_f,) = look((hot_hi, hot_lo), freq_map)
            used_rank = prefix(row_used.astype(I32))
            at_rank = (row(used_rank) == iota((COLD_MAX, rows_dev), 0)) & row(row_used)
            row_of = row_sum(jnp.where(at_rank, iota((COLD_MAX, rows_dev), 1), 0))
            packed = pack_rows(row_of, by_row)
            mine_no = jnp.where(hot_owner == me, FREQ_HOT + hot_place, -1)
            wanted = jnp.where(hot_f <= FREQ_HOT, hot_f - 1, -1)
            pick_no = iota((FREQ + hot_dev, n_hot), 0)
            hot_rows = pick_rows(((row(wanted) == pick_no) | (row(mine_no) == pick_no)).astype(BF), hot_table)
            table = jnp.stack([jnp.concatenate([
                hot_rows[i, :FREQ_HOT], dot32(one_hot(cold_owner, n_dev), freq_cold[:, i]).astype(BF),
                hot_rows[i, FREQ_HOT:FREQ_HOT + hot_dev], packed[:, i]]) for i in range(layers)])
            n_used = jnp.minimum(jnp.sum(row_used.astype(I32)), COLD_MAX)
            row_no = got_class - cold_at
            used_before = row_sum(jnp.where(row(row_used) & (iota((n_loc, rows_dev), 1) < col(row_no)), 1, 0))
            cls = jnp.where(row_no >= 0, cold_at + used_before, got_class)
            any_freq = (wanted.reshape(-1, 4 * RUN * n_dev) >= 0).any(axis=1).astype(I32)
            numbers = jnp.stack([n_used, my_row, jnp.minimum(jnp.sum(my_cold * jnp.arange(FREQ_COLD, dtype=I32)), FREQ_COLD - 1)])
            d_placed = dot32(move, d_out).astype(BF)
            return d_placed, table, cls, numbers, row_of, wanted.reshape(-1, 1), any_freq

        count, zeros = count_ids(swap(jnp.broadcast_to(row(token_ids), (n_dev, n_loc))), n_hi, (rows_dev, layers, emb_dim))
        tok, hot = digits(token_ids, n_hi), digits(hot_ids, n_hi)
        slot_no = jnp.arange(n_hot, dtype=I32)
        hot_place = slot_no // (RUN * n_dev) * RUN + slot_no % RUN
        hot_owner = slot_no // RUN % n_dev
        q_map = dot32(hot[0].T, hot[1] * col((hot_place + 1).astype(BF))).astype(BF)
        r_map = dot32(hot[0].T, hot[1] * col(hot_owner.astype(BF))).astype(BF)
        hot_no = number(jnp.where(q_map > 0, count, 0), FREQ_HOT)
        cold_no = number(jnp.where(q_map > 0, 0, count), FREQ_COLD)
        freq_map = jnp.where(hot_no > 0, hot_no, jnp.where(cold_no > 0, FREQ_HOT + cold_no, 0)).astype(BF)
        id_map = iota((n_hi, LO), 0) * LO + iota((n_hi, LO), 1) + 1
        cold_id = jnp.sum(jnp.where(cold_no.astype(I32)[None] == iota((FREQ_COLD, 1, 1), 0) + 1, id_map[None], 0), axis=(1, 2)) - 1
        cold_owner = jnp.where(cold_id >= 0, cold_id // rows_dev, -1)
        my_cold = (cold_owner == me).astype(I32)
        my_row = jnp.minimum(jnp.sum(my_cold * (cold_id - me * rows_dev + 1)) - 1, rows_dev - 1)
        by_row = emb_table.transpose(1, 0, 2)
        cold_row = lax.dynamic_slice_in_dim(by_row, jnp.maximum(my_row, 0), 1)
        freq_cold = swap(jnp.broadcast_to(cold_row, (n_dev, layers, emb_dim)))

        tok_f, tok_q, tok_r = look(tok, freq_map, q_map, r_map)
        rare = tok_f == 0
        owner = jnp.where(tok_q > 0, tok_r, token_ids // rows_dev)
        dev_no = iota((n_loc, n_dev), 1)
        to_dev = (col(owner) == dev_no) & col(rare)
        marks = beside(to_dev.astype(BF), col(jnp.logical_not(rare).astype(BF)))
        r, c = square(n_loc)
        ranks = dot32((r > c).astype(BF), marks)
        sent = down_sum(to_dev.astype(F32))
        free = jnp.maximum(places - sent, 0)
        free_at = prefix(free)
        fill = ranks[:, n_dev:]
        fill_dev = (fill >= free_at) & (fill < free_at + free)
        to_dev = jnp.where(col(rare), to_dev, fill_dev)
        place = jnp.where(col(rare), ranks[:, :n_dev], fill + (sent - free_at))
        slot = row_sum(jnp.where(to_dev, dev_no * places + place.astype(I32), 0))
        row_ids = me * rows_dev + jnp.arange(rows_dev, dtype=I32)
        row_f, row_q, row_n = look(digits(row_ids, n_hi), freq_map, q_map, (count > 0).astype(BF))
        row_used = (row_n > 0) & (row_f == 0) & (row_q == 0)
        fits = ((jnp.max(sent) <= places) & (jnp.sum(row_used.astype(I32)) <= COLD_MAX) & (jnp.sum(my_cold) <= 1))
        tok_class = jnp.where(rare, jnp.where(tok_q > 0, hot_at + tok_q - 1, cold_at + token_ids % rows_dev), tok_f - 1)
        bad = 1 << 20
        move = r == row(slot)
        send_class, freq_cold = lax.optimization_barrier(
            (row_sum(jnp.where(move, row(tok_class), 0)) + jnp.where(fits, 0, bad), freq_cold))
        got_class = swap(send_class.reshape(n_dev, places)).reshape(n_loc)
        move = move.astype(BF)
        placed, got_class, hot_hi, hot_lo, row_used, cold_owner = lax.optimization_barrier(
            (dot32(move, x_in).astype(BF), got_class, *hot, row_used, cold_owner))
        x_moved = exchange(placed)
        given = prepare(got_class, hot_hi, hot_lo, row_used, cold_owner, freq_cold, freq_map, hot_table, by_row, move, d_out)
        all_fit = jnp.max(got_class) < bad

        x_moved, d_placed, table, cls, numbers, row_of, code, any_freq = lax.optimization_barrier((x_moved, *given))
        cls_row = cls.reshape(1, n_loc)
        xs, hs, ss, es, x_last, d_moved = forward(x_moved, cls.reshape(n_loc, 1), table, w_up, w_down, w_gate, w_proj, d_placed, n_dev)
        sums, gathered = backward(d_moved, cls_row, es, xs, hs, ss, w_up, w_down, w_gate, w_proj, n_dev)
        x_last, gathered = lax.optimization_barrier((x_last, gathered))
        x_back = exchange(x_last)
        d_table = put_rows(numbers, row_of, sums, gathered, zeros)
        d_hot = hot_out(gathered, code, any_freq, layers)
        x_out = dot32((col(slot) == iota((n_loc, n_loc), 1)).astype(BF), x_back).astype(BF)
        *fast, fit = lax.optimization_barrier((x_out, d_table, d_hot, all_fit))

        def slow():
            x, table_grad, hot_grad = general_path(n_dev, me, token_ids, hot_ids, x_in, d_out, emb_table, hot_table, w_up, w_down, w_gate, w_proj)
            return x, table_grad.transpose(1, 0, 2), hot_grad

        general = lax.cond(fit, lambda: tuple(empty(fast)), slow)
        x_out, d_table, d_hot = merge(fit.astype(I32).reshape(1), fast, general)
        return x_out, d_table.transpose(1, 0, 2), d_hot

    return jax.shard_map(body, mesh=mesh,
                         in_specs=(P('emb'), P(), P('emb', None), P('emb', None), P(None, 'emb', None), P(), P(), P(), P(), P()),
                         out_specs=(P('emb', None), P(None, 'emb', None), P()),
                         check_vma=False)
```
